32 devices in a mesh: dp: 8 (over y, x, core), tensor: 4 (over z).
Axes of the slice: x: 2, y: 2, z: 4, core: 2. Of those that a mesh axis runs over, the one named last changes fastest.
Arguments:
- activations: bfloat16 [64, 1024, 1024], P(('dp', 'tensor')), may hold values from -6 to 6
- routes: int32 [64, 128], P('dp'), may hold values from 0 to 1023, as said below
- pic_start: int32 [64], P('dp'), may hold values from 0 to 768, as said below
- router_w: bfloat16 [1024], P('dp'), may hold values from -0.1875 to 0.1875
- gain_attn: bfloat16 [1024], P('dp'), may hold values from 0.099609375 to 1.8984375
- gain_mlp: bfloat16 [1024], P('dp'), may hold values from 0.099609375 to 1.8984375
- w_query: bfloat16 [1024, 1024], P('dp', 'tensor'), may hold values from -0.1875 to 0.1875
- w_key: bfloat16 [1024, 1024], P('dp', 'tensor'), may hold values from -0.1875 to 0.1875
- w_value: bfloat16 [1024, 1024], P('dp', 'tensor'), may hold values from -0.1875 to 0.1875
- w_proj: bfloat16 [1024, 1024], P('dp', 'tensor'), may hold values from -1.5 to 1.5
- w_up: bfloat16 [1024, 4096], P('dp', 'tensor'), may hold values from -0.1875 to 0.1875
- w_down: bfloat16 [1024, 4096], P('dp', 'tensor'), may hold values from -0.09375 to 0.09375
- cotangent: bfloat16 [64, 1024, 1024], P(('dp', 'tensor')), may hold values from -6 to 6
Outputs:
- result: bfloat16 [64, 1024, 1024], P(('dp', 'tensor'))
- grad_input: bfloat16 [64, 1024, 1024], P(('dp', 'tensor'))
- grad_router: float32 [1024], P('dp')
- grad_gain_attn: float32 [1024], P('dp')
- grad_gain_mlp: float32 [1024], P('dp')
- grad_query: float32 [1024, 1024], P('dp', 'tensor')
- grad_key: float32 [1024, 1024], P('dp', 'tensor')
- grad_value: float32 [1024, 1024], P('dp', 'tensor')
- grad_proj: float32 [1024, 1024], P('dp', 'tensor')
- grad_up: float32 [1024, 4096], P('dp', 'tensor')
- grad_down: float32 [1024, 4096], P('dp', 'tensor')
The draws below stay inside these ranges and needn't reach their ends.
Inputs may be any that keep to these rules, and one draw needn't show every extreme that they name: `routes`: each row names 128 different positions of its sequence, in increasing order. A sequence's picture span holds the positions pic_start to pic_start + 255.
All inputs are finite; a program needn't handle non-finite values.
Results may differ from the reference program's by a relative error of at most 0.014.
Values may be sent and summed in bfloat16 or wider, within the bound.
A program may use at most 128 MiB of HBM per device.

```python
import math
import jax
import jax.numpy as jnp
from jax import lax

D = 1024
H = 16
HD = 64
FF = 4096
SEQ = 1024
CAP = 128
PIC = 256
SEQS = 64


def draw_routes(key, part):
    seq_keys = jax.random.split(jax.random.fold_in(key, 11), SEQS)

    def pick_one(seq_key):
        return jnp.sort(jax.random.permutation(seq_key, SEQ)[:CAP]).astype(jnp.int32)
    return jax.vmap(pick_one)(seq_keys)


def draw_pic_start(key, part):
    base = jax.random.fold_in(key, 23)
    starts = jax.random.randint(jax.random.fold_in(base, 1), (SEQS,), 0, SEQ - PIC + 1).astype(jnp.int32)
    first = jax.random.randint(jax.random.fold_in(base, 2), (), 0, SEQS)
    other = (first + 1 + jax.random.randint(jax.random.fold_in(base, 3), (), 0, SEQS - 1)) % SEQS
    starts = starts.at[first].set(0)
    starts = starts.at[other].set(SEQ - PIC)
    return starts.astype(jnp.int32)


def strengthened(drawn, rng, source, target, parts, factor):
    owner, partner = [(jnp.arange(drawn.shape[position]) // (drawn.shape[position] // parts)).reshape([-1 if axis == position else 1 for axis in range(drawn.ndim)]) for position in (source, target)]
    chosen = jax.random.permutation(rng, parts)[partner]
    strong = (owner == chosen) | (owner == (partner + parts // 2) % parts)
    return jnp.where(strong, factor * drawn, drawn)


def block_levels(stream_key, shape, pieces, low, largest):
    def one(dim, shards_of):
        heights = jax.random.uniform(jax.random.fold_in(jax.random.fold_in(stream_key, 6), dim), (shards_of,), jnp.float32, low / len(pieces), largest / len(pieces))
        return jnp.repeat(jnp.exp(heights), shape[dim] // shards_of).reshape((-1,) + (1,) * (len(shape) - dim - 1))

    loudness = one(*pieces[0])
    for cut in pieces[1:]:
        loudness = loudness * one(*cut)
    return loudness


def gaussian(rng, extent, width, most, cuts=(), held_as=jnp.bfloat16):
    factor_of = block_levels(rng, extent, cuts, -0.22, 0.18) if cuts else 1.0
    values = jax.random.normal(rng, extent, jnp.float32) * width * factor_of
    return jnp.minimum(jnp.maximum(values, -most), most).astype(held_as)


def gaussian_with(own_key, dims, spread, reach, cuts, heavy, kind=jnp.bfloat16):
    values = spread * jax.random.normal(own_key, dims, jnp.float32)
    if cuts:
        values = values * block_levels(own_key, dims, cuts, -0.22, 0.18)
    return jnp.clip(strengthened(values, jax.random.fold_in(own_key, 3), *heavy), -reach, reach).astype(kind)


def setup_inputs(seed: int = 0) -> dict:
    keys = jax.random.split(jax.random.key(seed), 14)
    activations = gaussian_with(keys[0], (SEQS, SEQ, D), 1.0, 6.0, ((0, 32),), (0, 2, 32, 2.75))
    routes = draw_routes(jax.random.fold_in(keys[13], 71), 0)
    pic_start = draw_pic_start(jax.random.fold_in(keys[13], 71), 0)
    router_w = gaussian(keys[3], (D,), D ** -0.5, 0.1875, ((0, 8),))
    gain_attn = jnp.clip(1.0 + 0.18 * jax.random.normal(keys[4], (D,), jnp.float32), 0.099609375, 1.8984375).astype(jnp.bfloat16)
    gain_mlp = jnp.clip(1.0 + 0.18 * jax.random.normal(keys[5], (D,), jnp.float32), 0.099609375, 1.8984375).astype(jnp.bfloat16)
    w_query = gaussian(keys[6], (D, H * HD), D ** -0.5, 0.1875, ((0, 8), (1, 4)))
    w_key = gaussian(keys[7], (D, H * HD), D ** -0.5, 0.1875, ((0, 8), (1, 4)))
    w_value = gaussian(keys[8], (D, H * HD), D ** -0.5, 0.1875, ((0, 8), (1, 4)))
    w_proj = gaussian(keys[9], (D, H * HD), (H * HD * 2 // CAP) ** -0.5, 1.5, ((0, 8), (1, 4)))
    w_up = gaussian(keys[10], (D, FF), D ** -0.5, 0.1875, ((0, 8), (1, 4)))
    w_down = gaussian(keys[11], (D, FF), FF ** -0.5, 0.09375, ((0, 8), (1, 4)))
    cotangent = gaussian_with(keys[12], (SEQS, SEQ, D), 1.0, 6.0, ((0, 32),), (0, 2, 32, 2.75))
    return dict(activations=activations, routes=routes, pic_start=pic_start, router_w=router_w, gain_attn=gain_attn, gain_mlp=gain_mlp, w_query=w_query, w_key=w_key, w_value=w_value, w_proj=w_proj, w_up=w_up, w_down=w_down, cotangent=cotangent)


@jax.custom_vjp
def low(v):
    return lax.optimization_barrier(v.astype(jnp.bfloat16)).astype(jnp.float32)

@jax.custom_vjp
def low_back(v):
    return v

def low_keep(v):
    return (low(v), None)

def low_pass(kept, grad):
    return (grad,)

def back_keep(v):
    return (v, None)

def back_low(kept, grad):
    return (low(grad),)
low.defvjp(low_keep, low_pass)
low_back.defvjp(back_keep, back_low)

def precise(form, left, right):
    return jnp.einsum(form, left, right, precision=lax.Precision.HIGHEST)

def normalize(values, gain):
    return values * lax.rsqrt(lax.optimization_barrier(jnp.mean(values * values, axis=-1, keepdims=True)) + 1e-06) * gain

def span_mask(positions, starts):
    later = positions[:, None, :] <= positions[:, :, None]
    begin = starts[:, None]
    inside = (positions >= begin) & (positions < begin + PIC)
    return later | inside[:, :, None] & inside[:, None, :]

def layer(seq_block, route_block, start_block, w_query, w_key, w_value, w_proj, w_up, w_down, gain_attn, gain_mlp, router_w):
    nseqs = seq_block.shape[0]
    seq_lines = jnp.arange(nseqs).astype(jnp.int32)[:, None]
    picked = seq_block[seq_lines, route_block]
    gating = jax.nn.sigmoid(jnp.einsum('bcd,d->bc', picked, router_w, precision=lax.Precision.HIGHEST))
    norm_one = low(normalize(picked, gain_attn))
    queries = low(low_back(precise('bcd,de->bce', norm_one, w_query))).reshape(nseqs, CAP, H, HD)
    key_rows = low(low_back(precise('bcd,de->bce', norm_one, w_key))).reshape(nseqs, CAP, H, HD)
    value_rows = low(low_back(precise('bcd,de->bce', norm_one, w_value))).reshape(nseqs, CAP, H, HD)
    allowed = span_mask(route_block, start_block)
    scores = low_back(precise('bqhe,bkhe->bhqk', queries, key_rows) * (1.0 / math.sqrt(HD)))
    scores = jnp.where(allowed[:, None], scores, -1e+30)
    attn_probs = jax.nn.softmax(scores, axis=-1)
    context = precise('bhqk,bkhe->bqhe', low(attn_probs), value_rows).reshape(nseqs, CAP, H * HD)
    context = low(low_back(context))
    attended = low_back(precise('bce,de->bcd', context, w_proj))
    residual = picked + attended
    norm_two = low(normalize(residual, gain_mlp))
    pre_act = low_back(precise('bcd,df->bcf', norm_two, w_up))
    hidden = low(jax.nn.gelu(pre_act, approximate=False))
    mlp_out = low_back(precise('bcf,df->bcd', hidden, w_down))
    return seq_block.at[seq_lines, route_block].add(gating[..., None] * (attended + mlp_out))

def reference(activations, routes, pic_start, router_w, gain_attn, gain_mlp, w_query, w_key, w_value, w_proj, w_up, w_down, cotangent):
    weights = tuple((w.astype(jnp.float32) for w in (w_query, w_key, w_value, w_proj, w_up, w_down, gain_attn, gain_mlp, router_w)))
    group_size = math.gcd(SEQS, 4)
    blocks = SEQS // group_size
    seq_blocks = activations.reshape(blocks, group_size, SEQ, D)
    route_blocks = routes.reshape(blocks, group_size, CAP)
    start_blocks = pic_start.reshape(blocks, group_size)
    grad_blocks = cotangent.reshape(blocks, group_size, SEQ, D)

    def advance(totals, item):
        seq_block, route_block, start_block, grad_block = item

        def forward(inputs_f32, *params):
            return layer(inputs_f32, route_block, start_block, *params)
        result_rows, pullback = jax.vjp(forward, seq_block.astype(jnp.float32), *weights)
        gradients = pullback(grad_block.astype(jnp.float32))
        totals = tuple((a + g for a, g in zip(totals, gradients[1:])))
        return (totals, (result_rows.astype(jnp.bfloat16), gradients[0].astype(jnp.bfloat16)))
    initial = tuple((jnp.zeros(w.shape, jnp.float32) for w in weights))
    totals, outputs = lax.scan(advance, initial, (seq_blocks, route_blocks, start_blocks, grad_blocks))
    result = outputs[0].reshape(SEQS, SEQ, D)
    grad_input = outputs[1].reshape(SEQS, SEQ, D)
    return (result, grad_input, totals[8], totals[6], totals[7], totals[0], totals[1], totals[2], totals[3], totals[4], totals[5])
```

```python
import functools
import math

import jax
import jax.numpy as jnp
from jax import lax
from jax.experimental import pallas as pl
from jax.experimental.pallas import tpu as pltpu
from jax.sharding import PartitionSpec as P

HD = 64
PIC = 256
AHEAD = 1
MESH = pl.DeviceIdType.MESH
ANY = pl.BlockSpec(memory_space=pl.ANY)
VMEM = pl.BlockSpec(memory_space=pltpu.VMEM)
BF16 = jnp.bfloat16
F32 = jnp.float32

inv_root_two = 0.7071067811865476
inv_root_two_pi = 0.3989422804014327


def bit_of(value, bit):
    return lax.rem(lax.div(value, 1 << bit), 2)


def flipped(value, bit):
    return value + (1 - 2 * bit_of(value, bit)) * (1 << bit)


def cleared(value, bits):
    for bit in bits:
        value = value - bit_of(value, bit) * (1 << bit)
    return value


def spread(step, bits):
    value = 0
    for place, bit in enumerate(bits):
        value = value + lax.rem(lax.div(step, 1 << place), 2) * (1 << bit)
    return value


def each(count, body):
    if count <= 4:
        for step in range(count):
            body(jnp.int32(step))
    else:
        lax.fori_loop(0, count, lambda step, _: body(step), None)


def orders(bits):
    return (tuple(range(bits - 1, 0, -1)), tuple(range(1, bits)))


def meet(bits, ranks):
    me, rank = lax.axis_index("dp"), lax.axis_index("tensor")
    barrier = pltpu.get_barrier_semaphore()
    for bit in range(bits):
        pl.semaphore_signal(barrier, 1, device_id=(flipped(me, bit), rank), device_id_type=MESH)
    for hop in range(1, ranks):
        pl.semaphore_signal(
            barrier, 1, device_id=(me, lax.rem(rank + hop, ranks)), device_id_type=MESH
        )
    pl.semaphore_wait(barrier, bits + ranks - 1)


def remote(src, dst, send, recv, where):
    return pltpu.make_async_remote_copy(
        src_ref=src, dst_ref=dst, send_sem=send, recv_sem=recv, device_id=where, device_id_type=MESH
    )


def gather_kernel(bits, ranks, chunks, *refs):
    shards, (vec,) = refs[:chunks], refs[chunks : chunks + 1]
    wholes = refs[chunks + 1 : 2 * chunks + 1]
    (
        vec_out,
        held,
        vecs,
        send_z,
        recv_z,
        send_p,
        recv_p,
        send_c,
        recv_c,
        send_v,
        recv_v,
        local,
        leave,
    ) = refs[2 * chunks + 1 :]
    me, rank = lax.axis_index("dp"), lax.axis_index("tensor")
    rows, width = shards[0].shape
    full = held.shape[2]
    half = full // 2
    paths = orders(bits)
    meet(bits, ranks)

    def band(index):
        return pl.ds(pl.multiple_of(index * rows, rows), rows)

    mine = band(me)
    columns = pl.ds(pl.multiple_of(rank * width, width), width)
    for chunk in range(chunks):
        pltpu.make_async_copy(shards[chunk], held.at[chunk, mine, columns], local.at[chunk]).start()
    pltpu.make_async_copy(vec, vecs.at[me], local.at[chunks]).start()
    for chunk in range(chunks):
        for hop in range(1, ranks):
            remote(
                shards[chunk],
                held.at[chunk, mine, columns],
                send_z.at[chunk],
                recv_z.at[chunk],
                (me, lax.rem(rank + hop, ranks)),
            ).start()
    pltpu.make_async_copy(vec, vecs.at[me], local.at[chunks]).wait()
    path = tuple(range(bits - 1, -1, -1))
    for stage, bit in enumerate(path):
        other = (flipped(me, bit), rank)

        def send(step, stage=stage, other=other):
            index = cleared(me, path[:stage]) + spread(step, path[:stage])
            remote(
                vecs.at[index], vecs.at[index], send_v.at[stage], recv_v.at[stage], other
            ).start()

        each(1 << stage, send)
        span = vecs.at[pl.ds(0, 1 << stage)]
        remote(span, span, send_v.at[stage], recv_v.at[stage], other).wait()

    def bulk(chunk, depth, breadth):
        return held.at[chunk, pl.ds(0, depth), pl.ds(0, breadth)]

    def wait_z(chunk):
        pltpu.make_async_copy(
            shards[chunk], held.at[chunk, mine, columns], local.at[chunk]
        ).wait()
        span = bulk(chunk, rows, width * (ranks - 1))
        remote(span, span, send_z.at[chunk], recv_z.at[chunk], (me, rank)).wait_recv()

    def send_path(chunk, colour, stage):
        order = paths[colour]
        other = (flipped(me, order[stage]), rank)

        def send(step):
            index = cleared(me, order[:stage]) + spread(step, order[:stage])
            block = held.at[chunk, band(index), pl.ds(colour * half, half)]
            remote(
                block,
                block,
                send_p.at[chunk, colour, stage],
                recv_p.at[chunk, colour, stage],
                other,
            ).start()

        each(1 << stage, send)

    def path_copy(chunk, colour, stage):
        span = bulk(chunk, rows << stage, half)
        return remote(
            span,
            span,
            send_p.at[chunk, colour, stage],
            recv_p.at[chunk, colour, stage],
            (me, rank),
        )

    def send_core(chunk):
        other = (flipped(me, 0), rank)

        def send(step):
            index = cleared(me, range(1, bits)) + spread(step, range(1, bits))
            block = held.at[chunk, band(index)]
            remote(block, block, send_c.at[chunk], recv_c.at[chunk], other).start()

        each(1 << (bits - 1), send)

    def core_copy(chunk):
        span = bulk(chunk, rows << (bits - 1), full)
        return remote(span, span, send_c.at[chunk], recv_c.at[chunk], (me, rank))

    last = bits
    for tick in range(chunks + AHEAD * last):
        for stage in range(last, -1, -1):
            chunk = tick - AHEAD * stage
            if not 0 <= chunk < chunks:
                continue
            if stage == 0:
                wait_z(chunk)
            elif stage < last:
                for colour in range(2):
                    path_copy(chunk, colour, stage - 1).wait_recv()
            else:
                core_copy(chunk).wait_recv()
            if stage < last - 1:
                for colour in range(2):
                    send_path(chunk, colour, stage)
            elif stage == last - 1:
                send_core(chunk)
            else:
                pltpu.make_async_copy(held.at[chunk], wholes[chunk], leave.at[chunk]).start()
    vec_out[...] = vecs[...]
    for chunk in range(chunks):
        pltpu.make_async_copy(held.at[chunk], wholes[chunk], leave.at[chunk]).wait()
        span = bulk(chunk, rows, width * (ranks - 1))
        remote(span, span, send_z.at[chunk], recv_z.at[chunk], (me, rank)).wait_send()
        for colour in range(2):
            for stage in range(bits - 1):
                path_copy(chunk, colour, stage).wait_send()
        core_copy(chunk).wait_send()


def gather_weights(bits, ranks, shards, vec):
    chunks = len(shards)
    rows, width = shards[0].shape
    depth, breadth = rows << bits, width * ranks
    dma = pltpu.SemaphoreType.DMA
    outs = pl.pallas_call(
        functools.partial(gather_kernel, bits, ranks, chunks),
        out_shape=[jax.ShapeDtypeStruct((depth, breadth), BF16)] * chunks
        + [jax.ShapeDtypeStruct((1 << bits, 8, 128), F32)],
        in_specs=[ANY] * chunks + [VMEM],
        out_specs=[ANY] * chunks + [VMEM],
        scratch_shapes=[
            pltpu.VMEM((chunks, depth, breadth), BF16),
            pltpu.VMEM((1 << bits, 8, 128), F32),
            dma((chunks,)),
            dma((chunks,)),
            dma((chunks, 2, bits - 1)),
            dma((chunks, 2, bits - 1)),
            dma((chunks,)),
            dma((chunks,)),
            dma((bits,)),
            dma((bits,)),
            dma((chunks + 1,)),
            dma((chunks,)),
        ],
        compiler_params=pltpu.CompilerParams(
            collective_id=1, has_side_effects=True, vmem_limit_bytes=60 << 20
        ),
        name="gather_weights",
    )(*shards, vec)
    return outs[:chunks], outs[chunks]


def scatter_kernel(bits, ranks, chunks, *refs):
    grads, (vec,) = refs[:chunks], refs[chunks : chunks + 1]
    outs = refs[chunks + 1 : 2 * chunks + 1]
    (
        vec_out,
        total,
        from_core,
        *from_path,
        from_z,
        vecs,
        vec_path,
        vec_z,
        send_c,
        recv_c,
        send_p,
        recv_p,
        send_z,
        recv_z,
        send_v,
        recv_v,
        local,
    ) = refs[2 * chunks + 1 :]
    me, rank = lax.axis_index("dp"), lax.axis_index("tensor")
    rows, width = outs[0].shape
    full = total.shape[3]
    half = full // 2
    seat, pair = bit_of(me, 0), lax.div(me, 2)
    pairs = 1 << (bits - 1)
    paths = tuple(tuple(bit - 1 for bit in order[::-1]) for order in orders(bits))
    meet(bits, ranks)

    def band(index):
        return pl.ds(pl.multiple_of(index * rows, rows), rows)

    for chunk in range(chunks):

        def send(step, chunk=chunk):
            remote(
                grads[chunk].at[band(2 * step + 1 - seat)],
                from_core.at[chunk, step],
                send_c.at[chunk],
                recv_c.at[chunk],
                (flipped(me, 0), rank),
            ).start()
            pltpu.make_async_copy(
                grads[chunk].at[band(2 * step + seat)], total.at[chunk, step], local.at[chunk]
            ).start()

        each(pairs, send)

    def core_copy(chunk):
        span = from_core.at[chunk]
        return remote(span, span, send_c.at[chunk], recv_c.at[chunk], (me, rank))

    tile = min(rows, 32)

    def add_to(chunk, index, columns, source):
        for start in range(0, rows, tile):
            part = pl.ds(start, tile)
            here = total.at[chunk, index, part, columns]
            here[...] = (here[...].astype(F32) + source[part].astype(F32)).astype(BF16)

    def add_core(chunk):
        lax.fori_loop(
            0,
            pairs,
            lambda step, _: add_to(chunk, step, pl.ds(0, full), from_core.at[chunk, step]),
            None,
        )

    def members(stage, order, step, kept):
        bit, later = order[stage], order[stage + 1 :]
        index = pair if kept else flipped(pair, bit)
        return cleared(index, later) + spread(step, later)

    def send_path(chunk, colour, stage):
        order = paths[colour]
        other = (2 * flipped(pair, order[stage]) + seat, rank)

        def send(step):
            index = members(stage, order, step, False)
            remote(
                total.at[chunk, index, :, pl.ds(colour * half, half)],
                from_path[stage].at[chunk, colour, step],
                send_p.at[chunk, colour, stage],
                recv_p.at[chunk, colour, stage],
                other,
            ).start()

        each(1 << (len(order) - stage - 1), send)

    def path_copy(chunk, colour, stage):
        span = from_path[stage].at[chunk, colour]
        return remote(
            span,
            span,
            send_p.at[chunk, colour, stage],
            recv_p.at[chunk, colour, stage],
            (me, rank),
        )

    def add_path(chunk, colour, stage):
        order = paths[colour]

        def add(step, _):
            index = members(stage, order, step, True)
            add_to(
                chunk,
                index,
                pl.ds(colour * half, half),
                from_path[stage].at[chunk, colour, step],
            )

        lax.fori_loop(0, 1 << (len(order) - stage - 1), add, None)

    def send_across(chunk):
        for hop in range(1, ranks):
            to = lax.rem(rank + hop, ranks)
            remote(
                total.at[chunk, pair, :, pl.ds(pl.multiple_of(to * width, width), width)],
                from_z.at[chunk, hop - 1],
                send_z.at[chunk],
                recv_z.at[chunk],
                (me, to),
            ).start()

    def z_copy(chunk):
        span = from_z.at[chunk]
        return remote(span, span, send_z.at[chunk], recv_z.at[chunk], (me, rank))

    def finish(chunk):
        own = total[chunk, pair, :, pl.ds(pl.multiple_of(rank * width, width), width)]
        summed = own.astype(F32)
        for hop in range(1, ranks):
            summed = summed + from_z[chunk, hop - 1].astype(F32)
        outs[chunk][...] = summed

    last = bits
    for tick in range(chunks + AHEAD * last):
        for stage in range(last, -1, -1):
            chunk = tick - AHEAD * stage
            if not 0 <= chunk < chunks:
                continue
            if stage == 0:
                span = total.at[chunk]
                pltpu.make_async_copy(span, span, local.at[chunk]).wait()
                core_copy(chunk).wait_recv()
                add_core(chunk)
            elif stage < last:
                for colour in range(2):
                    path_copy(chunk, colour, stage - 1).wait_recv()
                    add_path(chunk, colour, stage - 1)
            else:
                z_copy(chunk).wait_recv()
                finish(chunk)
            if stage < last - 1:
                for colour in range(2):
                    send_path(chunk, colour, stage)
            elif stage == last - 1:
                send_across(chunk)
    pltpu.make_async_copy(vec, vecs, local.at[chunks]).start()
    pltpu.make_async_copy(vec, vecs, local.at[chunks]).wait()
    path = tuple(range(bits))
    for stage, bit in enumerate(path):
        later = path[stage + 1 :]
        count = 1 << len(later)
        base = count - 1
        other = (flipped(me, bit), rank)

        def send(step, later=later, bit=bit, base=base, other=other, stage=stage):
            index = cleared(flipped(me, bit), later) + spread(step, later)
            remote(
                vecs.at[index], vec_path.at[base + step], send_v.at[stage], recv_v.at[stage], other
            ).start()

        each(count, send)
        span = vec_path.at[pl.ds(base, count)]
        remote(span, span, send_v.at[stage], recv_v.at[stage], other).wait()

        def add(step, _, later=later, base=base):
            index = cleared(me, later) + spread(step, later)
            vecs[index] = vecs[index] + vec_path[base + step]

        lax.fori_loop(0, count, add, None)
    for hop in range(1, ranks):
        to = (me, lax.rem(rank + hop, ranks))
        remote(vecs.at[me], vec_z.at[hop - 1], send_v.at[bits], recv_v.at[bits], to).start()
    remote(vec_z, vec_z, send_v.at[bits], recv_v.at[bits], (me, rank)).wait()
    summed = vecs[me]
    for hop in range(1, ranks):
        summed = summed + vec_z[hop - 1]
    vec_out[...] = summed
    for chunk in range(chunks):
        core_copy(chunk).wait_send()
        for colour in range(2):
            for stage in range(bits - 1):
                path_copy(chunk, colour, stage).wait_send()
        z_copy(chunk).wait_send()


def scatter_grads(bits, ranks, grads, vec):
    chunks = len(grads)
    depth, breadth = grads[0].shape
    rows, width, pairs = depth >> bits, breadth // ranks, 1 << (bits - 1)
    dma = pltpu.SemaphoreType.DMA
    outs = pl.pallas_call(
        functools.partial(scatter_kernel, bits, ranks, chunks),
        out_shape=[jax.ShapeDtypeStruct((rows, width), F32)] * chunks
        + [jax.ShapeDtypeStruct((8, 128), F32)],
        in_specs=[ANY] * chunks + [VMEM],
        out_specs=[VMEM] * (chunks + 1),
        scratch_shapes=[
            pltpu.VMEM((chunks, pairs, rows, breadth), BF16),
            pltpu.VMEM((chunks, pairs, rows, breadth), BF16),
            *[
                pltpu.VMEM((chunks, 2, pairs >> (stage + 1), rows, breadth // 2), BF16)
                for stage in range(bits - 1)
            ],
            pltpu.VMEM((chunks, ranks - 1, rows, width), BF16),
            pltpu.VMEM((1 << bits, 8, 128), F32),
            pltpu.VMEM((1 << bits, 8, 128), F32),
            pltpu.VMEM((ranks - 1, 8, 128), F32),
            dma((chunks,)),
            dma((chunks,)),
            dma((chunks, 2, bits - 1)),
            dma((chunks, 2, bits - 1)),
            dma((chunks,)),
            dma((chunks,)),
            dma((bits + 1,)),
            dma((bits + 1,)),
            dma((chunks + 1,)),
        ],
        compiler_params=pltpu.CompilerParams(
            collective_id=2, has_side_effects=True, vmem_limit_bytes=60 << 20
        ),
        name="scatter_grads",
    )(*grads, vec)
    return outs[:chunks], outs[chunks]


def normalize(values, gain):
    inverse = lax.rsqrt(jnp.mean(values * values, axis=-1, keepdims=True) + 1e-06)
    return (values * inverse * gain, inverse)


def norm_back(grad_out, values, inverse, gain):
    scaled = grad_out * gain
    grad_in = inverse * scaled - values * inverse * inverse * inverse * jnp.mean(
        scaled * values, axis=-1, keepdims=True
    )
    grad_gain = jnp.sum(grad_out * values * inverse, axis=0)
    return (grad_in, grad_gain)


def gelu_parts(values):
    bell = 0.5 * (1.0 + jax.scipy.special.erf(values * inv_root_two))
    slope = bell + values * jnp.exp(-0.5 * values * values) * inv_root_two_pi
    return (values * bell).astype(BF16), slope


def span_mask(positions, starts):
    later = positions[:, None, :] <= positions[:, :, None]
    begin = starts[:, None]
    inside = (positions >= begin) & (positions < begin + PIC)
    return later | inside[:, :, None] & inside[:, None, :]


def dot(form, left, right):
    return jnp.einsum(form, left, right, preferred_element_type=F32)


def shards(
    activations,
    routes,
    pic_start,
    router_w,
    gain_attn,
    gain_mlp,
    w_query,
    w_key,
    w_value,
    w_proj,
    w_up,
    w_down,
    cotangent,
):
    seqs, length, features = activations.shape
    ranks = lax.axis_size("tensor")
    bits = lax.axis_size("dp").bit_length() - 1
    rank = lax.axis_index("tensor")
    rows, width = w_query.shape
    parts = w_up.shape[1] // width
    own_routes = lax.dynamic_slice_in_dim(routes, rank * seqs, seqs, 0)
    own_start = lax.dynamic_slice_in_dim(pic_start, rank * seqs, seqs, 0)
    caps = routes.shape[1]
    heads = features // HD

    vec = jnp.stack([router_w, gain_attn, gain_mlp]).astype(F32)
    vec = jnp.pad(vec, ((0, 5), (0, 128 - rows)))
    pieces = [w_query, w_key, w_value, w_proj]
    for part in range(parts):
        columns = slice(part * width, (part + 1) * width)
        pieces += [w_up[:, columns], w_down[:, columns]]
    weights, vec_all = gather_weights(bits, ranks, pieces, vec)
    full_query, full_key, full_value, full_proj = weights[:4]
    full_up, full_down = weights[4::2], weights[5::2]
    vec_all = vec_all[:, :3, :rows].transpose(1, 0, 2).reshape(3, features)
    router, gain1, gain2 = vec_all[0], vec_all[1], vec_all[2]

    chosen = (own_routes[:, :, None] == jnp.arange(length)[None, None, :]).astype(BF16)
    picked = dot("scl,sld->scd", chosen, activations).reshape(seqs * caps, features)
    grad_rows = dot("scl,sld->scd", chosen, cotangent).reshape(seqs * caps, features)
    gating = jax.nn.sigmoid(jnp.sum(picked * router, axis=-1, keepdims=True))
    grad_delta = gating * grad_rows
    branch = grad_delta.astype(BF16)

    normed1, inverse1 = normalize(picked, gain1)
    norm_one = normed1.astype(BF16)
    queries = dot("nd,de->ne", norm_one, full_query).astype(BF16)
    key_rows = dot("nd,de->ne", norm_one, full_key).astype(BF16)
    value_rows = dot("nd,de->ne", norm_one, full_value).astype(BF16)
    split = lambda a: a.reshape(seqs, caps, heads, HD)
    allowed = span_mask(own_routes, own_start)
    scores = dot("gqhe,gkhe->ghqk", split(queries), split(key_rows)) * (1.0 / math.sqrt(HD))
    scores = jnp.where(allowed[:, None], scores, -1e30)
    attn_probs = jax.nn.softmax(scores, axis=-1)
    probs_low = attn_probs.astype(BF16)
    context = dot("ghqk,gkhe->gqhe", probs_low, split(value_rows)).astype(BF16)
    context = context.reshape(seqs * caps, features)
    attended = dot("ne,de->nd", context, full_proj)
    residual = picked + attended
    normed2, inverse2 = normalize(residual, gain2)
    norm_two = normed2.astype(BF16)
    mlp_out = 0.0
    grad_norm_two = 0.0
    grad_mlp = []
    for up, down in zip(full_up, full_down):
        hidden, slope = gelu_parts(dot("nd,df->nf", norm_two, up))
        mlp_out = mlp_out + dot("nf,df->nd", hidden, down)
        grad_pre = (dot("nd,df->nf", branch, down) * slope).astype(BF16)
        grad_norm_two = grad_norm_two + dot("nf,df->nd", grad_pre, up)
        grad_mlp += [
            dot("nd,nf->df", norm_two, grad_pre).astype(BF16),
            dot("nd,nf->df", branch, hidden).astype(BF16),
        ]
    delta = attended + mlp_out
    new_rows = (picked + gating * delta).astype(BF16)
    grad_score = jnp.sum(grad_rows * delta, axis=-1, keepdims=True) * gating * (1.0 - gating)
    grad_mid, grad_gain2 = norm_back(grad_norm_two, residual, inverse2, gain2)
    grad_attended = (grad_delta + grad_mid).astype(BF16)
    grad_proj = dot("nd,ne->de", grad_attended, context).astype(BF16)
    grad_context = split(dot("nd,de->ne", grad_attended, full_proj).astype(BF16))
    grad_probs = dot("gqhe,gkhe->ghqk", grad_context, split(value_rows))
    grad_scores = (
        attn_probs * (grad_probs - jnp.sum(attn_probs * grad_probs, axis=-1, keepdims=True))
    ).astype(BF16)
    join = lambda a: a.astype(BF16).reshape(seqs * caps, features)
    grad_values = join(dot("ghqk,gqhe->gkhe", probs_low, grad_context))
    grad_queries = join(
        dot("ghqk,gkhe->gqhe", grad_scores, split(key_rows)) * (1.0 / math.sqrt(HD))
    )
    grad_keys = join(dot("ghqk,gqhe->gkhe", grad_scores, split(queries)) * (1.0 / math.sqrt(HD)))
    grad_query = dot("nd,ne->de", norm_one, grad_queries).astype(BF16)
    grad_key = dot("nd,ne->de", norm_one, grad_keys).astype(BF16)
    grad_value = dot("nd,ne->de", norm_one, grad_values).astype(BF16)
    grad_norm_one = (
        dot("ne,de->nd", grad_queries, full_query)
        + dot("ne,de->nd", grad_keys, full_key)
        + dot("ne,de->nd", grad_values, full_value)
    )
    grad_picked_norm, grad_gain1 = norm_back(grad_norm_one, picked, inverse1, gain1)
    grad_router = jnp.sum(grad_score * picked, axis=0)
    grad_picked = (grad_rows + grad_mid + grad_picked_norm + grad_score * router).astype(BF16)

    small = jnp.stack([grad_router, grad_gain1, grad_gain2]).reshape(3, 1 << bits, rows)
    small = jnp.pad(small.transpose(1, 0, 2), ((0, 0), (0, 5), (0, 128 - rows)))
    grads = grad_mlp + [grad_proj, grad_query, grad_key, grad_value]
    summed, small = scatter_grads(bits, ranks, grads, small)
    out_up = jnp.concatenate(summed[0 : 2 * parts : 2], axis=1)
    out_down = jnp.concatenate(summed[1 : 2 * parts : 2], axis=1)
    out_proj, out_query, out_key, out_value = summed[2 * parts :]

    def put(base, new):
        placed = dot("scl,scd->sld", chosen, new.reshape(seqs, caps, features)).astype(BF16)
        routed = jnp.sum(chosen.astype(F32), axis=1) > 0
        return jnp.where(routed[:, :, None], placed, base)

    return (
        put(activations, new_rows),
        put(cotangent, grad_picked),
        small[0, :rows],
        small[1, :rows],
        small[2, :rows],
        out_query,
        out_key,
        out_value,
        out_proj,
        out_up,
        out_down,
    )


def solution(mesh):
    both = P(("dp", "tensor"), None, None)
    cut = P("dp", "tensor")
    one = P("dp")
    return jax.shard_map(
        shards,
        mesh=mesh,
        in_specs=(both, P("dp", None), one, one, one, one) + (cut,) * 6 + (both,),
        out_specs=(both, both, one, one, one) + (cut,) * 6,
        check_vma=False,
    )
```

```python
import functools
import math

import jax
import jax.numpy as jnp
from jax import lax
from jax.experimental import pallas as pl
from jax.experimental.pallas import tpu as pltpu
from jax.sharding import PartitionSpec as P

HD = 64
PIC = 256
AHEAD = 2
RING = 8
PAUSE = 2
MESH = pl.DeviceIdType.MESH
ANY = pl.BlockSpec(memory_space=pl.ANY)
VMEM = pl.BlockSpec(memory_space=pltpu.VMEM)
BF16 = jnp.bfloat16
F32 = jnp.float32

inv_root_two = 0.7071067811865476
inv_root_two_pi = 0.3989422804014327


def bit_of(value, bit):
    return lax.rem(lax.div(value, 1 << bit), 2)


def flipped(value, bit):
    return value + (1 - 2 * bit_of(value, bit)) * (1 << bit)


def cleared(value, bits):
    for bit in bits:
        value = value - bit_of(value, bit) * (1 << bit)
    return value


def spread(step, bits):
    value = 0
    for place, bit in enumerate(bits):
        value = value + lax.rem(lax.div(step, 1 << place), 2) * (1 << bit)
    return value


def each(count, body):
    if count <= 4:
        for step in range(count):
            body(jnp.int32(step))
    else:
        lax.fori_loop(0, count, lambda step, _: body(step), None)


def repeat(count, body):
    def step(index, _):
        body(index)

    lax.fori_loop(0, count, step, None)


def span(index, size):
    return pl.ds(pl.multiple_of(index * size, size), size)


def orders(bits):
    return (tuple(range(bits - 1, 0, -1)), tuple(range(1, bits)))


def remote(src, dst, send, recv, where):
    return pltpu.make_async_remote_copy(
        src_ref=src, dst_ref=dst, send_sem=send, recv_sem=recv, device_id=where, device_id_type=MESH
    )


def contract(left, right, axis_left, axis_right):
    return lax.dot_general(
        left, right, (((axis_left,), (axis_right,)), ((), ())), preferred_element_type=F32
    )


def layer_kernel(
    bits,
    ranks,
    chunks,
    shards,
    vec,
    picked,
    grad_rows,
    allowed,
    sums,
    vec_sum,
    new_rows,
    new_grads,
    held,
    from_core,
    from_z,
    vecs,
    grad_vecs,
    vec_path,
    vec_z,
    params,
    gates,
    scores_of,
    norm_one,
    qkv,
    context,
    attended,
    norm_two,
    norm_two_t,
    branch,
    branch_t,
    hidden,
    grad_pre,
    mlp,
    grad_two,
    send_z,
    recv_z,
    send_p,
    recv_p,
    send_c,
    recv_c,
    send_v,
    recv_v,
    local,
    out_c,
    in_c,
    out_p,
    in_p,
    out_z,
    in_z,
    out_v,
    in_v,
    *from_path,
):
    me, rank = lax.axis_index("dp"), lax.axis_index("tensor")
    _, rows, width = shards.shape
    count, full = picked.shape
    seqs, caps, _ = allowed.shape
    half = full // 2
    seat, pair = bit_of(me, 0), lax.div(me, 2)
    pairs = 1 << (bits - 1)
    paths = orders(bits)
    back_paths = tuple(tuple(bit - 1 for bit in order[::-1]) for order in paths)
    tile = 32
    block = 256
    blocks = full // block

    barrier = pltpu.get_barrier_semaphore()
    for bit in range(bits):
        pl.semaphore_signal(barrier, 1, device_id=(flipped(me, bit), rank), device_id_type=MESH)
    for hop in range(1, ranks):
        pl.semaphore_signal(
            barrier, 1, device_id=(me, lax.rem(rank + hop, ranks)), device_id_type=MESH
        )
    pl.semaphore_wait(barrier, bits + ranks - 1)

    mine = span(me, rows)
    columns = span(rank, width)

    def keep_own(chunk):
        return pltpu.make_async_copy(
            shards.at[chunk], held.at[chunk, mine, columns], local.at[chunk]
        )

    def bulk(chunk, depth, breadth):
        return held.at[chunk, pl.ds(0, depth), pl.ds(0, breadth)]

    def z_copy(chunk):
        part = bulk(chunk, rows, width * (ranks - 1))
        return remote(part, part, send_z.at[chunk], recv_z.at[chunk], (me, rank))

    def send_path(chunk, colour, stage):
        order = paths[colour]
        other = (flipped(me, order[stage]), rank)

        def send(step):
            index = cleared(me, order[:stage]) + spread(step, order[:stage])
            part = held.at[chunk, span(index, rows), pl.ds(colour * half, half)]
            remote(
                part,
                part,
                send_p.at[chunk, colour, stage],
                recv_p.at[chunk, colour, stage],
                other,
            ).start()

        each(1 << stage, send)

    def path_copy(chunk, colour, stage):
        part = bulk(chunk, rows << stage, half)
        return remote(
            part,
            part,
            send_p.at[chunk, colour, stage],
            recv_p.at[chunk, colour, stage],
            (me, rank),
        )

    def send_core(chunk):
        other = (flipped(me, 0), rank)

        def send(step):
            part = held.at[chunk, span(2 * step + seat, rows)]
            remote(part, part, send_c.at[chunk], recv_c.at[chunk], other).start()

        each(pairs, send)

    def core_copy(chunk):
        part = bulk(chunk, rows << (bits - 1), full)
        return remote(part, part, send_c.at[chunk], recv_c.at[chunk], (me, rank))

    def all_sent(chunk):
        for colour in range(2):
            for stage in range(bits - 1):
                path_copy(chunk, colour, stage).wait_send()
        core_copy(chunk).wait_send()

    def gather_stage(chunk, stage):
        if stage == 0:
            keep_own(chunk).wait()
            z_copy(chunk).wait_recv()
        elif stage < bits:
            for colour in range(2):
                path_copy(chunk, colour, stage - 1).wait_recv()
        else:
            core_copy(chunk).wait_recv()
        if stage < bits - 1:
            for colour in range(2):
                send_path(chunk, colour, stage)
        elif stage == bits - 1:
            send_core(chunk)

    def turn(item):
        return jnp.where(item < chunks - 4, item, item - PAUSE)

    def slot(item):
        return jnp.where(item < chunks - 4, item + 4, item - PAUSE - chunks + 4)

    def give_core(item):
        def send(step):
            remote(
                held.at[slot(item), span(2 * step + 1 - seat, rows)],
                from_core.at[lax.rem(turn(item), RING), step],
                out_c.at[turn(item)],
                in_c.at[turn(item)],
                (flipped(me, 0), rank),
            ).start()

        each(pairs, send)

    def given_core(item):
        part = from_core.at[lax.rem(turn(item), RING)]
        return remote(part, part, out_c.at[turn(item)], in_c.at[turn(item)], (me, rank))

    def add_to(item, index, where, source):
        step = min(rows, tile)
        for start in range(0, rows, step):
            place = pl.ds(pl.multiple_of((2 * index + seat) * rows, rows) + start, step)
            here = held.at[slot(item), place, where]
            here[...] = (
                here[...].astype(F32) + source[pl.ds(start, step)].astype(F32)
            ).astype(BF16)

    def add_core(item):
        repeat(
            pairs,
            lambda step: add_to(
                item, step, pl.ds(0, full), from_core.at[lax.rem(turn(item), RING), step]
            ),
        )

    def members(stage, order, step, kept):
        bit, later = order[stage], order[stage + 1 :]
        index = pair if kept else flipped(pair, bit)
        return cleared(index, later) + spread(step, later)

    def give_path(item, colour, stage):
        order = back_paths[colour]
        other = (2 * flipped(pair, order[stage]) + seat, rank)

        def send(step):
            index = members(stage, order, step, False)
            remote(
                held.at[
                    slot(item), span(2 * index + seat, rows), pl.ds(colour * half, half)
                ],
                from_path[stage].at[turn(item), colour, step],
                out_p.at[turn(item), colour, stage],
                in_p.at[turn(item), colour, stage],
                other,
            ).start()

        each(1 << (len(order) - stage - 1), send)

    def given_path(item, colour, stage):
        part = from_path[stage].at[turn(item), colour]
        return remote(
            part,
            part,
            out_p.at[turn(item), colour, stage],
            in_p.at[turn(item), colour, stage],
            (me, rank),
        )

    def add_path(item, colour, stage):
        order = back_paths[colour]
        repeat(
            1 << (len(order) - stage - 1),
            lambda step: add_to(
                item,
                members(stage, order, step, True),
                pl.ds(colour * half, half),
                from_path[stage].at[turn(item), colour, step],
            ),
        )

    def give_across(item):
        for hop in range(1, ranks):
            to = lax.rem(rank + hop, ranks)
            remote(
                held.at[slot(item), mine, span(to, width)],
                from_z.at[turn(item), hop - 1],
                out_z.at[turn(item)],
                in_z.at[turn(item)],
                (me, to),
            ).start()

    def given_across(item):
        part = from_z.at[turn(item)]
        return remote(part, part, out_z.at[turn(item)], in_z.at[turn(item)], (me, rank))

    def finish(item):
        total = held[slot(item), mine, columns].astype(F32)
        for hop in range(1, ranks):
            total = total + from_z[turn(item), hop - 1].astype(F32)
        sums[slot(item)] = total

    def scatter_stage(item, stage):
        if stage == 1:
            given_core(item).wait_recv()
            add_core(item)
        elif 1 < stage <= bits:
            for colour in range(2):
                given_path(item, colour, stage - 2).wait_recv()
                add_path(item, colour, stage - 2)
        elif stage == bits + 1:
            given_across(item).wait_recv()
            finish(item)
        if stage == 0:
            give_core(item)
        elif stage < bits:
            for colour in range(2):
                give_path(item, colour, stage - 1)
        elif stage == bits:
            give_across(item)

    def vec_gather():
        path = tuple(range(bits - 1, -1, -1))
        for stage, bit in enumerate(path):
            other = (flipped(me, bit), rank)

            def send(step, stage=stage, other=other):
                index = cleared(me, path[:stage]) + spread(step, path[:stage])
                remote(
                    vecs.at[index], vecs.at[index], send_v.at[stage], recv_v.at[stage], other
                ).start()

            each(1 << stage, send)
            part = vecs.at[pl.ds(0, 1 << stage)]
            remote(part, part, send_v.at[stage], recv_v.at[stage], other).wait()
        params[...] = jnp.zeros_like(params)
        lane = lax.broadcasted_iota(jnp.int32, (128, full), 0)
        column = lax.broadcasted_iota(jnp.int32, (128, full), 1)

        def place(index):
            chosen = ((lane < rows) & (column == index * rows + lane)).astype(F32).astype(BF16)
            params[...] += contract(vecs[index].astype(BF16), chosen, 1, 0)

        repeat(1 << bits, place)

    vec_path_of = tuple(range(bits))

    def vec_stage(stage):
        if stage > 0:
            earlier = vec_path_of[stage:]
            amount = 1 << len(earlier)
            part = vec_path.at[pl.ds(amount - 1, amount)]
            remote(part, part, out_v.at[stage - 1], in_v.at[stage - 1], (me, rank)).wait()

            def add(step):
                index = cleared(me, earlier) + spread(step, earlier)
                grad_vecs[index] = grad_vecs[index] + vec_path[amount - 1 + step]

            repeat(amount, add)
        if stage < bits:
            bit, later = vec_path_of[stage], vec_path_of[stage + 1 :]
            amount = 1 << len(later)

            def send(step):
                index = cleared(flipped(me, bit), later) + spread(step, later)
                remote(
                    grad_vecs.at[index],
                    vec_path.at[amount - 1 + step],
                    out_v.at[stage],
                    in_v.at[stage],
                    (flipped(me, bit), rank),
                ).start()

            each(amount, send)
        else:
            for hop in range(1, ranks):
                to = (me, lax.rem(rank + hop, ranks))
                remote(
                    grad_vecs.at[me], vec_z.at[hop - 1], out_v.at[bits], in_v.at[bits], to
                ).start()

    def vec_finish():
        remote(vec_z, vec_z, out_v.at[bits], in_v.at[bits], (me, rank)).wait()
        total = grad_vecs[me]
        for hop in range(1, ranks):
            total = total + vec_z[hop - 1]
        vec_sum[...] = total

    def router():
        return params[0:1, :]

    def gain_one():
        return params[1:2, :]

    def gain_two():
        return params[2:3, :]

    def by_rows(body):
        repeat(count // tile, lambda index: body(span(index, tile)))

    def by_blocks(body):
        repeat(blocks, lambda index: body(span(index, block)))

    def inverse_of(values):
        return lax.rsqrt(jnp.mean(values * values, axis=-1, keepdims=True) + 1e-06)

    def wide(values):
        return jnp.broadcast_to(values, (values.shape[0], 128))

    def transpose_to(target, source):
        for start in range(0, full, 128):
            part = source[:, start : start + 128].astype(F32)
            target[start : start + 128, :] = part.T.astype(BF16)

    def prepare():
        def body(part):
            values = picked[part].astype(F32)
            logit = jnp.sum(values * router(), axis=-1, keepdims=True)
            gate = 1.0 / (1.0 + jnp.exp(-logit))
            gates[part] = wide(gate)
            norm_one[part] = (values * inverse_of(values) * gain_one()).astype(BF16)
            branch[part] = (gate * grad_rows[part].astype(F32)).astype(BF16)

        by_rows(body)
        transpose_to(branch_t, branch)

    def project(which):
        def body(part):
            qkv[which, :, part] = contract(norm_one[...], held[which, :, part], 1, 0).astype(BF16)

        by_blocks(body)

    lanes = lax.broadcasted_iota(jnp.int32, (1, 2 * HD), 1)

    def own_lanes(values, head):
        inside = (lanes < HD) if head == 0 else (lanes >= HD)
        return jnp.where(inside, values, jnp.zeros_like(values))

    def probabilities(seq, queries, keys, head):
        scores = contract(own_lanes(queries, head), keys, 1, 1) * (1.0 / math.sqrt(HD))
        scores = jnp.where(allowed[seq] > 0, scores, -1e30)
        powers = jnp.exp(scores - jnp.max(scores, axis=-1, keepdims=True))
        return powers / jnp.sum(powers, axis=-1, keepdims=True)

    def attend():
        def body(index):
            part = span(index, 2 * HD)
            for seq in range(seqs):
                place = pl.ds(seq * caps, caps)
                queries, keys = qkv[0, place, part], qkv[1, place, part]
                values = qkv[2, place, part]
                total = 0.0
                for head in range(2):
                    probs = probabilities(seq, queries, keys, head).astype(BF16)
                    total = total + contract(probs, own_lanes(values, head), 1, 0)
                context[place, part] = total.astype(BF16)

        repeat(full // (2 * HD), body)

    def leave_attention():
        def body(part):
            attended[:, part] = contract(context[...], held[3, part, :], 1, 1)

        by_blocks(body)

        def rest(part):
            values = picked[part].astype(F32) + attended[part]
            norm_two[part] = (values * inverse_of(values) * gain_two()).astype(BF16)
            mlp[part] = jnp.zeros((tile, full), F32)
            grad_two[part] = jnp.zeros((tile, full), F32)

        by_rows(rest)
        transpose_to(norm_two_t, norm_two)

    def feed_forward(up, down):
        def units(part):
            pre = contract(norm_two[...], held[up, :, part], 1, 0)
            bell = 0.5 * (1.0 + lax.erf(pre * inv_root_two))
            slope = bell + pre * jnp.exp(-0.5 * pre * pre) * inv_root_two_pi
            hidden[:, part] = (pre * bell).astype(BF16)
            grad_hidden = contract(branch[...], held[down, :, part], 1, 0)
            grad_pre[:, part] = (grad_hidden * slope).astype(BF16)

        by_blocks(units)

        def outputs(part):
            mlp[:, part] += contract(hidden[...], held[down, part, :], 1, 1)
            grad_two[:, part] += contract(grad_pre[...], held[up, part, :], 1, 1)

        by_blocks(outputs)
        all_sent(up)
        all_sent(down)

        def gradients(part):
            held[down, :, part] = contract(branch_t[...], hidden[:, part], 1, 0).astype(BF16)
            held[up, :, part] = contract(norm_two_t[...], grad_pre[:, part], 1, 0).astype(BF16)

        by_blocks(gradients)

    small = params

    def enter_back():
        grad_attended, grad_attended_t, grad_context = norm_two, norm_two_t, hidden
        small[3:6, :] = jnp.zeros((3, full), F32)

        def body(part):
            values = picked[part].astype(F32)
            gate = gates[part, 0:1]
            delta = attended[part] + mlp[part]
            new_rows[part] = (values + gate * delta).astype(BF16)
            rows_in = grad_rows[part].astype(F32)
            score = jnp.sum(rows_in * delta, axis=-1, keepdims=True) * gate * (1.0 - gate)
            scores_of[part] = wide(score)
            small[3:4, :] += jnp.sum(score * values, axis=0, keepdims=True)
            residual = values + attended[part]
            inverse = inverse_of(residual)
            grad = grad_two[part]
            small[5:6, :] += jnp.sum(grad * residual * inverse, axis=0, keepdims=True)
            scaled = grad * gain_two()
            mean = jnp.mean(scaled * residual, axis=-1, keepdims=True)
            grad_mid = inverse * scaled - residual * (inverse * inverse * inverse * mean)
            grad_two[part] = grad_mid
            grad_attended[part] = (gate * rows_in + grad_mid).astype(BF16)

        by_rows(body)
        transpose_to(grad_attended_t, grad_attended)

        def through(part):
            grad_context[:, part] = contract(grad_attended[...], held[3, :, part], 1, 0).astype(BF16)

        by_blocks(through)
        for chunk in range(4):
            all_sent(chunk)

        def weights(part):
            held[3, :, part] = contract(grad_attended_t[...], context[:, part], 1, 0).astype(BF16)

        by_blocks(weights)

    def attend_back():
        grad_context = hidden
        grads = (branch, grad_pre, context)

        def body(index):
            part = span(index, 2 * HD)
            for seq in range(seqs):
                place = pl.ds(seq * caps, caps)
                queries, keys = qkv[0, place, part], qkv[1, place, part]
                values, grad = qkv[2, place, part], grad_context[place, part]
                grad_q, grad_k, grad_v = 0.0, 0.0, 0.0
                for head in range(2):
                    probs = probabilities(seq, queries, keys, head)
                    grad_probs = contract(own_lanes(grad, head), values, 1, 1)
                    inner = jnp.sum(probs * grad_probs, axis=-1, keepdims=True)
                    grad_scores = (probs * (grad_probs - inner)).astype(BF16)
                    low = probs.astype(BF16)
                    grad_v = grad_v + contract(low, own_lanes(grad, head), 0, 0)
                    grad_q = grad_q + contract(grad_scores, own_lanes(keys, head), 1, 0)
                    grad_k = grad_k + contract(grad_scores, own_lanes(queries, head), 0, 0)
                scale = 1.0 / math.sqrt(HD)
                grads[0][place, part] = (grad_q * scale).astype(BF16)
                grads[1][place, part] = (grad_k * scale).astype(BF16)
                grads[2][place, part] = grad_v.astype(BF16)

        repeat(full // (2 * HD), body)

    def leave_back():
        grads = (branch, grad_pre, context)
        grad_one, norm_one_t = mlp, branch_t

        def through(part):
            total = contract(grads[0][...], held[0, part, :], 1, 1)
            for which in (1, 2):
                total = total + contract(grads[which][...], held[which, part, :], 1, 1)
            grad_one[:, part] = total

        by_blocks(through)
        transpose_to(norm_one_t, norm_one)

        def weights(part):
            for which in range(3):
                held[which, :, part] = contract(norm_one_t[...], grads[which][:, part], 1, 0).astype(
                    BF16
                )

        by_blocks(weights)

        def body(part):
            values = picked[part].astype(F32)
            inverse = inverse_of(values)
            grad = grad_one[part]
            small[4:5, :] += jnp.sum(grad * values * inverse, axis=0, keepdims=True)
            scaled = grad * gain_one()
            mean = jnp.mean(scaled * values, axis=-1, keepdims=True)
            grad_norm = inverse * scaled - values * (inverse * inverse * inverse * mean)
            score = scores_of[part, 0:1]
            total = grad_rows[part].astype(F32) + grad_two[part] + grad_norm + score * router()
            new_grads[part] = total.astype(BF16)

        by_rows(body)
        own = small[...]
        if rows == 128:
            for index in range(1 << bits):
                grad_vecs[index] = own[:, index * rows : (index + 1) * rows]
        else:
            column = lax.broadcasted_iota(jnp.int32, (full, 128), 0)
            lane = lax.broadcasted_iota(jnp.int32, (full, 128), 1)

            def place(index):
                chosen = ((lane < rows) & (column == index * rows + lane)).astype(F32)
                grad_vecs[index] = jnp.dot(
                    own, chosen, precision=lax.Precision.HIGHEST, preferred_element_type=F32
                )

            repeat(1 << bits, place)

    def start(chunk):
        keep_own(chunk).start()
        for hop in range(1, ranks):
            remote(
                shards.at[chunk],
                held.at[chunk, mine, columns],
                send_z.at[chunk],
                recv_z.at[chunk],
                (me, lax.rem(rank + hop, ranks)),
            ).start()

    keep_vec = pltpu.make_async_copy(vec, vecs.at[me], local.at[chunks])
    keep_vec.start()
    repeat(chunks, start)
    keep_vec.wait()
    vec_gather()
    prepare()
    lead = AHEAD * bits
    first = lead + 5
    items = chunks + PAUSE
    vec_first = lead + chunks + PAUSE + 1

    def tick(now, _):
        for stage in range(bits, -1, -1):
            chunk = now - AHEAD * stage

            @pl.when((chunk >= 0) & (chunk < chunks))
            def _(chunk=chunk, stage=stage):
                gather_stage(chunk, stage)

        whole = now - lead
        pl.when((whole >= 0) & (whole < 3))(lambda: project(whole))
        pl.when(whole == 2)(attend)
        pl.when(whole == 3)(leave_attention)
        pl.when((whole >= 5) & (whole < chunks) & (lax.rem(whole, 2) == 1))(
            lambda: feed_forward(whole - 1, whole)
        )
        for stage in range(bits + 1, -1, -1):
            item = now - first - AHEAD * stage
            inside = (item >= 0) & (item < items)
            paused = (item >= chunks - 4) & (item < chunks - 4 + PAUSE)

            @pl.when(inside & jnp.logical_not(paused))
            def _(item=item, stage=stage):
                scatter_stage(item, stage)

        pl.when(whole == chunks)(enter_back)
        pl.when(whole == chunks + 1)(attend_back)
        pl.when(whole == chunks + 2)(leave_back)
        for stage in range(bits + 1):
            pl.when(now == vec_first + AHEAD * stage)(functools.partial(vec_stage, stage))
        pl.when(now == vec_first + AHEAD * (bits + 1))(vec_finish)

    last = max(first + items - 1 + AHEAD * (bits + 1), vec_first + AHEAD * (bits + 1))
    lax.fori_loop(0, last + 1, tick, None)

    def drain(chunk):
        z_copy(chunk).wait_send()
        item = jnp.where(chunk < chunks - 4, chunk, chunk + PAUSE)
        given_core(item).wait_send()
        for colour in range(2):
            for stage in range(bits - 1):
                given_path(item, colour, stage).wait_send()
        given_across(item).wait_send()

    repeat(chunks, drain)


def run_layer(bits, ranks, shards, vec, picked, grad_rows, allowed):
    chunks, rows, width = shards.shape
    depth, breadth, pairs = rows << bits, width * ranks, 1 << (bits - 1)
    count, full = picked.shape
    dma = pltpu.SemaphoreType.DMA
    low = pltpu.VMEM((count, full), BF16)
    turned = pltpu.VMEM((full, count), BF16)
    high = pltpu.VMEM((count, full), F32)
    return pl.pallas_call(
        functools.partial(layer_kernel, bits, ranks, chunks),
        out_shape=[
            jax.ShapeDtypeStruct((chunks, rows, width), F32),
            jax.ShapeDtypeStruct((8, 128), F32),
            jax.ShapeDtypeStruct((count, full), BF16),
            jax.ShapeDtypeStruct((count, full), BF16),
        ],
        in_specs=[ANY] + [VMEM] * 4,
        out_specs=[VMEM] * 4,
        scratch_shapes=[
            pltpu.VMEM((chunks, depth, breadth), BF16),
            pltpu.VMEM((RING, pairs, rows, breadth), BF16),
            pltpu.VMEM((chunks, ranks - 1, rows, width), BF16),
            pltpu.VMEM((1 << bits, 8, 128), F32),
            pltpu.VMEM((1 << bits, 8, 128), F32),
            pltpu.VMEM((1 << bits, 8, 128), F32),
            pltpu.VMEM((ranks - 1, 8, 128), F32),
            pltpu.VMEM((8, full), F32),
            pltpu.VMEM((count, 128), F32),
            pltpu.VMEM((count, 128), F32),
            low,
            pltpu.VMEM((3, count, full), BF16),
            low,
            high,
            low,
            turned,
            low,
            turned,
            low,
            low,
            high,
            high,
            dma((chunks,)),
            dma((chunks,)),
            dma((chunks, 2, bits - 1)),
            dma((chunks, 2, bits - 1)),
            dma((chunks,)),
            dma((chunks,)),
            dma((bits,)),
            dma((bits,)),
            dma((chunks + 1,)),
            dma((chunks,)),
            dma((chunks,)),
            dma((chunks, 2, bits - 1)),
            dma((chunks, 2, bits - 1)),
            dma((chunks,)),
            dma((chunks,)),
            dma((bits + 1,)),
            dma((bits + 1,)),
            *[
                pltpu.VMEM((chunks, 2, pairs >> (stage + 1), rows, breadth // 2), BF16)
                for stage in range(bits - 1)
            ],
        ],
        compiler_params=pltpu.CompilerParams(
            collective_id=1, has_side_effects=True, vmem_limit_bytes=67043328
        ),
        name="layer_kernel",
    )(shards, vec, picked, grad_rows, allowed)


def span_mask(positions, starts):
    later = positions[:, None, :] <= positions[:, :, None]
    begin = starts[:, None]
    inside = (positions >= begin) & (positions < begin + PIC)
    return later | inside[:, :, None] & inside[:, None, :]


def dot(form, left, right):
    return jnp.einsum(form, left, right, preferred_element_type=F32)


def shards(
    activations,
    routes,
    pic_start,
    router_w,
    gain_attn,
    gain_mlp,
    w_query,
    w_key,
    w_value,
    w_proj,
    w_up,
    w_down,
    cotangent,
):
    seqs, length, features = activations.shape
    ranks = lax.axis_size("tensor")
    bits = lax.axis_size("dp").bit_length() - 1
    rank = lax.axis_index("tensor")
    rows, width = w_query.shape
    parts = w_up.shape[1] // width
    own_routes = lax.dynamic_slice_in_dim(routes, rank * seqs, seqs, 0)
    own_start = lax.dynamic_slice_in_dim(pic_start, rank * seqs, seqs, 0)
    caps = routes.shape[1]

    vec = jnp.stack([router_w, gain_attn, gain_mlp]).astype(F32)
    vec = jnp.pad(vec, ((0, 5), (0, 128 - rows)))
    pieces = [w_query, w_key, w_value, w_proj]
    for part in range(parts):
        columns = slice(part * width, (part + 1) * width)
        pieces += [w_up[:, columns], w_down[:, columns]]
    chosen = (own_routes[:, :, None] == jnp.arange(length)[None, None, :]).astype(BF16)
    picked = dot("scl,sld->scd", chosen, activations).astype(BF16)
    grad_rows = dot("scl,sld->scd", chosen, cotangent).astype(BF16)
    sums, small, new_rows, new_grads = run_layer(
        bits,
        ranks,
        jnp.stack(pieces),
        vec,
        picked.reshape(seqs * caps, features),
        grad_rows.reshape(seqs * caps, features),
        span_mask(own_routes, own_start).astype(F32),
    )

    def put(base, new):
        placed = dot("scl,scd->sld", chosen, new.reshape(seqs, caps, features)).astype(BF16)
        routed = jnp.sum(chosen.astype(F32), axis=1) > 0
        return jnp.where(routed[:, :, None], placed, base)

    def side_by_side(first):
        return jnp.concatenate([sums[first + 2 * part] for part in range(parts)], axis=1)

    return (
        put(activations, new_rows),
        put(cotangent, new_grads),
        small[3, :rows],
        small[4, :rows],
        small[5, :rows],
        sums[0],
        sums[1],
        sums[2],
        sums[3],
        side_by_side(4),
        side_by_side(5),
    )


def solution(mesh):
    both = P(("dp", "tensor"), None, None)
    cut = P("dp", "tensor")
    one = P("dp")
    return jax.shard_map(
        shards,
        mesh=mesh,
        in_specs=(both, P("dp", None), one, one, one, one) + (cut,) * 6 + (both,),
        out_specs=(both, both, one, one, one) + (cut,) * 6,
        check_vma=False,
    )
```

```python
import functools
import math

import jax
import jax.numpy as jnp
from jax import lax
from jax.experimental import pallas as pl
from jax.experimental.pallas import tpu as pltpu
from jax.sharding import PartitionSpec as P

HD = 64
PIC = 256
AHEAD = 2
RING = 8
PAUSE = 2
MESH = pl.DeviceIdType.MESH
ANY = pl.BlockSpec(memory_space=pl.ANY)
VMEM = pl.BlockSpec(memory_space=pltpu.VMEM)
BF16 = jnp.bfloat16
F32 = jnp.float32

inv_root_two = 0.7071067811865476
inv_root_two_pi = 0.3989422804014327


def bit_of(value, bit):
    return lax.rem(lax.div(value, 1 << bit), 2)


def flipped(value, bit):
    return value + (1 - 2 * bit_of(value, bit)) * (1 << bit)


def cleared(value, bits):
    for bit in bits:
        value = value - bit_of(value, bit) * (1 << bit)
    return value


def spread(step, bits):
    value = 0
    for place, bit in enumerate(bits):
        value = value + lax.rem(lax.div(step, 1 << place), 2) * (1 << bit)
    return value


def each(count, body):
    if count <= 4:
        for step in range(count):
            body(jnp.int32(step))
    else:
        lax.fori_loop(0, count, lambda step, _: body(step), None)


def repeat(count, body):
    def step(index, _):
        body(index)

    lax.fori_loop(0, count, step, None)


def span(index, size):
    return pl.ds(pl.multiple_of(index * size, size), size)


def orders(bits):
    return (tuple(range(bits - 1, 0, -1)), tuple(range(1, bits)))


def remote(src, dst, send, recv, where):
    return pltpu.make_async_remote_copy(
        src_ref=src, dst_ref=dst, send_sem=send, recv_sem=recv, device_id=where, device_id_type=MESH
    )


def contract(left, right, axis_left, axis_right):
    return lax.dot_general(
        left, right, (((axis_left,), (axis_right,)), ((), ())), preferred_element_type=F32
    )


def layer_kernel(
    bits,
    ranks,
    chunks,
    parts,
    *refs,
):
    shards = refs[:6]
    (
    vec,
    routes,
    pic_start,
    activations,
    cotangent,
    sums,
    vec_sum,
    new_rows,
    new_grads,
    picked,
    grad_rows,
    allowed,
    held,
    from_core,
    from_z,
    vecs,
    grad_vecs,
    vec_path,
    vec_z,
    params,
    gates,
    scores_of,
    norm_one,
    qkv,
    context,
    attended,
    norm_two,
    norm_two_t,
    branch,
    branch_t,
    hidden,
    grad_pre,
    mlp,
    grad_two,
    send_z,
    recv_z,
    send_p,
    recv_p,
    send_c,
    recv_c,
    send_v,
    recv_v,
    local,
    out_c,
    in_c,
    out_p,
    in_p,
    out_z,
    in_z,
    out_v,
    in_v,
    fetched,
    *from_path,
    ) = refs[6:]
    me, rank = lax.axis_index("dp"), lax.axis_index("tensor")
    rows, width = shards[0].shape
    count, full = picked.shape
    length = activations.shape[1]
    seqs, caps, _ = allowed.shape
    half = full // 2
    seat, pair = bit_of(me, 0), lax.div(me, 2)
    pairs = 1 << (bits - 1)
    paths = orders(bits)
    back_paths = tuple(tuple(bit - 1 for bit in order[::-1]) for order in paths)
    tile = 32
    block = 256
    blocks = full // block

    barrier = pltpu.get_barrier_semaphore()
    for bit in range(bits):
        pl.semaphore_signal(barrier, 1, device_id=(flipped(me, bit), rank), device_id_type=MESH)
    for hop in range(1, ranks):
        pl.semaphore_signal(
            barrier, 1, device_id=(me, lax.rem(rank + hop, ranks)), device_id_type=MESH
        )
    pl.semaphore_wait(barrier, bits + ranks - 1)

    mine = span(me, rows)
    columns = span(rank, width)

    def shard(chunk):
        if chunk < 4:
            return shards[chunk]
        return shards[4 + chunk % 2].at[:, pl.ds((chunk - 4) // 2 * width, width)]

    def keep_own(chunk, source=shards[0]):
        return pltpu.make_async_copy(source, held.at[chunk, mine, columns], local.at[chunk])

    def bulk(chunk, depth, breadth):
        return held.at[chunk, pl.ds(0, depth), pl.ds(0, breadth)]

    def z_copy(chunk):
        part = bulk(chunk, rows, width * (ranks - 1))
        return remote(part, part, send_z.at[chunk], recv_z.at[chunk], (me, rank))

    def send_path(chunk, colour, stage):
        order = paths[colour]
        other = (flipped(me, order[stage]), rank)

        def send(step):
            index = cleared(me, order[:stage]) + spread(step, order[:stage])
            part = held.at[chunk, span(index, rows), pl.ds(colour * half, half)]
            remote(
                part,
                part,
                send_p.at[chunk, colour, stage],
                recv_p.at[chunk, colour, stage],
                other,
            ).start()

        each(1 << stage, send)

    def path_copy(chunk, colour, stage):
        part = bulk(chunk, rows << stage, half)
        return remote(
            part,
            part,
            send_p.at[chunk, colour, stage],
            recv_p.at[chunk, colour, stage],
            (me, rank),
        )

    def send_core(chunk):
        other = (flipped(me, 0), rank)

        def send(step):
            part = held.at[chunk, span(2 * step + seat, rows)]
            remote(part, part, send_c.at[chunk], recv_c.at[chunk], other).start()

        each(pairs, send)

    def core_copy(chunk):
        part = bulk(chunk, rows << (bits - 1), full)
        return remote(part, part, send_c.at[chunk], recv_c.at[chunk], (me, rank))

    def all_sent(chunk):
        for colour in range(2):
            for stage in range(bits - 1):
                path_copy(chunk, colour, stage).wait_send()
        core_copy(chunk).wait_send()

    def gather_stage(chunk, stage):
        if stage == 0:
            keep_own(chunk).wait()
            z_copy(chunk).wait_recv()
        elif stage < bits:
            for colour in range(2):
                path_copy(chunk, colour, stage - 1).wait_recv()
        else:
            core_copy(chunk).wait_recv()
        if stage < bits - 1:
            for colour in range(2):
                send_path(chunk, colour, stage)
        elif stage == bits - 1:
            send_core(chunk)

    def turn(item):
        return jnp.where(item < chunks - 4, item, item - PAUSE)

    def slot(item):
        return jnp.where(item < chunks - 4, item + 4, item - PAUSE - chunks + 4)

    def give_core(item):
        def send(step):
            remote(
                held.at[slot(item), span(2 * step + 1 - seat, rows)],
                from_core.at[lax.rem(turn(item), RING), step],
                out_c.at[turn(item)],
                in_c.at[turn(item)],
                (flipped(me, 0), rank),
            ).start()

        each(pairs, send)

    def given_core(item):
        part = from_core.at[lax.rem(turn(item), RING)]
        return remote(part, part, out_c.at[turn(item)], in_c.at[turn(item)], (me, rank))

    def add_to(item, index, where, source):
        step = min(rows, tile)
        for start in range(0, rows, step):
            place = pl.ds(pl.multiple_of((2 * index + seat) * rows, rows) + start, step)
            here = held.at[slot(item), place, where]
            here[...] = (
                here[...].astype(F32) + source[pl.ds(start, step)].astype(F32)
            ).astype(BF16)

    def add_core(item):
        repeat(
            pairs,
            lambda step: add_to(
                item, step, pl.ds(0, full), from_core.at[lax.rem(turn(item), RING), step]
            ),
        )

    def members(stage, order, step, kept):
        bit, later = order[stage], order[stage + 1 :]
        index = pair if kept else flipped(pair, bit)
        return cleared(index, later) + spread(step, later)

    def give_path(item, colour, stage):
        order = back_paths[colour]
        other = (2 * flipped(pair, order[stage]) + seat, rank)

        def send(step):
            index = members(stage, order, step, False)
            remote(
                held.at[
                    slot(item), span(2 * index + seat, rows), pl.ds(colour * half, half)
                ],
                from_path[stage].at[turn(item), colour, step],
                out_p.at[turn(item), colour, stage],
                in_p.at[turn(item), colour, stage],
                other,
            ).start()

        each(1 << (len(order) - stage - 1), send)

    def given_path(item, colour, stage):
        part = from_path[stage].at[turn(item), colour]
        return remote(
            part,
            part,
            out_p.at[turn(item), colour, stage],
            in_p.at[turn(item), colour, stage],
            (me, rank),
        )

    def add_path(item, colour, stage):
        order = back_paths[colour]
        repeat(
            1 << (len(order) - stage - 1),
            lambda step: add_to(
                item,
                members(stage, order, step, True),
                pl.ds(colour * half, half),
                from_path[stage].at[turn(item), colour, step],
            ),
        )

    def give_across(item):
        for hop in range(1, ranks):
            to = lax.rem(rank + hop, ranks)
            remote(
                held.at[slot(item), mine, span(to, width)],
                from_z.at[turn(item), hop - 1],
                out_z.at[turn(item)],
                in_z.at[turn(item)],
                (me, to),
            ).start()

    def given_across(item):
        part = from_z.at[turn(item)]
        return remote(part, part, out_z.at[turn(item)], in_z.at[turn(item)], (me, rank))

    def finish(item):
        total = held[slot(item), mine, columns].astype(F32)
        for hop in range(1, ranks):
            total = total + from_z[turn(item), hop - 1].astype(F32)
        sums[slot(item)] = total

    def scatter_stage(item, stage):
        if stage == 1:
            given_core(item).wait_recv()
            add_core(item)
        elif 1 < stage <= bits:
            for colour in range(2):
                given_path(item, colour, stage - 2).wait_recv()
                add_path(item, colour, stage - 2)
        elif stage == bits + 1:
            given_across(item).wait_recv()
            finish(item)
        if stage == 0:
            give_core(item)
        elif stage < bits:
            for colour in range(2):
                give_path(item, colour, stage - 1)
        elif stage == bits:
            give_across(item)

    def vec_gather():
        path = tuple(range(bits - 1, -1, -1))
        for stage, bit in enumerate(path):
            other = (flipped(me, bit), rank)

            def send(step, stage=stage, other=other):
                index = cleared(me, path[:stage]) + spread(step, path[:stage])
                remote(
                    vecs.at[index], vecs.at[index], send_v.at[stage], recv_v.at[stage], other
                ).start()

            each(1 << stage, send)
            part = vecs.at[pl.ds(0, 1 << stage)]
            remote(part, part, send_v.at[stage], recv_v.at[stage], other).wait()
        params[...] = jnp.zeros_like(params)
        lane = lax.broadcasted_iota(jnp.int32, (128, full), 0)
        column = lax.broadcasted_iota(jnp.int32, (128, full), 1)

        def place(index):
            chosen = ((lane < rows) & (column == index * rows + lane)).astype(F32).astype(BF16)
            params[...] += contract(vecs[index].astype(BF16), chosen, 1, 0)

        repeat(1 << bits, place)

    vec_path_of = tuple(range(bits))

    def vec_stage(stage):
        if stage > 0:
            earlier = vec_path_of[stage:]
            amount = 1 << len(earlier)
            part = vec_path.at[pl.ds(amount - 1, amount)]
            remote(part, part, out_v.at[stage - 1], in_v.at[stage - 1], (me, rank)).wait()

            def add(step):
                index = cleared(me, earlier) + spread(step, earlier)
                grad_vecs[index] = grad_vecs[index] + vec_path[amount - 1 + step]

            repeat(amount, add)
        if stage < bits:
            bit, later = vec_path_of[stage], vec_path_of[stage + 1 :]
            amount = 1 << len(later)

            def send(step):
                index = cleared(flipped(me, bit), later) + spread(step, later)
                remote(
                    grad_vecs.at[index],
                    vec_path.at[amount - 1 + step],
                    out_v.at[stage],
                    in_v.at[stage],
                    (flipped(me, bit), rank),
                ).start()

            each(amount, send)
        else:
            for hop in range(1, ranks):
                to = (me, lax.rem(rank + hop, ranks))
                remote(
                    grad_vecs.at[me], vec_z.at[hop - 1], out_v.at[bits], in_v.at[bits], to
                ).start()

    def vec_finish():
        remote(vec_z, vec_z, out_v.at[bits], in_v.at[bits], (me, rank)).wait()
        total = grad_vecs[me]
        for hop in range(1, ranks):
            total = total + vec_z[hop - 1]
        vec_sum[...] = total

    def router():
        return params[0:1, :]

    def gain_one():
        return params[1:2, :]

    def gain_two():
        return params[2:3, :]

    def by_rows(body):
        repeat(count // tile, lambda index: body(span(index, tile)))

    def by_blocks(body):
        repeat(blocks, lambda index: body(span(index, block)))

    def inverse_of(values):
        return lax.rsqrt(jnp.mean(values * values, axis=-1, keepdims=True) + 1e-06)

    def wide(values):
        return jnp.broadcast_to(values, (values.shape[0], 128))

    def transpose_to(target, source):
        for start in range(0, full, 128):
            part = source[:, start : start + 128].astype(F32)
            target[start : start + 128, :] = part.T.astype(BF16)

    slab = pairs * rows
    halves = length // slab

    def fetch(source, seq, step, place):
        def copy(index):
            pltpu.make_async_copy(
                source.at[seq, pl.ds(pl.multiple_of(index * rows, rows) + step * slab, rows)],
                from_core.at[place, index],
                fetched.at[place],
            ).start()

        each(pairs, copy)

    def down_and_across(seq):
        across = routes[pl.ds(rank * seqs + seq, 1), :].astype(F32)
        return jnp.broadcast_to(across, (caps, caps)).T, across

    def mask(seq):
        down, across = down_and_across(seq)
        begin = pic_start[rank * seqs + seq].astype(F32)
        inside_down = (down >= begin) & (down < begin + PIC)
        inside_across = (across >= begin) & (across < begin + PIC)
        seen = (across <= down) | (inside_down & inside_across)
        allowed[seq] = seen.astype(F32)

    def pick(target, seq, place):
        down, _ = down_and_across(seq)
        column = lax.broadcasted_iota(jnp.int32, (caps, slab), 1).astype(F32)
        for step in range(halves):
            pltpu.make_async_copy(
                from_core.at[place + step], from_core.at[place + step], fetched.at[place + step]
            ).wait()

        def body(part):
            total = 0.0
            for step in range(halves):
                chosen = (down[:, 0:1] == column + step * slab).astype(F32).astype(BF16)
                source = from_core[place + step, :, :, part].reshape(slab, block)
                total = total + contract(chosen, source, 1, 0)
            target[pl.ds(seq * caps, caps), part] = total.astype(BF16)

        by_blocks(body)

    def prepare():
        def body(part):
            values = picked[part].astype(F32)
            logit = jnp.sum(values * router(), axis=-1, keepdims=True)
            gate = 1.0 / (1.0 + jnp.exp(-logit))
            gates[part] = wide(gate)
            norm_one[part] = (values * inverse_of(values) * gain_one()).astype(BF16)
            branch[part] = (gate * grad_rows[part].astype(F32)).astype(BF16)

        by_rows(body)
        transpose_to(branch_t, branch)

    def project(which):
        def body(part):
            qkv[which, :, part] = contract(norm_one[...], held[which, :, part], 1, 0).astype(BF16)

        by_blocks(body)

    lanes = lax.broadcasted_iota(jnp.int32, (1, 2 * HD), 1)

    def own_lanes(values, head):
        inside = (lanes < HD) if head == 0 else (lanes >= HD)
        return jnp.where(inside, values, jnp.zeros_like(values))

    def probabilities(seq, queries, keys, head):
        scores = contract(own_lanes(queries, head), keys, 1, 1) * (1.0 / math.sqrt(HD))
        scores = jnp.where(allowed[seq] > 0, scores, -1e30)
        powers = jnp.exp(scores - jnp.max(scores, axis=-1, keepdims=True))
        return powers / jnp.sum(powers, axis=-1, keepdims=True)

    def attend():
        def body(index):
            part = span(index, 2 * HD)
            for seq in range(seqs):
                place = pl.ds(seq * caps, caps)
                queries, keys = qkv[0, place, part], qkv[1, place, part]
                values = qkv[2, place, part]
                total = 0.0
                for head in range(2):
                    probs = probabilities(seq, queries, keys, head).astype(BF16)
                    total = total + contract(probs, own_lanes(values, head), 1, 0)
                context[place, part] = total.astype(BF16)

        repeat(full // (2 * HD), body)

    def leave_attention():
        def body(part):
            attended[:, part] = contract(context[...], held[3, part, :], 1, 1)

        by_blocks(body)

        def rest(part):
            values = picked[part].astype(F32) + attended[part]
            norm_two[part] = (values * inverse_of(values) * gain_two()).astype(BF16)
            mlp[part] = jnp.zeros((tile, full), F32)
            grad_two[part] = jnp.zeros((tile, full), F32)

        by_rows(rest)
        transpose_to(norm_two_t, norm_two)

    def feed_forward(up, down):
        def units(part):
            pre = contract(norm_two[...], held[up, :, part], 1, 0)
            bell = 0.5 * (1.0 + lax.erf(pre * inv_root_two))
            slope = bell + pre * jnp.exp(-0.5 * pre * pre) * inv_root_two_pi
            hidden[:, part] = (pre * bell).astype(BF16)
            grad_hidden = contract(branch[...], held[down, :, part], 1, 0)
            grad_pre[:, part] = (grad_hidden * slope).astype(BF16)

        by_blocks(units)

        def outputs(part):
            mlp[:, part] += contract(hidden[...], held[down, part, :], 1, 1)
            grad_two[:, part] += contract(grad_pre[...], held[up, part, :], 1, 1)

        by_blocks(outputs)
        all_sent(up)
        all_sent(down)

        def gradients(part):
            held[down, :, part] = contract(branch_t[...], hidden[:, part], 1, 0).astype(BF16)
            held[up, :, part] = contract(norm_two_t[...], grad_pre[:, part], 1, 0).astype(BF16)

        by_blocks(gradients)

    small = params

    def enter_back():
        grad_attended, grad_attended_t, grad_context = norm_two, norm_two_t, hidden
        small[3:6, :] = jnp.zeros((3, full), F32)

        def body(part):
            values = picked[part].astype(F32)
            gate = gates[part, 0:1]
            delta = attended[part] + mlp[part]
            new_rows[part] = (values + gate * delta).astype(BF16)
            rows_in = grad_rows[part].astype(F32)
            score = jnp.sum(rows_in * delta, axis=-1, keepdims=True) * gate * (1.0 - gate)
            scores_of[part] = wide(score)
            small[3:4, :] += jnp.sum(score * values, axis=0, keepdims=True)
            residual = values + attended[part]
            inverse = inverse_of(residual)
            grad = grad_two[part]
            small[5:6, :] += jnp.sum(grad * residual * inverse, axis=0, keepdims=True)
            scaled = grad * gain_two()
            mean = jnp.mean(scaled * residual, axis=-1, keepdims=True)
            grad_mid = inverse * scaled - residual * (inverse * inverse * inverse * mean)
            grad_two[part] = grad_mid
            grad_attended[part] = (gate * rows_in + grad_mid).astype(BF16)

        by_rows(body)
        transpose_to(grad_attended_t, grad_attended)

        def through(part):
            grad_context[:, part] = contract(grad_attended[...], held[3, :, part], 1, 0).astype(BF16)

        by_blocks(through)
        for chunk in range(4):
            all_sent(chunk)

        def weights(part):
            held[3, :, part] = contract(grad_attended_t[...], context[:, part], 1, 0).astype(BF16)

        by_blocks(weights)

    def attend_back():
        grad_context = hidden
        grads = (branch, grad_pre, context)

        def body(index):
            part = span(index, 2 * HD)
            for seq in range(seqs):
                place = pl.ds(seq * caps, caps)
                queries, keys = qkv[0, place, part], qkv[1, place, part]
                values, grad = qkv[2, place, part], grad_context[place, part]
                grad_q, grad_k, grad_v = 0.0, 0.0, 0.0
                for head in range(2):
                    probs = probabilities(seq, queries, keys, head)
                    grad_probs = contract(own_lanes(grad, head), values, 1, 1)
                    inner = jnp.sum(probs * grad_probs, axis=-1, keepdims=True)
                    grad_scores = (probs * (grad_probs - inner)).astype(BF16)
                    low = probs.astype(BF16)
                    grad_v = grad_v + contract(low, own_lanes(grad, head), 0, 0)
                    grad_q = grad_q + contract(grad_scores, own_lanes(keys, head), 1, 0)
                    grad_k = grad_k + contract(grad_scores, own_lanes(queries, head), 0, 0)
                scale = 1.0 / math.sqrt(HD)
                grads[0][place, part] = (grad_q * scale).astype(BF16)
                grads[1][place, part] = (grad_k * scale).astype(BF16)
                grads[2][place, part] = grad_v.astype(BF16)

        repeat(full // (2 * HD), body)

    def leave_back():
        grads = (branch, grad_pre, context)
        grad_one, norm_one_t = mlp, branch_t

        def through(part):
            total = contract(grads[0][...], held[0, part, :], 1, 1)
            for which in (1, 2):
                total = total + contract(grads[which][...], held[which, part, :], 1, 1)
            grad_one[:, part] = total

        by_blocks(through)
        transpose_to(norm_one_t, norm_one)

        def weights(part):
            for which in range(3):
                held[which, :, part] = contract(norm_one_t[...], grads[which][:, part], 1, 0).astype(
                    BF16
                )

        by_blocks(weights)

        def body(part):
            values = picked[part].astype(F32)
            inverse = inverse_of(values)
            grad = grad_one[part]
            small[4:5, :] += jnp.sum(grad * values * inverse, axis=0, keepdims=True)
            scaled = grad * gain_one()
            mean = jnp.mean(scaled * values, axis=-1, keepdims=True)
            grad_norm = inverse * scaled - values * (inverse * inverse * inverse * mean)
            score = scores_of[part, 0:1]
            total = grad_rows[part].astype(F32) + grad_two[part] + grad_norm + score * router()
            new_grads[part] = total.astype(BF16)

        by_rows(body)
        own = small[...]
        if rows == 128:
            for index in range(1 << bits):
                grad_vecs[index] = own[:, index * rows : (index + 1) * rows]
        else:
            column = lax.broadcasted_iota(jnp.int32, (full, 128), 0)
            lane = lax.broadcasted_iota(jnp.int32, (full, 128), 1)

            def place(index):
                chosen = ((lane < rows) & (column == index * rows + lane)).astype(F32)
                grad_vecs[index] = jnp.dot(
                    own, chosen, precision=lax.Precision.HIGHEST, preferred_element_type=F32
                )

            repeat(1 << bits, place)

    def start(chunk):
        keep_own(chunk, shard(chunk)).start()
        for hop in range(1, ranks):
            remote(
                shard(chunk),
                held.at[chunk, mine, columns],
                send_z.at[chunk],
                recv_z.at[chunk],
                (me, lax.rem(rank + hop, ranks)),
            ).start()

    keep_vec = pltpu.make_async_copy(vec, vecs.at[me], local.at[chunks])
    keep_vec.start()
    for chunk in range(chunks):
        start(chunk)
    for which, source in enumerate((activations, cotangent)):
        for seq in range(seqs):
            for step in range(halves):
                fetch(source, seq, step, (which * seqs + seq) * halves + step)
    keep_vec.wait()
    vec_gather()
    for seq in range(seqs):
        mask(seq)
        for which, target in enumerate((picked, grad_rows)):
            pick(target, seq, (which * seqs + seq) * halves)
    prepare()
    lead = AHEAD * bits
    first = lead + 5
    items = chunks + PAUSE
    vec_first = lead + chunks + PAUSE + 1

    def tick(now, _):
        for stage in range(bits, -1, -1):
            chunk = now - AHEAD * stage

            @pl.when((chunk >= 0) & (chunk < chunks))
            def _(chunk=chunk, stage=stage):
                gather_stage(chunk, stage)

        whole = now - lead
        pl.when((whole >= 0) & (whole < 3))(lambda: project(whole))
        pl.when(whole == 2)(attend)
        pl.when(whole == 3)(leave_attention)
        pl.when((whole >= 5) & (whole < chunks) & (lax.rem(whole, 2) == 1))(
            lambda: feed_forward(whole - 1, whole)
        )
        for stage in range(bits + 1, -1, -1):
            item = now - first - AHEAD * stage
            inside = (item >= 0) & (item < items)
            paused = (item >= chunks - 4) & (item < chunks - 4 + PAUSE)

            @pl.when(inside & jnp.logical_not(paused))
            def _(item=item, stage=stage):
                scatter_stage(item, stage)

        pl.when(whole == chunks)(enter_back)
        pl.when(whole == chunks + 1)(attend_back)
        pl.when(whole == chunks + 2)(leave_back)
        for stage in range(bits + 1):
            pl.when(now == vec_first + AHEAD * stage)(functools.partial(vec_stage, stage))
        pl.when(now == vec_first + AHEAD * (bits + 1))(vec_finish)

    last = max(first + items - 1 + AHEAD * (bits + 1), vec_first + AHEAD * (bits + 1))
    lax.fori_loop(0, last + 1, tick, None)

    def drain(chunk):
        z_copy(chunk).wait_send()
        item = jnp.where(chunk < chunks - 4, chunk, chunk + PAUSE)
        given_core(item).wait_send()
        for colour in range(2):
            for stage in range(bits - 1):
                given_path(item, colour, stage).wait_send()
        given_across(item).wait_send()

    repeat(chunks, drain)


def run_layer(bits, ranks, shards, vec, routes, pic_start, activations, cotangent):
    rows, width = shards[0].shape
    parts = shards[4].shape[1] // width
    chunks = 4 + 2 * parts
    depth, breadth, pairs = rows << bits, width * ranks, 1 << (bits - 1)
    seqs, _, full = activations.shape
    caps = routes.shape[1]
    count = seqs * caps
    dma = pltpu.SemaphoreType.DMA
    low = pltpu.VMEM((count, full), BF16)
    turned = pltpu.VMEM((full, count), BF16)
    high = pltpu.VMEM((count, full), F32)
    return pl.pallas_call(
        functools.partial(layer_kernel, bits, ranks, chunks, parts),
        out_shape=[
            jax.ShapeDtypeStruct((chunks, rows, width), F32),
            jax.ShapeDtypeStruct((8, 128), F32),
            jax.ShapeDtypeStruct((count, full), BF16),
            jax.ShapeDtypeStruct((count, full), BF16),
        ],
        in_specs=[ANY] * 6 + [VMEM] * 2 + [pl.BlockSpec(memory_space=pltpu.SMEM)] + [ANY] * 2,
        out_specs=[VMEM] * 4,
        scratch_shapes=[
            low,
            low,
            pltpu.VMEM((seqs, caps, caps), F32),
            pltpu.VMEM((chunks, depth, breadth), BF16),
            pltpu.VMEM((RING, pairs, rows, breadth), BF16),
            pltpu.VMEM((chunks, ranks - 1, rows, width), BF16),
            pltpu.VMEM((1 << bits, 8, 128), F32),
            pltpu.VMEM((1 << bits, 8, 128), F32),
            pltpu.VMEM((1 << bits, 8, 128), F32),
            pltpu.VMEM((ranks - 1, 8, 128), F32),
            pltpu.VMEM((8, full), F32),
            pltpu.VMEM((count, 128), F32),
            pltpu.VMEM((count, 128), F32),
            low,
            pltpu.VMEM((3, count, full), BF16),
            low,
            high,
            low,
            turned,
            low,
            turned,
            low,
            low,
            high,
            high,
            dma((chunks,)),
            dma((chunks,)),
            dma((chunks, 2, bits - 1)),
            dma((chunks, 2, bits - 1)),
            dma((chunks,)),
            dma((chunks,)),
            dma((bits,)),
            dma((bits,)),
            dma((chunks + 1,)),
            dma((chunks,)),
            dma((chunks,)),
            dma((chunks, 2, bits - 1)),
            dma((chunks, 2, bits - 1)),
            dma((chunks,)),
            dma((chunks,)),
            dma((bits + 1,)),
            dma((bits + 1,)),
            dma((RING,)),
            *[
                pltpu.VMEM((chunks, 2, pairs >> (stage + 1), rows, breadth // 2), BF16)
                for stage in range(bits - 1)
            ],
        ],
        compiler_params=pltpu.CompilerParams(
            collective_id=1, has_side_effects=True, vmem_limit_bytes=67043328
        ),
        name="layer_kernel",
    )(*shards, vec, routes, pic_start, activations, cotangent)


def put_kernel(seqs, steps, routes, new_rows, new_grads, activations, cotangent, result, grad_input):
    index = pl.program_id(0)
    seq, step = lax.div(index, steps), lax.rem(index, steps)
    size, caps = activations.shape[1], routes.shape[1]
    place = routes[pl.ds(lax.axis_index("tensor") * seqs + seq, 1), :]
    line = lax.broadcasted_iota(jnp.int32, (size, caps), 0) + step * size
    chosen = (line == place).astype(F32)
    routed = jnp.max(chosen, axis=-1, keepdims=True) > 0
    chosen = chosen.astype(BF16)
    for new, base, out in (
        (new_rows, activations, result),
        (new_grads, cotangent, grad_input),
    ):
        placed = contract(chosen, new[...], 1, 0)
        out[0] = jnp.where(routed, placed, base[0].astype(F32)).astype(BF16)


def put_rows(routes, new_rows, new_grads, activations, cotangent):
    seqs, length, full = activations.shape
    caps = routes.shape[1]
    steps = 4
    size = length // steps
    large = pl.BlockSpec((1, size, full), lambda index: (index // steps, index % steps, 0))
    small = pl.BlockSpec((caps, full), lambda index: (index // steps, 0))
    return pl.pallas_call(
        functools.partial(put_kernel, seqs, steps),
        grid=(seqs * steps,),
        out_shape=[jax.ShapeDtypeStruct(activations.shape, BF16)] * 2,
        in_specs=[pl.BlockSpec(routes.shape, lambda index: (0, 0)), small, small, large, large],
        out_specs=[large, large],
        name="put_rows",
    )(routes, new_rows, new_grads, activations, cotangent)


def shards(
    activations,
    routes,
    pic_start,
    router_w,
    gain_attn,
    gain_mlp,
    w_query,
    w_key,
    w_value,
    w_proj,
    w_up,
    w_down,
    cotangent,
):
    ranks = lax.axis_size("tensor")
    bits = lax.axis_size("dp").bit_length() - 1
    rows, width = w_query.shape
    parts = w_up.shape[1] // width
    vec = jnp.stack([router_w, gain_attn, gain_mlp]).astype(F32)
    vec = jnp.pad(vec, ((0, 5), (0, 128 - rows)))
    weights = (w_query, w_key, w_value, w_proj, w_up, w_down)
    sums, small, new_rows, new_grads = run_layer(
        bits, ranks, weights, vec, routes, pic_start, activations, cotangent
    )
    result, grad_input = put_rows(routes, new_rows, new_grads, activations, cotangent)

    def side_by_side(first):
        return jnp.concatenate([sums[first + 2 * part] for part in range(parts)], axis=1)

    return (
        result,
        grad_input,
        small[3, :rows],
        small[4, :rows],
        small[5, :rows],
        sums[0],
        sums[1],
        sums[2],
        sums[3],
        side_by_side(4),
        side_by_side(5),
    )


def solution(mesh):
    both = P(("dp", "tensor"), None, None)
    cut = P("dp", "tensor")
    one = P("dp")
    return jax.shard_map(
        shards,
        mesh=mesh,
        in_specs=(both, P("dp", None), one, one, one, one) + (cut,) * 6 + (both,),
        out_specs=(both, both, one, one, one) + (cut,) * 6,
        check_vma=False,
    )
```

```python
import functools
import math

import jax
import jax.numpy as jnp
from jax import lax
from jax.experimental import pallas as pl
from jax.experimental.pallas import tpu as pltpu
from jax.sharding import PartitionSpec as P

HD = 64
PIC = 256
AHEAD = 2
RING = 8
PAUSE = 1
MESH = pl.DeviceIdType.MESH
ANY = pl.BlockSpec(memory_space=pl.ANY)
VMEM = pl.BlockSpec(memory_space=pltpu.VMEM)
BF16 = jnp.bfloat16
F32 = jnp.float32

inv_root_two = 0.7071067811865476
inv_root_two_pi = 0.3989422804014327


def bit_of(value, bit):
    return lax.rem(lax.div(value, 1 << bit), 2)


def flipped(value, bit):
    return value + (1 - 2 * bit_of(value, bit)) * (1 << bit)


def cleared(value, bits):
    for bit in bits:
        value = value - bit_of(value, bit) * (1 << bit)
    return value


def spread(step, bits):
    value = 0
    for place, bit in enumerate(bits):
        value = value + lax.rem(lax.div(step, 1 << place), 2) * (1 << bit)
    return value


def each(count, body):
    if count <= 4:
        for step in range(count):
            body(jnp.int32(step))
    else:
        lax.fori_loop(0, count, lambda step, _: body(step), None)


def repeat(count, body):
    def step(index, _):
        body(index)

    lax.fori_loop(0, count, step, None)


def span(index, size):
    return pl.ds(pl.multiple_of(index * size, size), size)


def sides(bits):
    return (tuple(range(bits - 1, 1, -1)),) * 2


def orders(bits):
    return (tuple(range(bits - 1, 0, -1)), tuple(range(1, bits)))


def remote(src, dst, send, recv, where):
    return pltpu.make_async_remote_copy(
        src_ref=src, dst_ref=dst, send_sem=send, recv_sem=recv, device_id=where, device_id_type=MESH
    )


def contract(left, right, axis_left, axis_right):
    return lax.dot_general(
        left, right, (((axis_left,), (axis_right,)), ((), ())), preferred_element_type=F32
    )


def layer_kernel(
    bits,
    ranks,
    chunks,
    parts,
    *refs,
):
    shards = refs[:6]
    (
    vec,
    routes,
    pic_start,
    activations,
    cotangent,
    sums,
    vec_sum,
    new_rows,
    new_grads,
    picked,
    grad_rows,
    allowed,
    held,
    from_core,
    from_z,
    vecs,
    grad_vecs,
    vec_path,
    vec_z,
    params,
    gates,
    norm_one,
    qkv,
    context,
    attended,
    norm_two,
    norm_two_t,
    branch,
    branch_t,
    hidden,
    grad_pre,
    mlp,
    grad_two,
    slopes,
    mlp_low,
    grad_low,
    mlp_in,
    grad_in,
    grad_attended,
    grad_attended_t,
    grad_context,
    grad_qkv,
    grad_one,
    norm_one_t,
    side_out,
    side_in,
    send_x,
    recv_x,
    act_out,
    act_in,
    out_x,
    in_x,
    send_z,
    recv_z,
    send_p,
    recv_p,
    send_c,
    recv_c,
    send_v,
    recv_v,
    local,
    out_c,
    in_c,
    out_p,
    in_p,
    out_z,
    in_z,
    out_v,
    in_v,
    fetched,
    *from_path,
    ) = refs[6:]
    me, rank = lax.axis_index("dp"), lax.axis_index("tensor")
    rows, width = shards[0].shape
    count, full = picked.shape
    length = activations.shape[1]
    seqs, caps, _ = allowed.shape
    half = full // 2
    seat, pair = bit_of(me, 0), lax.div(me, 2)
    pairs = 1 << (bits - 1)
    paths = (orders(bits), sides(bits))
    back_paths = tuple(
        tuple(tuple(bit - 1 for bit in order[::-1]) for order in kind) for kind in paths
    )
    side, beside = bit_of(me, 1), flipped(me, 1)
    tile = 32
    block = 256
    blocks = full // block

    barrier = pltpu.get_barrier_semaphore()
    for bit in range(bits):
        pl.semaphore_signal(barrier, 1, device_id=(flipped(me, bit), rank), device_id_type=MESH)
    for hop in range(1, ranks):
        pl.semaphore_signal(
            barrier, 1, device_id=(me, lax.rem(rank + hop, ranks)), device_id_type=MESH
        )
    pl.semaphore_wait(barrier, bits + ranks - 1)

    mine = span(me, rows)
    columns = span(rank, width)

    def shard(chunk, which):
        if chunk < 4:
            return shards[chunk]
        index = which * (parts // 2) + (chunk - 4) // 2
        return shards[4 + chunk % 2].at[:, span(index, width)]

    def keep_own(chunk, source=shards[0]):
        return pltpu.make_async_copy(source, held.at[chunk, mine, columns], local.at[chunk])

    def bulk(chunk, depth, breadth):
        return held.at[chunk, pl.ds(0, depth), pl.ds(0, breadth)]

    def send_z_of(chunk, source, index):
        for hop in range(1, ranks):
            remote(
                source,
                held.at[chunk, span(index, rows), columns],
                send_z.at[chunk],
                recv_z.at[chunk],
                (me, lax.rem(rank + hop, ranks)),
            ).start()

    def x_copy(chunk):
        part = bulk(chunk, rows, width)
        return remote(part, part, send_x.at[chunk], recv_x.at[chunk], (me, rank))

    def start(chunk):
        keep_own(chunk, shard(chunk, side)).start()
        if chunk >= 4:
            remote(
                shard(chunk, 1 - side),
                held.at[chunk, mine, columns],
                send_x.at[chunk],
                recv_x.at[chunk],
                (beside, rank),
            ).start()

    def start_z(chunk):
        if chunk >= 4:
            x_copy(chunk).wait_recv()
            send_z_of(chunk, held.at[chunk, span(beside, rows), columns], beside)
        send_z_of(chunk, shard(chunk, side), me)

    def z_copy(chunk, kind):
        part = bulk(chunk, rows << kind, width * (ranks - 1))
        return remote(part, part, send_z.at[chunk], recv_z.at[chunk], (me, rank))

    def send_path(chunk, kind, colour, stage):
        order = paths[kind][colour]
        earlier = order[:stage] + (1,) * kind
        other = (flipped(me, order[stage]), rank)

        def send(step):
            index = cleared(me, earlier) + spread(step, earlier)
            part = held.at[chunk, span(index, rows), pl.ds(colour * half, half)]
            remote(
                part,
                part,
                send_p.at[chunk, colour, stage],
                recv_p.at[chunk, colour, stage],
                other,
            ).start()

        each(1 << len(earlier), send)

    def path_copy(chunk, kind, colour, stage):
        part = bulk(chunk, rows << (stage + kind), half)
        return remote(
            part,
            part,
            send_p.at[chunk, colour, stage],
            recv_p.at[chunk, colour, stage],
            (me, rank),
        )

    def send_core(chunk):
        other = (flipped(me, 0), rank)

        def send(step):
            part = held.at[chunk, span(2 * step + seat, rows)]
            remote(part, part, send_c.at[chunk], recv_c.at[chunk], other).start()

        each(pairs, send)

    def core_copy(chunk):
        part = bulk(chunk, rows << (bits - 1), full)
        return remote(part, part, send_c.at[chunk], recv_c.at[chunk], (me, rank))

    def all_sent(chunk, kind):
        z_copy(chunk, kind).wait_send()
        if kind:
            x_copy(chunk).wait_send()
        for colour in range(2):
            for stage in range(bits - 1 - kind):
                path_copy(chunk, kind, colour, stage).wait_send()
        core_copy(chunk).wait_send()

    def gather_stage(chunk, kind, stage):
        if stage < kind:
            return
        if stage == kind:
            keep_own(chunk).wait()
            z_copy(chunk, kind).wait_recv()
        elif stage < bits:
            for colour in range(2):
                path_copy(chunk, kind, colour, stage - 1 - kind).wait_recv()
        else:
            core_copy(chunk).wait_recv()
        if stage < bits - 1:
            for colour in range(2):
                send_path(chunk, kind, colour, stage - kind)
        elif stage == bits - 1:
            send_core(chunk)

    units = chunks - 4

    def turn(item):
        return jnp.where(item < units, item, item - PAUSE)

    def slot(item):
        return jnp.where(item < units, item + 4, lax.rem(item - PAUSE - units + 3, 4))

    def give_core(item):
        def send(step):
            remote(
                held.at[slot(item), span(2 * step + 1 - seat, rows)],
                from_core.at[lax.rem(turn(item), RING), step],
                out_c.at[turn(item)],
                in_c.at[turn(item)],
                (flipped(me, 0), rank),
            ).start()

        each(pairs, send)

    def given_core(item):
        part = from_core.at[lax.rem(turn(item), RING)]
        return remote(part, part, out_c.at[turn(item)], in_c.at[turn(item)], (me, rank))

    def add_to(item, index, where, source):
        step = min(rows, tile)
        for start in range(0, rows, step):
            place = pl.ds(pl.multiple_of((2 * index + seat) * rows, rows) + start, step)
            here = held.at[slot(item), place, where]
            here[...] = (
                here[...].astype(F32) + source[pl.ds(start, step)].astype(F32)
            ).astype(BF16)

    def add_core(item):
        repeat(
            pairs,
            lambda step: add_to(
                item, step, pl.ds(0, full), from_core.at[lax.rem(turn(item), RING), step]
            ),
        )

    def members(kind, colour, stage, step, kept):
        order = back_paths[kind][colour]
        later = order[stage + 1 :] + (0,) * kind
        index = pair if kept else flipped(pair, order[stage])
        return cleared(index, later) + spread(step, later)

    def give_path(item, kind, colour, stage):
        other = (2 * flipped(pair, back_paths[kind][colour][stage]) + seat, rank)

        def send(step):
            index = members(kind, colour, stage, step, False)
            remote(
                held.at[
                    slot(item), span(2 * index + seat, rows), pl.ds(colour * half, half)
                ],
                from_path[stage].at[turn(item), colour, step],
                out_p.at[turn(item), colour, stage],
                in_p.at[turn(item), colour, stage],
                other,
            ).start()

        each(pairs >> (stage + 1), send)

    def given_path(item, colour, stage):
        part = from_path[stage].at[turn(item), colour]
        return remote(
            part,
            part,
            out_p.at[turn(item), colour, stage],
            in_p.at[turn(item), colour, stage],
            (me, rank),
        )

    def add_path(item, kind, colour, stage):
        repeat(
            pairs >> (stage + 1),
            lambda step: add_to(
                item,
                members(kind, colour, stage, step, True),
                pl.ds(colour * half, half),
                from_path[stage].at[turn(item), colour, step],
            ),
        )

    def give_across(item, kind):
        for hop in range(1, ranks):
            to = lax.rem(rank + hop, ranks)
            for which in range(1 + kind):
                remote(
                    held.at[slot(item), span((me, beside)[which], rows), span(to, width)],
                    from_z.at[turn(item), (hop - 1) * (1 + kind) + which],
                    out_z.at[turn(item)],
                    in_z.at[turn(item)],
                    (me, to),
                ).start()

    def given_across(item, kind):
        part = from_z.at[turn(item), pl.ds(0, (ranks - 1) * (1 + kind))]
        return remote(part, part, out_z.at[turn(item)], in_z.at[turn(item)], (me, rank))

    def total_of(item, kind, which):
        total = held[slot(item), span((me, beside)[which], rows), columns].astype(F32)
        for hop in range(1, ranks):
            total = total + from_z[turn(item), (hop - 1) * (1 + kind) + which].astype(F32)
        return total

    def unit_place(item, which):
        return 4 + 2 * (which * (parts // 2) + lax.div(item, 2)) + lax.rem(item, 2)

    def side_copy(item):
        return remote(
            side_out.at[item], side_in.at[item], out_x.at[item], in_x.at[item], (beside, rank)
        )

    def scatter_stage(item, kind, stage):
        if stage == 1:
            given_core(item).wait_recv()
            add_core(item)
        elif 1 < stage <= bits - kind:
            for colour in range(2):
                given_path(item, colour, stage - 2).wait_recv()
                add_path(item, kind, colour, stage - 2)
        elif stage == bits - kind + 1:
            given_across(item, kind).wait_recv()
            if kind:
                side_out[item] = total_of(item, kind, 1).astype(BF16)
                side_copy(item).start()
                sums[unit_place(item, side)] = total_of(item, kind, 0)
            else:
                sums[slot(item)] = total_of(item, kind, 0)
        elif stage == bits - kind + 2:
            side_copy(item).wait_recv()
            sums[unit_place(item, 1 - side)] = side_in[item].astype(F32)
        if stage == 0:
            give_core(item)
        elif stage < bits - kind:
            for colour in range(2):
                give_path(item, kind, colour, stage - 1)
        elif stage == bits - kind:
            give_across(item, kind)

    vec_ways = tuple(range(bits - 1, -1, -1))

    def vec_gather(stage):
        if stage > 0:
            part = vecs.at[pl.ds(0, 1 << (stage - 1))]
            remote(part, part, send_v.at[stage - 1], recv_v.at[stage - 1], (me, rank)).wait()
        if stage < bits:

            def send(step):
                index = cleared(me, vec_ways[:stage]) + spread(step, vec_ways[:stage])
                remote(
                    vecs.at[index],
                    vecs.at[index],
                    send_v.at[stage],
                    recv_v.at[stage],
                    (flipped(me, vec_ways[stage]), rank),
                ).start()

            each(1 << stage, send)

    def spell_params():
        params[...] = jnp.zeros_like(params)
        lane = lax.broadcasted_iota(jnp.int32, (128, full), 0)
        column = lax.broadcasted_iota(jnp.int32, (128, full), 1)

        def place(index):
            chosen = ((lane < rows) & (column == index * rows + lane)).astype(F32).astype(BF16)
            params[...] += contract(vecs[index].astype(BF16), chosen, 1, 0)

        if rows == 128:
            for index in range(1 << bits):
                params[:, index * rows : (index + 1) * rows] = vecs[index]
        else:
            repeat(1 << bits, place)

    vec_path_of = tuple(range(bits))

    def vec_stage(stage):
        if stage > 0:
            earlier = vec_path_of[stage:]
            amount = 1 << len(earlier)
            part = vec_path.at[pl.ds(amount - 1, amount)]
            remote(part, part, out_v.at[stage - 1], in_v.at[stage - 1], (me, rank)).wait()

            def add(step):
                index = cleared(me, earlier) + spread(step, earlier)
                grad_vecs[index] = grad_vecs[index] + vec_path[amount - 1 + step]

            repeat(amount, add)
        if stage < bits:
            bit, later = vec_path_of[stage], vec_path_of[stage + 1 :]
            amount = 1 << len(later)

            def send(step):
                index = cleared(flipped(me, bit), later) + spread(step, later)
                remote(
                    grad_vecs.at[index],
                    vec_path.at[amount - 1 + step],
                    out_v.at[stage],
                    in_v.at[stage],
                    (flipped(me, bit), rank),
                ).start()

            each(amount, send)
        else:
            for hop in range(1, ranks):
                to = (me, lax.rem(rank + hop, ranks))
                remote(
                    grad_vecs.at[me], vec_z.at[hop - 1], out_v.at[bits], in_v.at[bits], to
                ).start()

    def vec_finish():
        remote(vec_z, vec_z, out_v.at[bits], in_v.at[bits], (me, rank)).wait()
        total = grad_vecs[me]
        for hop in range(1, ranks):
            total = total + vec_z[hop - 1]
        vec_sum[...] = total

    def router():
        return params[0:1, :]

    def gain_one():
        return params[1:2, :]

    def gain_two():
        return params[2:3, :]

    def by_rows(body):
        repeat(count // tile, lambda index: body(span(index, tile)))

    def by_blocks(body):
        repeat(blocks, lambda index: body(span(index, block)))

    def inverse_of(values):
        return lax.rsqrt(jnp.mean(values * values, axis=-1, keepdims=True) + 1e-06)

    def wide(values):
        return jnp.broadcast_to(values, (values.shape[0], 128))

    def transpose_to(target, source, first=0):
        def turn_over(index):
            part = span(index, 128)
            values = source[first : first + count, part].astype(F32)
            target[part, first : first + count] = values.T.astype(BF16)

        repeat(full // 128, turn_over)

    def to_beside(which, source, target):
        return remote(source, target, act_out.at[which], act_in.at[which], (beside, rank))

    own_rows, their_rows = pl.ds(0, count), pl.ds(count, count)

    def branch_copy():
        return to_beside(0, branch.at[own_rows], branch.at[their_rows])

    def norm_copy():
        return to_beside(1, norm_two.at[own_rows], norm_two.at[their_rows])

    def grad_copy():
        return to_beside(2, grad_low, grad_in)

    def mlp_copy():
        return to_beside(3, mlp_low, mlp_in)

    slab = pairs * rows
    halves = length // slab

    def fetch(source, seq, step, place):
        def copy(index):
            pltpu.make_async_copy(
                source.at[seq, pl.ds(pl.multiple_of(index * rows, rows) + step * slab, rows)],
                from_core.at[place, index],
                fetched.at[place],
            ).start()

        each(pairs, copy)

    def down_and_across(seq):
        across = routes[pl.ds(rank * seqs + seq, 1), :].astype(F32)
        return jnp.broadcast_to(across, (caps, caps)).T, across

    def mask(seq):
        down, across = down_and_across(seq)
        begin = pic_start[rank * seqs + seq].astype(F32)
        inside_down = (down >= begin) & (down < begin + PIC)
        inside_across = (across >= begin) & (across < begin + PIC)
        seen = (across <= down) | (inside_down & inside_across)
        allowed[seq] = seen.astype(F32)

    def pick(target, seq, place):
        down, _ = down_and_across(seq)
        column = lax.broadcasted_iota(jnp.int32, (caps, slab), 1).astype(F32)
        for step in range(halves):
            pltpu.make_async_copy(
                from_core.at[place + step], from_core.at[place + step], fetched.at[place + step]
            ).wait()

        def body(part):
            total = 0.0
            for step in range(halves):
                chosen = (down[:, 0:1] == column + step * slab).astype(F32).astype(BF16)
                source = from_core[place + step, :, :, part].reshape(slab, block)
                total = total + contract(chosen, source, 1, 0)
            target[pl.ds(seq * caps, caps), part] = total.astype(BF16)

        by_blocks(body)

    def prepare():
        def body(part):
            values = picked[part].astype(F32)
            logit = jnp.sum(values * router(), axis=-1, keepdims=True)
            gate = 1.0 / (1.0 + jnp.exp(-logit))
            gates[part] = wide(gate)
            norm_one[part] = (values * inverse_of(values) * gain_one()).astype(BF16)
            branch[part] = (gate * grad_rows[part].astype(F32)).astype(BF16)

        by_rows(body)
        branch_copy().start()
        transpose_to(branch_t, branch)

    def project(which):
        def body(part):
            qkv[which, :, part] = contract(norm_one[...], held[which, :, part], 1, 0).astype(BF16)

        by_blocks(body)

    lanes = lax.broadcasted_iota(jnp.int32, (1, 2 * HD), 1)

    def own_lanes(values, head):
        inside = (lanes < HD) if head == 0 else (lanes >= HD)
        return jnp.where(inside, values, jnp.zeros_like(values))

    def probabilities(seq, queries, keys, head):
        scores = contract(own_lanes(queries, head), keys, 1, 1) * (1.0 / math.sqrt(HD))
        scores = jnp.where(allowed[seq] > 0, scores, -1e30)
        powers = jnp.exp(scores - jnp.max(scores, axis=-1, keepdims=True))
        return powers / jnp.sum(powers, axis=-1, keepdims=True)

    def attend():
        def body(index):
            part = span(index, 2 * HD)
            for seq in range(seqs):
                place = pl.ds(seq * caps, caps)
                queries, keys = qkv[0, place, part], qkv[1, place, part]
                values = qkv[2, place, part]
                total = 0.0
                for head in range(2):
                    probs = probabilities(seq, queries, keys, head).astype(BF16)
                    total = total + contract(probs, own_lanes(values, head), 1, 0)
                context[place, part] = total.astype(BF16)

        repeat(full // (2 * HD), body)

    def leave_attention():
        def body(part):
            attended[:, part] = contract(context[...], held[3, part, :], 1, 1)

        by_blocks(body)

        def rest(part):
            values = picked[part].astype(F32) + attended[part]
            norm_two[part] = (values * inverse_of(values) * gain_two()).astype(BF16)

        by_rows(rest)
        norm_copy().start()
        transpose_to(norm_two_t, norm_two)
        mlp[...] = jnp.zeros_like(mlp)
        grad_two[...] = jnp.zeros_like(grad_two)

    def by_lines(body):
        repeat(2 * blocks, lambda i: body(span(lax.rem(i, 2), count), span(lax.div(i, 2), block)))

    def go_up(up):
        @pl.when(up == 4)
        def _():
            branch_copy().wait_recv()
            transpose_to(branch_t, branch, count)
            norm_copy().wait_recv()
            transpose_to(norm_two_t, norm_two, count)

        def units_of(lines, part):
            pre = contract(norm_two[lines], held[up, :, part], 1, 0)
            bell = 0.5 * (1.0 + lax.erf(pre * inv_root_two))
            slopes[lines, part] = bell + pre * jnp.exp(-0.5 * pre * pre) * inv_root_two_pi
            hidden[lines, part] = (pre * bell).astype(BF16)

        by_lines(units_of)

    def go_down(up, down):
        def units_of(lines, part):
            grad_hidden = contract(branch[lines], held[down, :, part], 1, 0)
            grad_pre[lines, part] = (grad_hidden * slopes[lines, part]).astype(BF16)

        by_lines(units_of)

        def add_out(target, source, weight, lines):
            def body(part):
                target[lines, part] += contract(source[lines], held[weight, part, :], 1, 1)

            by_blocks(body)

        def pass_on(source, target, copy):
            @pl.when(down == chunks - 1)
            def _():
                def body(part):
                    target[part] = source[pl.ds(part.start + count, tile)].astype(BF16)

                by_rows(body)
                copy().start()

        add_out(grad_two, grad_pre, up, their_rows)
        pass_on(grad_two, grad_low, grad_copy)
        add_out(mlp, hidden, down, their_rows)
        pass_on(mlp, mlp_low, mlp_copy)
        add_out(grad_two, grad_pre, up, own_rows)
        add_out(mlp, hidden, down, own_rows)
        all_sent(up, 1)
        all_sent(down, 1)

        def gradients(part):
            held[down, :, part] = contract(branch_t[...], hidden[:, part], 1, 0).astype(BF16)
            held[up, :, part] = contract(norm_two_t[...], grad_pre[:, part], 1, 0).astype(BF16)

        by_blocks(gradients)

    small = params

    def enter_back():
        small[3:6, :] = jnp.zeros((3, full), F32)
        grad_copy().wait_recv()

        def body(part):
            values = picked[part].astype(F32)
            residual = values + attended[part]
            inverse = inverse_of(residual)
            grad = grad_two[part] + grad_in[part].astype(F32)
            small[5:6, :] += jnp.sum(grad * residual * inverse, axis=0, keepdims=True)
            scaled = grad * gain_two()
            mean = jnp.mean(scaled * residual, axis=-1, keepdims=True)
            grad_mid = inverse * scaled - residual * (inverse * inverse * inverse * mean)
            grad_two[part] = grad_mid
            rows_in = grad_rows[part].astype(F32)
            grad_attended[part] = (gates[part, 0:1] * rows_in + grad_mid).astype(BF16)

        by_rows(body)
        transpose_to(grad_attended_t, grad_attended)

        def through(part):
            grad_context[:, part] = contract(grad_attended[...], held[3, :, part], 1, 0).astype(BF16)

        by_blocks(through)
        for chunk in range(4):
            all_sent(chunk, 0)

        def weights(part):
            held[3, :, part] = contract(grad_attended_t[...], context[:, part], 1, 0).astype(BF16)

        by_blocks(weights)
        give_core(jnp.int32(units + PAUSE))

    def attend_back():
        def body(index):
            part = span(index, 2 * HD)
            for seq in range(seqs):
                place = pl.ds(seq * caps, caps)
                queries, keys = qkv[0, place, part], qkv[1, place, part]
                values, grad = qkv[2, place, part], grad_context[place, part]
                grad_q, grad_k, grad_v = 0.0, 0.0, 0.0
                for head in range(2):
                    probs = probabilities(seq, queries, keys, head)
                    grad_probs = contract(own_lanes(grad, head), values, 1, 1)
                    inner = jnp.sum(probs * grad_probs, axis=-1, keepdims=True)
                    grad_scores = (probs * (grad_probs - inner)).astype(BF16)
                    low = probs.astype(BF16)
                    grad_v = grad_v + contract(low, own_lanes(grad, head), 0, 0)
                    grad_q = grad_q + contract(grad_scores, own_lanes(keys, head), 1, 0)
                    grad_k = grad_k + contract(grad_scores, own_lanes(queries, head), 0, 0)
                scale = 1.0 / math.sqrt(HD)
                grad_qkv[0, place, part] = (grad_q * scale).astype(BF16)
                grad_qkv[1, place, part] = (grad_k * scale).astype(BF16)
                grad_qkv[2, place, part] = grad_v.astype(BF16)

        repeat(full // (2 * HD), body)

    def leave_back():
        def through(part):
            total = contract(grad_qkv[0], held[0, part, :], 1, 1)
            for which in (1, 2):
                total = total + contract(grad_qkv[which], held[which, part, :], 1, 1)
            grad_one[:, part] = total

        by_blocks(through)
        transpose_to(norm_one_t, norm_one)

        def weights(part):
            for which in range(3):
                held[which, :, part] = contract(norm_one_t[...], grad_qkv[which, :, part], 1, 0).astype(
                    BF16
                )

        by_blocks(weights)
        for item in range(units + PAUSE + 1, units + PAUSE + 4):
            give_core(jnp.int32(item))

    def close():
        mlp_copy().wait_recv()

        def body(part):
            values = picked[part].astype(F32)
            rows_in = grad_rows[part].astype(F32)
            gate = gates[part, 0:1]
            delta = attended[part] + (mlp[part] + mlp_in[part].astype(F32))
            new_rows[part] = (values + gate * delta).astype(BF16)
            score = jnp.sum(rows_in * delta, axis=-1, keepdims=True) * gate * (1.0 - gate)
            small[3:4, :] += jnp.sum(score * values, axis=0, keepdims=True)
            inverse = inverse_of(values)
            grad = grad_one[part]
            small[4:5, :] += jnp.sum(grad * values * inverse, axis=0, keepdims=True)
            scaled = grad * gain_one()
            mean = jnp.mean(scaled * values, axis=-1, keepdims=True)
            grad_norm = inverse * scaled - values * (inverse * inverse * inverse * mean)
            total = rows_in + grad_two[part] + grad_norm + score * router()
            new_grads[part] = total.astype(BF16)

        by_rows(body)
        own = small[...]
        if rows == 128:
            for index in range(1 << bits):
                grad_vecs[index] = own[:, index * rows : (index + 1) * rows]
        else:
            column = lax.broadcasted_iota(jnp.int32, (full, 128), 0)
            lane = lax.broadcasted_iota(jnp.int32, (full, 128), 1)

            def place(index):
                chosen = ((lane < rows) & (column == index * rows + lane)).astype(F32)
                grad_vecs[index] = jnp.dot(
                    own, chosen, precision=lax.Precision.HIGHEST, preferred_element_type=F32
                )

            repeat(1 << bits, place)

    keep_vec = pltpu.make_async_copy(vec, vecs.at[me], local.at[chunks])
    keep_vec.start()
    for chunk in range(4):
        start(chunk)
        start_z(chunk)
    for chunk in range(4, chunks):
        start(chunk)
    for which, source in enumerate((activations, cotangent)):
        for seq in range(seqs):
            for step in range(halves):
                fetch(source, seq, step, (which * seqs + seq) * halves + step)
    keep_vec.wait()
    vec_gather(0)

    lead = AHEAD * bits
    first = lead + 5
    items = chunks + PAUSE
    vec_first = lead + chunks + 6

    def tick(now, _):
        for stage in range(bits, -1, -1):
            chunk = now - AHEAD * stage

            @pl.when((chunk >= 0) & (chunk < chunks))
            def _(chunk=chunk, stage=stage):
                pl.when(chunk < 4)(lambda: gather_stage(chunk, 0, stage))
                pl.when(chunk >= 4)(lambda: gather_stage(chunk, 1, stage))

        for stage in range(1, bits + 1):
            pl.when(now == stage)(functools.partial(vec_gather, stage))

        @pl.when(now == 1)
        def _():
            for chunk in range(4, chunks):
                start_z(chunk)

        for seq in range(seqs):
            for which, target in enumerate((picked, grad_rows)):
                order = 2 * seq + which
                place = (which * seqs + seq) * halves
                pl.when(now == order)(functools.partial(pick, target, seq, place))
            pl.when(now == 2 * seq)(functools.partial(mask, seq))

        @pl.when(now == max(bits, 2 * seqs - 1) + 1)
        def _():
            spell_params()
            prepare()

        whole = now - lead
        pl.when((whole >= 0) & (whole < 3))(lambda: project(whole))
        pl.when(whole == 2)(attend)
        pl.when(whole == 3)(leave_attention)
        units_in = (whole >= 4) & (whole < chunks)
        pl.when(units_in & (lax.rem(whole, 2) == 0))(lambda: go_up(whole))
        pl.when(units_in & (lax.rem(whole, 2) == 1))(lambda: go_down(whole - 1, whole))
        for stage in range(bits + 1, -1, -1):
            item = now - first - AHEAD * stage
            inside = (item >= 0) & (item < items)
            pl.when(inside & (item < units))(functools.partial(scatter_stage, item, 1, stage))
            if stage > 0:
                late = inside & (item >= units + PAUSE)
                pl.when(late)(functools.partial(scatter_stage, item, 0, stage))

        pl.when(whole == chunks + 1)(enter_back)
        pl.when(whole == chunks + 2)(attend_back)
        pl.when(whole == chunks + 3)(leave_back)
        pl.when(whole == chunks + 5)(close)
        for stage in range(bits + 1):
            pl.when(now == vec_first + AHEAD * stage)(functools.partial(vec_stage, stage))
        pl.when(now == vec_first + AHEAD * (bits + 1))(vec_finish)

    last = max(first + items - 1 + AHEAD * (bits + 1), vec_first + AHEAD * (bits + 1))
    lax.fori_loop(0, last + 1, tick, None)

    branch_copy().wait_send()
    norm_copy().wait_send()
    grad_copy().wait_send()
    mlp_copy().wait_send()

    def drain(item, kind):
        given_core(item).wait_send()
        for colour in range(2):
            for stage in range(bits - 1 - kind):
                given_path(item, colour, stage).wait_send()
        given_across(item, kind).wait_send()
        if kind:
            side_copy(item).wait_send()

    repeat(units, lambda item: drain(item, 1))
    repeat(4, lambda item: drain(item + units + PAUSE, 0))


def run_layer(bits, ranks, shards, vec, routes, pic_start, activations, cotangent):
    rows, width = shards[0].shape
    parts = shards[4].shape[1] // width
    chunks = 4 + parts
    depth, breadth, pairs = rows << bits, width * ranks, 1 << (bits - 1)
    seqs, _, full = activations.shape
    caps = routes.shape[1]
    count = seqs * caps
    dma = pltpu.SemaphoreType.DMA
    low = pltpu.VMEM((count, full), BF16)
    turned = pltpu.VMEM((full, count), BF16)
    high = pltpu.VMEM((count, full), F32)
    low_two = pltpu.VMEM((2 * count, full), BF16)
    turned_two = pltpu.VMEM((full, 2 * count), BF16)
    high_two = pltpu.VMEM((2 * count, full), F32)
    return pl.pallas_call(
        functools.partial(layer_kernel, bits, ranks, chunks, parts),
        out_shape=[
            jax.ShapeDtypeStruct((4 + 2 * parts, rows, width), F32),
            jax.ShapeDtypeStruct((8, 128), F32),
            jax.ShapeDtypeStruct((count, full), BF16),
            jax.ShapeDtypeStruct((count, full), BF16),
        ],
        in_specs=[ANY] * 6 + [VMEM] * 2 + [pl.BlockSpec(memory_space=pltpu.SMEM)] + [ANY] * 2,
        out_specs=[VMEM] * 4,
        scratch_shapes=[
            low,
            low,
            pltpu.VMEM((seqs, caps, caps), F32),
            pltpu.VMEM((chunks, depth, breadth), BF16),
            pltpu.VMEM((RING, pairs, rows, breadth), BF16),
            pltpu.VMEM((chunks, 2 * (ranks - 1), rows, width), BF16),
            pltpu.VMEM((1 << bits, 8, 128), F32),
            pltpu.VMEM((1 << bits, 8, 128), F32),
            pltpu.VMEM((1 << bits, 8, 128), F32),
            pltpu.VMEM((ranks - 1, 8, 128), F32),
            pltpu.VMEM((8, full), F32),
            pltpu.VMEM((count, 128), F32),
            low,
            pltpu.VMEM((3, count, full), BF16),
            low,
            high,
            low_two,
            turned_two,
            low_two,
            turned_two,
            low_two,
            low_two,
            high_two,
            high_two,
            high_two,
            low,
            low,
            low,
            low,
            low,
            turned,
            low,
            pltpu.VMEM((3, count, full), BF16),
            high,
            turned,
            pltpu.VMEM((parts, rows, width), BF16),
            pltpu.VMEM((parts, rows, width), BF16),
            dma((chunks,)),
            dma((chunks,)),
            dma((4,)),
            dma((4,)),
            dma((parts,)),
            dma((parts,)),
            dma((chunks,)),
            dma((chunks,)),
            dma((chunks, 2, bits - 1)),
            dma((chunks, 2, bits - 1)),
            dma((chunks,)),
            dma((chunks,)),
            dma((bits,)),
            dma((bits,)),
            dma((chunks + 1,)),
            dma((chunks,)),
            dma((chunks,)),
            dma((chunks, 2, bits - 1)),
            dma((chunks, 2, bits - 1)),
            dma((chunks,)),
            dma((chunks,)),
            dma((bits + 1,)),
            dma((bits + 1,)),
            dma((RING,)),
            *[
                pltpu.VMEM((chunks, 2, pairs >> (stage + 1), rows, breadth // 2), BF16)
                for stage in range(bits - 1)
            ],
        ],
        compiler_params=pltpu.CompilerParams(
            collective_id=1, has_side_effects=True, vmem_limit_bytes=67043328
        ),
        name="layer_kernel",
    )(*shards, vec, routes, pic_start, activations, cotangent)


def put_kernel(seqs, steps, routes, new_rows, new_grads, activations, cotangent, result, grad_input):
    index = pl.program_id(0)
    seq, step = lax.div(index, steps), lax.rem(index, steps)
    size, caps = activations.shape[1], routes.shape[1]
    place = routes[pl.ds(lax.axis_index("tensor") * seqs + seq, 1), :]
    line = lax.broadcasted_iota(jnp.int32, (size, caps), 0) + step * size
    chosen = (line == place).astype(F32)
    routed = jnp.max(chosen, axis=-1, keepdims=True) > 0
    chosen = chosen.astype(BF16)
    for new, base, out in (
        (new_rows, activations, result),
        (new_grads, cotangent, grad_input),
    ):
        placed = contract(chosen, new[...], 1, 0)
        out[0] = jnp.where(routed, placed, base[0].astype(F32)).astype(BF16)


def put_rows(routes, new_rows, new_grads, activations, cotangent):
    seqs, length, full = activations.shape
    caps = routes.shape[1]
    steps = 4
    size = length // steps
    large = pl.BlockSpec((1, size, full), lambda index: (index // steps, index % steps, 0))
    small = pl.BlockSpec((caps, full), lambda index: (index // steps, 0))
    return pl.pallas_call(
        functools.partial(put_kernel, seqs, steps),
        grid=(seqs * steps,),
        out_shape=[jax.ShapeDtypeStruct(activations.shape, BF16)] * 2,
        in_specs=[pl.BlockSpec(routes.shape, lambda index: (0, 0)), small, small, large, large],
        out_specs=[large, large],
        name="put_rows",
    )(routes, new_rows, new_grads, activations, cotangent)


def shards(
    activations,
    routes,
    pic_start,
    router_w,
    gain_attn,
    gain_mlp,
    w_query,
    w_key,
    w_value,
    w_proj,
    w_up,
    w_down,
    cotangent,
):
    ranks = lax.axis_size("tensor")
    bits = lax.axis_size("dp").bit_length() - 1
    rows, width = w_query.shape
    parts = w_up.shape[1] // width
    vec = jnp.stack([router_w, gain_attn, gain_mlp]).astype(F32)
    vec = jnp.pad(vec, ((0, 5), (0, 128 - rows)))
    weights = (w_query, w_key, w_value, w_proj, w_up, w_down)
    sums, small, new_rows, new_grads = run_layer(
        bits, ranks, weights, vec, routes, pic_start, activations, cotangent
    )
    result, grad_input = put_rows(routes, new_rows, new_grads, activations, cotangent)

    def side_by_side(first):
        return jnp.concatenate([sums[first + 2 * part] for part in range(parts)], axis=1)

    return (
        result,
        grad_input,
        small[3, :rows],
        small[4, :rows],
        small[5, :rows],
        sums[0],
        sums[1],
        sums[2],
        sums[3],
        side_by_side(4),
        side_by_side(5),
    )


def solution(mesh):
    both = P(("dp", "tensor"), None, None)
    cut = P("dp", "tensor")
    one = P("dp")
    return jax.shard_map(
        shards,
        mesh=mesh,
        in_specs=(both, P("dp", None), one, one, one, one) + (cut,) * 6 + (both,),
        out_specs=(both, both, one, one, one) + (cut,) * 6,
        check_vma=False,
    )
```

```python
import functools
import math

import jax
import jax.numpy as jnp
from jax import lax
from jax.experimental import pallas as pl
from jax.experimental.pallas import tpu as pltpu
from jax.sharding import PartitionSpec as P

HD = 64
PIC = 256
RING = 8
MESH = pl.DeviceIdType.MESH
ANY = pl.BlockSpec(memory_space=pl.ANY)
VMEM = pl.BlockSpec(memory_space=pltpu.VMEM)
BF16 = jnp.bfloat16
F32 = jnp.float32

inv_root_two = 0.7071067811865476
inv_root_two_pi = 0.3989422804014327


def bit_of(value, bit):
    return lax.rem(lax.div(value, 1 << bit), 2)


def flipped(value, bit):
    return value + (1 - 2 * bit_of(value, bit)) * (1 << bit)


def cleared(value, bits):
    for bit in bits:
        value = value - bit_of(value, bit) * (1 << bit)
    return value


def spread(step, bits):
    value = 0
    for place, bit in enumerate(bits):
        value = value + lax.rem(lax.div(step, 1 << place), 2) * (1 << bit)
    return value


def each(count, body):
    if count <= 4:
        for step in range(count):
            body(jnp.int32(step))
    else:
        lax.fori_loop(0, count, lambda step, _: body(step), None)


def repeat(count, body):
    def step(index, _):
        body(index)

    lax.fori_loop(0, count, step, None)


def span(index, size):
    return pl.ds(pl.multiple_of(index * size, size), size)


def sides(bits):
    return (tuple(range(bits - 1, 1, -1)),) * 2


def orders(bits):
    return (tuple(range(bits - 1, 0, -1)), tuple(range(1, bits)))


def remote(src, dst, send, recv, where):
    return pltpu.make_async_remote_copy(
        src_ref=src, dst_ref=dst, send_sem=send, recv_sem=recv, device_id=where, device_id_type=MESH
    )


def contract(left, right, axis_left, axis_right):
    return lax.dot_general(
        left, right, (((axis_left,), (axis_right,)), ((), ())), preferred_element_type=F32
    )


def layer_kernel(
    bits,
    ranks,
    chunks,
    parts,
    *refs,
):
    shards = refs[:6]
    (
    vec,
    routes,
    pic_start,
    activations,
    cotangent,
    sums,
    vec_sum,
    new_rows,
    new_grads,
    picked,
    grad_rows,
    allowed,
    held,
    from_core,
    from_z,
    vecs,
    grad_vecs,
    vec_path,
    vec_z,
    params,
    gates,
    norm_one,
    qkv,
    context,
    attended,
    norm_two,
    norm_two_t,
    branch,
    branch_t,
    hidden,
    grad_pre,
    mlp,
    grad_two,
    slopes,
    mlp_low,
    grad_low,
    mlp_in,
    grad_in,
    grad_attended,
    grad_attended_t,
    grad_context,
    grad_qkv,
    grad_one,
    norm_one_t,
    side_out,
    side_in,
    send_x,
    recv_x,
    act_out,
    act_in,
    out_x,
    in_x,
    send_z,
    recv_z,
    send_p,
    recv_p,
    send_c,
    recv_c,
    send_v,
    recv_v,
    local,
    out_c,
    in_c,
    out_p,
    in_p,
    out_z,
    in_z,
    out_v,
    in_v,
    fetched,
    *from_path,
    ) = refs[6:]
    me, rank = lax.axis_index("dp"), lax.axis_index("tensor")
    rows, width = shards[0].shape
    count, full = picked.shape
    length = activations.shape[1]
    seqs, caps, _ = allowed.shape
    half = full // 2
    seat, pair = bit_of(me, 0), lax.div(me, 2)
    pairs = 1 << (bits - 1)
    paths = (orders(bits), sides(bits))
    back_paths = tuple(
        tuple(tuple(bit - 1 for bit in order[::-1]) for order in kind) for kind in paths
    )
    side, beside = bit_of(me, 1), flipped(me, 1)
    tile = 32
    block = 256
    blocks = full // block

    barrier = pltpu.get_barrier_semaphore()
    for bit in range(bits):
        pl.semaphore_signal(barrier, 1, device_id=(flipped(me, bit), rank), device_id_type=MESH)
    for hop in range(1, ranks):
        pl.semaphore_signal(
            barrier, 1, device_id=(me, lax.rem(rank + hop, ranks)), device_id_type=MESH
        )
    pl.semaphore_wait(barrier, bits + ranks - 1)

    mine = span(me, rows)
    columns = span(rank, width)

    def shard(chunk, which):
        if chunk < 4:
            return shards[chunk]
        index = which * (parts // 2) + (chunk - 4) // 2
        return shards[4 + chunk % 2].at[:, span(index, width)]

    def keep_own(chunk, source=shards[0]):
        return pltpu.make_async_copy(source, held.at[chunk, mine, columns], local.at[chunk])

    def bulk(chunk, depth, breadth):
        return held.at[chunk, pl.ds(0, depth), pl.ds(0, breadth)]

    def send_z_of(chunk, source, index):
        for hop in range(1, ranks):
            remote(
                source,
                held.at[chunk, span(index, rows), columns],
                send_z.at[chunk],
                recv_z.at[chunk],
                (me, lax.rem(rank + hop, ranks)),
            ).start()

    def x_copy(chunk):
        part = bulk(chunk, rows, width)
        return remote(part, part, send_x.at[chunk], recv_x.at[chunk], (me, rank))

    def start(chunk):
        keep_own(chunk, shard(chunk, side)).start()
        if chunk >= 4:
            remote(
                shard(chunk, 1 - side),
                held.at[chunk, mine, columns],
                send_x.at[chunk],
                recv_x.at[chunk],
                (beside, rank),
            ).start()

    def start_z(chunk):
        if chunk >= 4:
            x_copy(chunk).wait_recv()
            send_z_of(chunk, held.at[chunk, span(beside, rows), columns], beside)
        send_z_of(chunk, shard(chunk, side), me)

    def z_copy(chunk, kind):
        part = bulk(chunk, rows << kind, width * (ranks - 1))
        return remote(part, part, send_z.at[chunk], recv_z.at[chunk], (me, rank))

    def send_path(chunk, kind, colour, stage):
        order = paths[kind][colour]
        earlier = order[:stage] + (1,) * kind
        other = (flipped(me, order[stage]), rank)

        def send(step):
            index = cleared(me, earlier) + spread(step, earlier)
            part = held.at[chunk, span(index, rows), pl.ds(colour * half, half)]
            remote(
                part,
                part,
                send_p.at[chunk, colour, stage],
                recv_p.at[chunk, colour, stage],
                other,
            ).start()

        each(1 << len(earlier), send)

    def path_copy(chunk, kind, colour, stage):
        part = bulk(chunk, rows << (stage + kind), half)
        return remote(
            part,
            part,
            send_p.at[chunk, colour, stage],
            recv_p.at[chunk, colour, stage],
            (me, rank),
        )

    def send_core(chunk):
        other = (flipped(me, 0), rank)

        def send(step):
            part = held.at[chunk, span(2 * step + seat, rows)]
            remote(part, part, send_c.at[chunk], recv_c.at[chunk], other).start()

        each(pairs, send)

    def core_copy(chunk):
        part = bulk(chunk, rows << (bits - 1), full)
        return remote(part, part, send_c.at[chunk], recv_c.at[chunk], (me, rank))

    def all_sent(chunk, kind):
        z_copy(chunk, kind).wait_send()
        if kind:
            x_copy(chunk).wait_send()
        for colour in range(2):
            for stage in range(bits - 1 - kind):
                path_copy(chunk, kind, colour, stage).wait_send()
        core_copy(chunk).wait_send()

    def gather_stage(chunk, kind, stage):
        if stage < kind:
            return
        if stage == kind:
            keep_own(chunk).wait()
            z_copy(chunk, kind).wait_recv()
        elif stage < bits:
            for colour in range(2):
                path_copy(chunk, kind, colour, stage - 1 - kind).wait_recv()
        else:
            core_copy(chunk).wait_recv()
        if stage < bits - 1:
            for colour in range(2):
                send_path(chunk, kind, colour, stage - kind)
        elif stage == bits - 1:
            send_core(chunk)

    units = chunks - 4

    def turn(item):
        return item

    def slot(item):
        return item + 4 if item < units else (item - units + 3) % 4

    def give_core(item):
        def send(step):
            remote(
                held.at[slot(item), span(2 * step + 1 - seat, rows)],
                from_core.at[turn(item) % RING, step],
                out_c.at[turn(item)],
                in_c.at[turn(item)],
                (flipped(me, 0), rank),
            ).start()

        each(pairs, send)

    def given_core(item):
        part = from_core.at[turn(item) % RING]
        return remote(part, part, out_c.at[turn(item)], in_c.at[turn(item)], (me, rank))

    def add_to(item, index, where, source):
        step = min(rows, tile)
        for start in range(0, rows, step):
            place = pl.ds(pl.multiple_of((2 * index + seat) * rows, rows) + start, step)
            here = held.at[slot(item), place, where]
            here[...] = (
                here[...].astype(F32) + source[pl.ds(start, step)].astype(F32)
            ).astype(BF16)

    def add_core(item):
        repeat(
            pairs,
            lambda step: add_to(
                item, step, pl.ds(0, full), from_core.at[turn(item) % RING, step]
            ),
        )

    def members(kind, colour, stage, step, kept):
        order = back_paths[kind][colour]
        later = order[stage + 1 :] + (0,) * kind
        index = pair if kept else flipped(pair, order[stage])
        return cleared(index, later) + spread(step, later)

    def give_path(item, kind, colour, stage):
        other = (2 * flipped(pair, back_paths[kind][colour][stage]) + seat, rank)

        def send(step):
            index = members(kind, colour, stage, step, False)
            remote(
                held.at[
                    slot(item), span(2 * index + seat, rows), pl.ds(colour * half, half)
                ],
                from_path[stage].at[turn(item), colour, step],
                out_p.at[turn(item), colour, stage],
                in_p.at[turn(item), colour, stage],
                other,
            ).start()

        each(pairs >> (stage + 1), send)

    def given_path(item, colour, stage):
        part = from_path[stage].at[turn(item), colour]
        return remote(
            part,
            part,
            out_p.at[turn(item), colour, stage],
            in_p.at[turn(item), colour, stage],
            (me, rank),
        )

    def add_path(item, kind, colour, stage):
        repeat(
            pairs >> (stage + 1),
            lambda step: add_to(
                item,
                members(kind, colour, stage, step, True),
                pl.ds(colour * half, half),
                from_path[stage].at[turn(item), colour, step],
            ),
        )

    def give_across(item, kind):
        for hop in range(1, ranks):
            to = lax.rem(rank + hop, ranks)
            for which in range(1 + kind):
                remote(
                    held.at[slot(item), span((me, beside)[which], rows), span(to, width)],
                    from_z.at[turn(item), (hop - 1) * (1 + kind) + which],
                    out_z.at[turn(item)],
                    in_z.at[turn(item)],
                    (me, to),
                ).start()

    def given_across(item, kind):
        part = from_z.at[turn(item), pl.ds(0, (ranks - 1) * (1 + kind))]
        return remote(part, part, out_z.at[turn(item)], in_z.at[turn(item)], (me, rank))

    def total_of(item, kind, which):
        total = held[slot(item), span((me, beside)[which], rows), columns].astype(F32)
        for hop in range(1, ranks):
            total = total + from_z[turn(item), (hop - 1) * (1 + kind) + which].astype(F32)
        return total

    def unit_place(item, which):
        return 4 + 2 * (which * (parts // 2) + item // 2) + item % 2

    def side_copy(item):
        return remote(
            side_out.at[item], side_in.at[item], out_x.at[item], in_x.at[item], (beside, rank)
        )

    def scatter_stage(item, kind, stage):
        if stage == 1:
            given_core(item).wait_recv()
            add_core(item)
        elif 1 < stage <= bits - kind:
            for colour in range(2):
                given_path(item, colour, stage - 2).wait_recv()
                add_path(item, kind, colour, stage - 2)
        elif stage == bits - kind + 1:
            given_across(item, kind).wait_recv()
            if kind:
                side_out[item] = total_of(item, kind, 1).astype(BF16)
                side_copy(item).start()
                sums[unit_place(item, side)] = total_of(item, kind, 0)
            else:
                sums[slot(item)] = total_of(item, kind, 0)
        elif stage == bits - kind + 2:
            side_copy(item).wait_recv()
            sums[unit_place(item, 1 - side)] = side_in[item].astype(F32)
        if stage == 0:
            give_core(item)
        elif stage < bits - kind:
            for colour in range(2):
                give_path(item, kind, colour, stage - 1)
        elif stage == bits - kind:
            give_across(item, kind)

    vec_ways = tuple(range(bits - 1, -1, -1))

    def vec_gather(stage):
        if stage > 0:
            part = vecs.at[pl.ds(0, 1 << (stage - 1))]
            remote(part, part, send_v.at[stage - 1], recv_v.at[stage - 1], (me, rank)).wait()
        if stage < bits:

            def send(step):
                index = cleared(me, vec_ways[:stage]) + spread(step, vec_ways[:stage])
                remote(
                    vecs.at[index],
                    vecs.at[index],
                    send_v.at[stage],
                    recv_v.at[stage],
                    (flipped(me, vec_ways[stage]), rank),
                ).start()

            each(1 << stage, send)

    def spell_params():
        params[...] = jnp.zeros_like(params)
        lane = lax.broadcasted_iota(jnp.int32, (128, full), 0)
        column = lax.broadcasted_iota(jnp.int32, (128, full), 1)

        def place(index):
            chosen = ((lane < rows) & (column == index * rows + lane)).astype(F32).astype(BF16)
            params[...] += contract(vecs[index].astype(BF16), chosen, 1, 0)

        if rows == 128:
            for index in range(1 << bits):
                params[:, index * rows : (index + 1) * rows] = vecs[index]
        else:
            repeat(1 << bits, place)

    vec_path_of = tuple(range(bits))

    def vec_stage(stage):
        if stage > 0:
            earlier = vec_path_of[stage:]
            amount = 1 << len(earlier)
            part = vec_path.at[pl.ds(amount - 1, amount)]
            remote(part, part, out_v.at[stage - 1], in_v.at[stage - 1], (me, rank)).wait()

            def add(step):
                index = cleared(me, earlier) + spread(step, earlier)
                grad_vecs[index] = grad_vecs[index] + vec_path[amount - 1 + step]

            repeat(amount, add)
        if stage < bits:
            bit, later = vec_path_of[stage], vec_path_of[stage + 1 :]
            amount = 1 << len(later)

            def send(step):
                index = cleared(flipped(me, bit), later) + spread(step, later)
                remote(
                    grad_vecs.at[index],
                    vec_path.at[amount - 1 + step],
                    out_v.at[stage],
                    in_v.at[stage],
                    (flipped(me, bit), rank),
                ).start()

            each(amount, send)
        else:
            for hop in range(1, ranks):
                to = (me, lax.rem(rank + hop, ranks))
                remote(
                    grad_vecs.at[me], vec_z.at[hop - 1], out_v.at[bits], in_v.at[bits], to
                ).start()

    def vec_finish():
        remote(vec_z, vec_z, out_v.at[bits], in_v.at[bits], (me, rank)).wait()
        total = grad_vecs[me]
        for hop in range(1, ranks):
            total = total + vec_z[hop - 1]
        vec_sum[...] = total

    def router():
        return params[0:1, :]

    def gain_one():
        return params[1:2, :]

    def gain_two():
        return params[2:3, :]

    def by_rows(body):
        repeat(count // tile, lambda index: body(span(index, tile)))

    def by_blocks(body):
        repeat(blocks, lambda index: body(span(index, block)))

    def inverse_of(values):
        return lax.rsqrt(jnp.mean(values * values, axis=-1, keepdims=True) + 1e-06)

    def wide(values):
        return jnp.broadcast_to(values, (values.shape[0], 128))

    def transpose_to(target, source, first=0):
        def turn_over(index):
            part = span(index, 128)
            values = source[first : first + count, part].astype(F32)
            target[part, first : first + count] = values.T.astype(BF16)

        repeat(full // 128, turn_over)

    def to_beside(which, source, target):
        return remote(source, target, act_out.at[which], act_in.at[which], (beside, rank))

    own_rows, their_rows = pl.ds(0, count), pl.ds(count, count)

    def branch_copy():
        return to_beside(0, branch.at[own_rows], branch.at[their_rows])

    def norm_copy():
        return to_beside(1, norm_two.at[own_rows], norm_two.at[their_rows])

    def grad_copy():
        return to_beside(2, grad_low, grad_in)

    def mlp_copy():
        return to_beside(3, mlp_low, mlp_in)

    slab = pairs * rows
    halves = length // slab

    def fetch(source, seq, step, place):
        def copy(index):
            pltpu.make_async_copy(
                source.at[seq, pl.ds(pl.multiple_of(index * rows, rows) + step * slab, rows)],
                from_core.at[place, index],
                fetched.at[place],
            ).start()

        each(pairs, copy)

    def down_and_across(seq):
        across = routes[pl.ds(rank * seqs + seq, 1), :].astype(F32)
        return jnp.broadcast_to(across, (caps, caps)).T, across

    def mask(seq):
        down, across = down_and_across(seq)
        begin = pic_start[rank * seqs + seq].astype(F32)
        inside_down = (down >= begin) & (down < begin + PIC)
        inside_across = (across >= begin) & (across < begin + PIC)
        seen = (across <= down) | (inside_down & inside_across)
        allowed[seq] = seen.astype(F32)

    def pick(target, seq, place):
        down, _ = down_and_across(seq)
        column = lax.broadcasted_iota(jnp.int32, (caps, slab), 1).astype(F32)
        for step in range(halves):
            pltpu.make_async_copy(
                from_core.at[place + step], from_core.at[place + step], fetched.at[place + step]
            ).wait()

        def body(part):
            total = 0.0
            for step in range(halves):
                chosen = (down[:, 0:1] == column + step * slab).astype(F32).astype(BF16)
                source = from_core[place + step, :, :, part].reshape(slab, block)
                total = total + contract(chosen, source, 1, 0)
            target[pl.ds(seq * caps, caps), part] = total.astype(BF16)

        by_blocks(body)

    def prepare():
        def body(part):
            values = picked[part].astype(F32)
            logit = jnp.sum(values * router(), axis=-1, keepdims=True)
            gate = 1.0 / (1.0 + jnp.exp(-logit))
            gates[part] = wide(gate)
            norm_one[part] = (values * inverse_of(values) * gain_one()).astype(BF16)
            branch[part] = (gate * grad_rows[part].astype(F32)).astype(BF16)

        by_rows(body)
        transpose_to(branch_t, branch)

    def send_branch():
        branch_copy().start()

    def project(which):
        def body(part):
            qkv[which, :, part] = contract(norm_one[...], held[which, :, part], 1, 0).astype(BF16)

        by_blocks(body)

    lanes = lax.broadcasted_iota(jnp.int32, (1, 2 * HD), 1)

    def own_lanes(values, head):
        inside = (lanes < HD) if head == 0 else (lanes >= HD)
        return jnp.where(inside, values, jnp.zeros_like(values))

    def probabilities(seq, queries, keys, head):
        scores = contract(own_lanes(queries, head), keys, 1, 1) * (1.0 / math.sqrt(HD))
        scores = jnp.where(allowed[seq] > 0, scores, -1e30)
        powers = jnp.exp(scores - jnp.max(scores, axis=-1, keepdims=True))
        return powers / jnp.sum(powers, axis=-1, keepdims=True)

    def attend():
        def body(index):
            part = span(index, 2 * HD)
            for seq in range(seqs):
                place = pl.ds(seq * caps, caps)
                queries, keys = qkv[0, place, part], qkv[1, place, part]
                values = qkv[2, place, part]
                total = 0.0
                for head in range(2):
                    probs = probabilities(seq, queries, keys, head).astype(BF16)
                    total = total + contract(probs, own_lanes(values, head), 1, 0)
                context[place, part] = total.astype(BF16)

        repeat(full // (2 * HD), body)

    def leave_attention():
        def body(part):
            attended[:, part] = contract(context[...], held[3, part, :], 1, 1)

        by_blocks(body)

        def rest(part):
            values = picked[part].astype(F32) + attended[part]
            norm_two[part] = (values * inverse_of(values) * gain_two()).astype(BF16)

        by_rows(rest)
        norm_copy().start()
        transpose_to(norm_two_t, norm_two)
        mlp[...] = jnp.zeros_like(mlp)
        grad_two[...] = jnp.zeros_like(grad_two)

    def by_lines(body):
        repeat(2 * blocks, lambda i: body(span(lax.rem(i, 2), count), span(lax.div(i, 2), block)))

    def go_up(up):
        if up == 4:
            norm_copy().wait_recv()
            transpose_to(norm_two_t, norm_two, count)

        def units_of(lines, part):
            pre = contract(norm_two[lines], held[up, :, part], 1, 0)
            bell = 0.5 * (1.0 + lax.erf(pre * inv_root_two))
            slopes[lines, part] = bell + pre * jnp.exp(-0.5 * pre * pre) * inv_root_two_pi
            hidden[lines, part] = (pre * bell).astype(BF16)

        by_lines(units_of)

    def go_down(up, down):
        if up == 4:
            branch_copy().wait_recv()
            transpose_to(branch_t, branch, count)

        def units_of(lines, part):
            grad_hidden = contract(branch[lines], held[down, :, part], 1, 0)
            grad_pre[lines, part] = (grad_hidden * slopes[lines, part]).astype(BF16)

        by_lines(units_of)

        def add_out(target, source, weight, lines):
            def body(part):
                target[lines, part] += contract(source[lines], held[weight, part, :], 1, 1)

            by_blocks(body)

        def pass_on(source, target, copy):
            if down == chunks - 1:

                def body(part):
                    target[part] = source[pl.ds(part.start + count, tile)].astype(BF16)

                by_rows(body)
                copy().start()

        add_out(grad_two, grad_pre, up, their_rows)
        pass_on(grad_two, grad_low, grad_copy)
        add_out(mlp, hidden, down, their_rows)
        pass_on(mlp, mlp_low, mlp_copy)
        add_out(grad_two, grad_pre, up, own_rows)
        add_out(mlp, hidden, down, own_rows)
        all_sent(up, 1)
        all_sent(down, 1)

        def gradients(part):
            held[down, :, part] = contract(branch_t[...], hidden[:, part], 1, 0).astype(BF16)
            held[up, :, part] = contract(norm_two_t[...], grad_pre[:, part], 1, 0).astype(BF16)

        by_blocks(gradients)

    small = params

    def enter_back():
        small[3:6, :] = jnp.zeros((3, full), F32)
        grad_copy().wait_recv()

        def body(part):
            values = picked[part].astype(F32)
            residual = values + attended[part]
            inverse = inverse_of(residual)
            grad = grad_two[part] + grad_in[part].astype(F32)
            small[5:6, :] += jnp.sum(grad * residual * inverse, axis=0, keepdims=True)
            scaled = grad * gain_two()
            mean = jnp.mean(scaled * residual, axis=-1, keepdims=True)
            grad_mid = inverse * scaled - residual * (inverse * inverse * inverse * mean)
            grad_two[part] = grad_mid
            rows_in = grad_rows[part].astype(F32)
            grad_attended[part] = (gates[part, 0:1] * rows_in + grad_mid).astype(BF16)

        by_rows(body)
        transpose_to(grad_attended_t, grad_attended)

        def through(part):
            grad_context[:, part] = contract(grad_attended[...], held[3, :, part], 1, 0).astype(BF16)

        by_blocks(through)
        for chunk in range(4):
            all_sent(chunk, 0)

        def weights(part):
            held[3, :, part] = contract(grad_attended_t[...], context[:, part], 1, 0).astype(BF16)

        by_blocks(weights)

    def recall():
        def body(index):
            part = span(index, 2 * HD)
            for seq in range(seqs):
                place = pl.ds(seq * caps, caps)
                queries, keys = qkv[0, place, part], qkv[1, place, part]
                for head in range(2):
                    slopes[pl.ds((2 * seq + head) * caps, caps), part] = probabilities(
                        seq, queries, keys, head
                    )

        repeat(full // (2 * HD), body)

    def attend_back():
        def body(index):
            part = span(index, 2 * HD)
            for seq in range(seqs):
                place = pl.ds(seq * caps, caps)
                queries, keys = qkv[0, place, part], qkv[1, place, part]
                values, grad = qkv[2, place, part], grad_context[place, part]
                grad_q, grad_k, grad_v = 0.0, 0.0, 0.0
                for head in range(2):
                    probs = slopes[pl.ds((2 * seq + head) * caps, caps), part]
                    grad_probs = contract(own_lanes(grad, head), values, 1, 1)
                    inner = jnp.sum(probs * grad_probs, axis=-1, keepdims=True)
                    grad_scores = (probs * (grad_probs - inner)).astype(BF16)
                    low = probs.astype(BF16)
                    grad_v = grad_v + contract(low, own_lanes(grad, head), 0, 0)
                    grad_q = grad_q + contract(grad_scores, own_lanes(keys, head), 1, 0)
                    grad_k = grad_k + contract(grad_scores, own_lanes(queries, head), 0, 0)
                scale = 1.0 / math.sqrt(HD)
                grad_qkv[0, place, part] = (grad_q * scale).astype(BF16)
                grad_qkv[1, place, part] = (grad_k * scale).astype(BF16)
                grad_qkv[2, place, part] = grad_v.astype(BF16)

        repeat(full // (2 * HD), body)

    def leave_back():
        def through(part):
            total = contract(grad_qkv[0], held[0, part, :], 1, 1)
            for which in (1, 2):
                total = total + contract(grad_qkv[which], held[which, part, :], 1, 1)
            grad_one[:, part] = total

        by_blocks(through)

    def weigh_back():
        transpose_to(norm_one_t, norm_one)

        def weights(part):
            for which in range(3):
                held[which, :, part] = contract(norm_one_t[...], grad_qkv[which, :, part], 1, 0).astype(
                    BF16
                )

        by_blocks(weights)

    def close():
        mlp_copy().wait_recv()

        def body(part):
            values = picked[part].astype(F32)
            rows_in = grad_rows[part].astype(F32)
            gate = gates[part, 0:1]
            delta = attended[part] + (mlp[part] + mlp_in[part].astype(F32))
            new_rows[part] = (values + gate * delta).astype(BF16)
            score = jnp.sum(rows_in * delta, axis=-1, keepdims=True) * gate * (1.0 - gate)
            small[3:4, :] += jnp.sum(score * values, axis=0, keepdims=True)
            inverse = inverse_of(values)
            grad = grad_one[part]
            small[4:5, :] += jnp.sum(grad * values * inverse, axis=0, keepdims=True)
            scaled = grad * gain_one()
            mean = jnp.mean(scaled * values, axis=-1, keepdims=True)
            grad_norm = inverse * scaled - values * (inverse * inverse * inverse * mean)
            total = rows_in + grad_two[part] + grad_norm + score * router()
            new_grads[part] = total.astype(BF16)

        by_rows(body)
        own = small[...]
        if rows == 128:
            for index in range(1 << bits):
                grad_vecs[index] = own[:, index * rows : (index + 1) * rows]
        else:
            column = lax.broadcasted_iota(jnp.int32, (full, 128), 0)
            lane = lax.broadcasted_iota(jnp.int32, (full, 128), 1)

            def place(index):
                chosen = ((lane < rows) & (column == index * rows + lane)).astype(F32)
                grad_vecs[index] = jnp.dot(
                    own, chosen, precision=lax.Precision.HIGHEST, preferred_element_type=F32
                )

            repeat(1 << bits, place)

    keep_vec = pltpu.make_async_copy(vec, vecs.at[me], local.at[chunks])
    keep_vec.start()
    for chunk in range(4):
        start(chunk)
        start_z(chunk)
    for chunk in range(4, chunks):
        start(chunk)
    for which, source in enumerate((activations, cotangent)):
        for seq in range(seqs):
            for step in range(halves):
                fetch(source, seq, step, (which * seqs + seq) * halves + step)
    keep_vec.wait()
    vec_gather(0)

    events = []

    def at(when, what, *args):
        events.append((when, len(events), functools.partial(what, *args)))

    def between(first, last, step, steps):
        return first + (last - first) * step / max(steps, 1)

    for stage in range(1, bits + 1):
        at(3.8 + 2.2 * stage, vec_gather, stage)
    for seq in range(seqs):
        at(9 + seq, mask, seq)
        for which, target in enumerate((picked, grad_rows)):
            at(9 + seq, pick, target, seq, (which * seqs + seq) * halves)
    for chunk in range(4, chunks):
        at(7.5, start_z, chunk)
    at(3.8 + 2.2 * bits + 3.2, spell_params)
    at(3.8 + 2.2 * bits + 3.2, prepare)
    weights_in = [33 + 8.5 * chunk for chunk in range(4)] + [
        71 + 11.2 * chunk for chunk in range(units)
    ]
    for chunk in range(chunks):
        kind = int(chunk >= 4)
        opened = (54 + 8.3 * (chunk - 4)) if kind else (13 + 8.5 * chunk)
        for stage in range(kind, bits):
            when = between(opened, weights_in[chunk] - 4, stage - kind, bits - 1 - kind)
            at(when, gather_stage, chunk, kind, stage)
        at(weights_in[chunk], gather_stage, chunk, kind, bits)
    for chunk in range(3):
        at(weights_in[chunk], project, chunk)
    at(47, send_branch)
    at(weights_in[2], attend)
    at(weights_in[3], leave_attention)
    for item in range(0, units, 2):
        up, down = item + 4, item + 5
        at(max(weights_in[up], 74) + 0.1, go_up, up)
        ready = weights_in[down] + 0.1
        at(ready, go_down, up, down)
        for one in (item, item + 1):
            at(ready, give_core, one)
    at(116.5, recall)
    at(120, enter_back)
    at(120, give_core, units)
    at(126, attend_back)
    at(134, leave_back)
    at(134, close)
    at(134.2, weigh_back)
    for item in range(units + 1, chunks):
        at(134.3, give_core, item)
    summed = [
        (93.1, 115, 116, 147, 178),
        (93.1, 123, 124, 147.1, 178),
        (115, 132, 133, 148, 178),
        (115.1, 145, 146, 172, 184),
        (125, 152, 163, 170, 0),
        (143, 158, 168, 175, 0),
        (143.2, 164, 174, 181, 0),
        (143.3, 170, 180, 187, 0),
    ]
    for item, (core_in, second, last, across, aside) in enumerate(summed):
        kind = int(item < units)
        final = bits - kind
        at(core_in, scatter_stage, item, kind, 1)
        for stage in range(2, final + 1):
            when = last if final == 2 else between(second, last, stage - 2, final - 2)
            at(when, scatter_stage, item, kind, stage)
        at(across, scatter_stage, item, kind, final + 1)
        if kind:
            at(aside, scatter_stage, item, kind, final + 2)
    for stage in range(bits + 1):
        when = (134.1, 142.9, 143.1, 164.5)[stage] if stage < 4 else 164.5 + 2 * stage
        at(when, vec_stage, stage)
    at(188, vec_finish)
    for _, _, event in sorted(events, key=lambda event: event[:2]):
        event()

    branch_copy().wait_send()
    norm_copy().wait_send()
    grad_copy().wait_send()
    mlp_copy().wait_send()

    def drain(item, kind):
        given_core(item).wait_send()
        for colour in range(2):
            for stage in range(bits - 1 - kind):
                given_path(item, colour, stage).wait_send()
        given_across(item, kind).wait_send()
        if kind:
            side_copy(item).wait_send()

    for item in range(chunks):
        drain(item, int(item < units))


def run_layer(bits, ranks, shards, vec, routes, pic_start, activations, cotangent):
    rows, width = shards[0].shape
    parts = shards[4].shape[1] // width
    chunks = 4 + parts
    depth, breadth, pairs = rows << bits, width * ranks, 1 << (bits - 1)
    seqs, _, full = activations.shape
    caps = routes.shape[1]
    count = seqs * caps
    dma = pltpu.SemaphoreType.DMA
    low = pltpu.VMEM((count, full), BF16)
    turned = pltpu.VMEM((full, count), BF16)
    high = pltpu.VMEM((count, full), F32)
    low_two = pltpu.VMEM((2 * count, full), BF16)
    turned_two = pltpu.VMEM((full, 2 * count), BF16)
    high_two = pltpu.VMEM((2 * count, full), F32)
    return pl.pallas_call(
        functools.partial(layer_kernel, bits, ranks, chunks, parts),
        out_shape=[
            jax.ShapeDtypeStruct((4 + 2 * parts, rows, width), F32),
            jax.ShapeDtypeStruct((8, 128), F32),
            jax.ShapeDtypeStruct((count, full), BF16),
            jax.ShapeDtypeStruct((count, full), BF16),
        ],
        in_specs=[ANY] * 6 + [VMEM] * 2 + [pl.BlockSpec(memory_space=pltpu.SMEM)] + [ANY] * 2,
        out_specs=[VMEM] * 4,
        scratch_shapes=[
            low,
            low,
            pltpu.VMEM((seqs, caps, caps), F32),
            pltpu.VMEM((chunks, depth, breadth), BF16),
            pltpu.VMEM((RING, pairs, rows, breadth), BF16),
            pltpu.VMEM((chunks, 2 * (ranks - 1), rows, width), BF16),
            pltpu.VMEM((1 << bits, 8, 128), F32),
            pltpu.VMEM((1 << bits, 8, 128), F32),
            pltpu.VMEM((1 << bits, 8, 128), F32),
            pltpu.VMEM((ranks - 1, 8, 128), F32),
            pltpu.VMEM((8, full), F32),
            pltpu.VMEM((count, 128), F32),
            low,
            pltpu.VMEM((3, count, full), BF16),
            low,
            high,
            low_two,
            turned_two,
            low_two,
            turned_two,
            low_two,
            low_two,
            high_two,
            high_two,
            high_two,
            low,
            low,
            low,
            low,
            low,
            turned,
            low,
            pltpu.VMEM((3, count, full), BF16),
            high,
            turned,
            pltpu.VMEM((parts, rows, width), BF16),
            pltpu.VMEM((parts, rows, width), BF16),
            dma((chunks,)),
            dma((chunks,)),
            dma((4,)),
            dma((4,)),
            dma((parts,)),
            dma((parts,)),
            dma((chunks,)),
            dma((chunks,)),
            dma((chunks, 2, bits - 1)),
            dma((chunks, 2, bits - 1)),
            dma((chunks,)),
            dma((chunks,)),
            dma((bits,)),
            dma((bits,)),
            dma((chunks + 1,)),
            dma((chunks,)),
            dma((chunks,)),
            dma((chunks, 2, bits - 1)),
            dma((chunks, 2, bits - 1)),
            dma((chunks,)),
            dma((chunks,)),
            dma((bits + 1,)),
            dma((bits + 1,)),
            dma((RING,)),
            *[
                pltpu.VMEM((chunks, 2, pairs >> (stage + 1), rows, breadth // 2), BF16)
                for stage in range(bits - 1)
            ],
        ],
        compiler_params=pltpu.CompilerParams(
            collective_id=1, has_side_effects=True, vmem_limit_bytes=67043328
        ),
        name="layer_kernel",
    )(*shards, vec, routes, pic_start, activations, cotangent)


def put_kernel(seqs, steps, routes, new_rows, new_grads, activations, cotangent, result, grad_input):
    index = pl.program_id(0)
    seq, step = lax.div(index, steps), lax.rem(index, steps)
    size, caps = activations.shape[1], routes.shape[1]
    place = routes[pl.ds(lax.axis_index("tensor") * seqs + seq, 1), :]
    line = lax.broadcasted_iota(jnp.int32, (size, caps), 0) + step * size
    chosen = (line == place).astype(F32)
    routed = jnp.max(chosen, axis=-1, keepdims=True) > 0
    chosen = chosen.astype(BF16)
    for new, base, out in (
        (new_rows, activations, result),
        (new_grads, cotangent, grad_input),
    ):
        placed = contract(chosen, new[...], 1, 0)
        out[0] = jnp.where(routed, placed, base[0].astype(F32)).astype(BF16)


def put_rows(routes, new_rows, new_grads, activations, cotangent):
    seqs, length, full = activations.shape
    caps = routes.shape[1]
    steps = 4
    size = length // steps
    large = pl.BlockSpec((1, size, full), lambda index: (index // steps, index % steps, 0))
    small = pl.BlockSpec((caps, full), lambda index: (index // steps, 0))
    return pl.pallas_call(
        functools.partial(put_kernel, seqs, steps),
        grid=(seqs * steps,),
        out_shape=[jax.ShapeDtypeStruct(activations.shape, BF16)] * 2,
        in_specs=[pl.BlockSpec(routes.shape, lambda index: (0, 0)), small, small, large, large],
        out_specs=[large, large],
        name="put_rows",
    )(routes, new_rows, new_grads, activations, cotangent)


def shards(
    activations,
    routes,
    pic_start,
    router_w,
    gain_attn,
    gain_mlp,
    w_query,
    w_key,
    w_value,
    w_proj,
    w_up,
    w_down,
    cotangent,
):
    ranks = lax.axis_size("tensor")
    bits = lax.axis_size("dp").bit_length() - 1
    rows, width = w_query.shape
    parts = w_up.shape[1] // width
    vec = jnp.stack([router_w, gain_attn, gain_mlp]).astype(F32)
    vec = jnp.pad(vec, ((0, 5), (0, 128 - rows)))
    weights = (w_query, w_key, w_value, w_proj, w_up, w_down)
    sums, small, new_rows, new_grads = run_layer(
        bits, ranks, weights, vec, routes, pic_start, activations, cotangent
    )
    result, grad_input = put_rows(routes, new_rows, new_grads, activations, cotangent)

    def side_by_side(first):
        return jnp.concatenate([sums[first + 2 * part] for part in range(parts)], axis=1)

    return (
        result,
        grad_input,
        small[3, :rows],
        small[4, :rows],
        small[5, :rows],
        sums[0],
        sums[1],
        sums[2],
        sums[3],
        side_by_side(4),
        side_by_side(5),
    )


def solution(mesh):
    both = P(("dp", "tensor"), None, None)
    cut = P("dp", "tensor")
    one = P("dp")
    return jax.shard_map(
        shards,
        mesh=mesh,
        in_specs=(both, P("dp", None), one, one, one, one) + (cut,) * 6 + (both,),
        out_specs=(both, both, one, one, one) + (cut,) * 6,
        check_vma=False,
    )
```

```python
import functools
import math

import jax
import jax.numpy as jnp
from jax import lax
from jax.experimental import pallas as pl
from jax.experimental.pallas import tpu as pltpu
from jax.sharding import PartitionSpec as P

HD = 64
PIC = 256
RING = 8
MESH = pl.DeviceIdType.MESH
ANY = pl.BlockSpec(memory_space=pl.ANY)
VMEM = pl.BlockSpec(memory_space=pltpu.VMEM)
BF16 = jnp.bfloat16
F32 = jnp.float32

inv_root_two = 0.7071067811865476
inv_root_two_pi = 0.3989422804014327


def bit_of(value, bit):
    return lax.rem(lax.div(value, 1 << bit), 2)


def flipped(value, bit):
    return value + (1 - 2 * bit_of(value, bit)) * (1 << bit)


def cleared(value, bits):
    for bit in bits:
        value = value - bit_of(value, bit) * (1 << bit)
    return value


def spread(step, bits):
    value = 0
    for place, bit in enumerate(bits):
        value = value + lax.rem(lax.div(step, 1 << place), 2) * (1 << bit)
    return value


def each(count, body):
    if count <= 4:
        for step in range(count):
            body(jnp.int32(step))
    else:
        lax.fori_loop(0, count, lambda step, _: body(step), None)


def repeat(count, body):
    def step(index, _):
        body(index)

    lax.fori_loop(0, count, step, None)


def span(index, size):
    return pl.ds(pl.multiple_of(index * size, size), size)


def sides(bits):
    return (tuple(range(bits - 1, 1, -1)),) * 2


def orders(bits):
    return (tuple(range(bits - 1, 0, -1)), tuple(range(1, bits)))


def remote(src, dst, send, recv, where):
    return pltpu.make_async_remote_copy(
        src_ref=src, dst_ref=dst, send_sem=send, recv_sem=recv, device_id=where, device_id_type=MESH
    )


def contract(left, right, axis_left, axis_right):
    return lax.dot_general(
        left, right, (((axis_left,), (axis_right,)), ((), ())), preferred_element_type=F32
    )


def layer_kernel(
    bits,
    ranks,
    chunks,
    parts,
    *refs,
):
    shards = refs[:6]
    (
    vec,
    routes,
    pic_start,
    activations,
    cotangent,
    sums,
    vec_sum,
    new_rows,
    new_grads,
    picked,
    grad_rows,
    allowed,
    held,
    from_core,
    from_z,
    vecs,
    grad_vecs,
    vec_path,
    vec_z,
    params,
    gates,
    norm_one,
    qkv,
    context,
    attended,
    norm_two,
    norm_two_t,
    branch,
    branch_t,
    hidden,
    grad_pre,
    mlp,
    grad_two,
    slopes,
    mlp_low,
    grad_low,
    mlp_in,
    grad_in,
    grad_attended,
    grad_attended_t,
    grad_context,
    grad_qkv,
    grad_one,
    norm_one_t,
    side_out,
    side_in,
    send_x,
    recv_x,
    act_out,
    act_in,
    out_x,
    in_x,
    send_z,
    recv_z,
    send_p,
    recv_p,
    send_c,
    recv_c,
    send_v,
    recv_v,
    local,
    out_c,
    in_c,
    out_p,
    in_p,
    out_z,
    in_z,
    out_v,
    in_v,
    fetched,
    *from_path,
    ) = refs[6:]
    me, rank = lax.axis_index("dp"), lax.axis_index("tensor")
    rows, width = shards[0].shape
    count, full = picked.shape
    length = activations.shape[1]
    seqs, caps, _ = allowed.shape
    half = full // 2
    seat, pair = bit_of(me, 0), lax.div(me, 2)
    pairs = 1 << (bits - 1)
    paths = (orders(bits), sides(bits))
    back_paths = tuple(
        tuple(tuple(bit - 1 for bit in order[::-1]) for order in kind) for kind in paths
    )
    side, beside = bit_of(me, 1), flipped(me, 1)
    tile = 32
    block = 256
    blocks = full // block

    barrier = pltpu.get_barrier_semaphore()
    for bit in range(bits):
        pl.semaphore_signal(barrier, 1, device_id=(flipped(me, bit), rank), device_id_type=MESH)
    for hop in range(1, ranks):
        pl.semaphore_signal(
            barrier, 1, device_id=(me, lax.rem(rank + hop, ranks)), device_id_type=MESH
        )
    pl.semaphore_wait(barrier, bits + ranks - 1)

    mine = span(me, rows)
    columns = span(rank, width)

    def shard(chunk, which):
        if chunk < 4:
            return shards[chunk]
        index = which * (parts // 2) + (chunk - 4) // 2
        return shards[4 + chunk % 2].at[:, span(index, width)]

    def keep_own(chunk, source=shards[0]):
        return pltpu.make_async_copy(source, held.at[chunk, mine, columns], local.at[chunk])

    def bulk(chunk, depth, breadth):
        return held.at[chunk, pl.ds(0, depth), pl.ds(0, breadth)]

    def send_z_of(chunk, source, index):
        for hop in range(1, ranks):
            remote(
                source,
                held.at[chunk, span(index, rows), columns],
                send_z.at[chunk],
                recv_z.at[chunk],
                (me, lax.rem(rank + hop, ranks)),
            ).start()

    def x_copy(chunk):
        part = bulk(chunk, rows, width)
        return remote(part, part, send_x.at[chunk], recv_x.at[chunk], (me, rank))

    def start(chunk):
        keep_own(chunk, shard(chunk, side)).start()
        if chunk >= 4:
            remote(
                shard(chunk, 1 - side),
                held.at[chunk, mine, columns],
                send_x.at[chunk],
                recv_x.at[chunk],
                (beside, rank),
            ).start()

    def start_z(chunk):
        if chunk >= 4:
            x_copy(chunk).wait_recv()
            send_z_of(chunk, held.at[chunk, span(beside, rows), columns], beside)
        send_z_of(chunk, shard(chunk, side), me)

    def z_copy(chunk, kind):
        part = bulk(chunk, rows << kind, width * (ranks - 1))
        return remote(part, part, send_z.at[chunk], recv_z.at[chunk], (me, rank))

    def send_path(chunk, kind, colour, stage):
        order = paths[kind][colour]
        earlier = order[:stage] + (1,) * kind
        other = (flipped(me, order[stage]), rank)

        def send(step):
            index = cleared(me, earlier) + spread(step, earlier)
            part = held.at[chunk, span(index, rows), pl.ds(colour * half, half)]
            remote(
                part,
                part,
                send_p.at[chunk, colour, stage],
                recv_p.at[chunk, colour, stage],
                other,
            ).start()

        each(1 << len(earlier), send)

    def path_copy(chunk, kind, colour, stage):
        part = bulk(chunk, rows << (stage + kind), half)
        return remote(
            part,
            part,
            send_p.at[chunk, colour, stage],
            recv_p.at[chunk, colour, stage],
            (me, rank),
        )

    def send_core(chunk):
        other = (flipped(me, 0), rank)

        def send(step):
            part = held.at[chunk, span(2 * step + seat, rows)]
            remote(part, part, send_c.at[chunk], recv_c.at[chunk], other).start()

        each(pairs, send)

    def core_copy(chunk):
        part = bulk(chunk, rows << (bits - 1), full)
        return remote(part, part, send_c.at[chunk], recv_c.at[chunk], (me, rank))

    def all_sent(chunk, kind):
        z_copy(chunk, kind).wait_send()
        if kind:
            x_copy(chunk).wait_send()
        for colour in range(2):
            for stage in range(bits - 1 - kind):
                path_copy(chunk, kind, colour, stage).wait_send()
        core_copy(chunk).wait_send()

    def gather_stage(chunk, kind, stage):
        if stage < kind:
            return
        if stage == kind:
            keep_own(chunk).wait()
            z_copy(chunk, kind).wait_recv()
        elif stage < bits:
            for colour in range(2):
                path_copy(chunk, kind, colour, stage - 1 - kind).wait_recv()
        else:
            core_copy(chunk).wait_recv()
        if stage < bits - 1:
            for colour in range(2):
                send_path(chunk, kind, colour, stage - kind)
        elif stage == bits - 1:
            send_core(chunk)

    units = chunks - 4

    def turn(item):
        return item

    def slot(item):
        return item + 4 if item < units else (item - units + 3) % 4

    def give_core(item):
        def send(step):
            remote(
                held.at[slot(item), span(2 * step + 1 - seat, rows)],
                from_core.at[turn(item) % RING, step],
                out_c.at[turn(item)],
                in_c.at[turn(item)],
                (flipped(me, 0), rank),
            ).start()

        each(pairs, send)

    def given_core(item):
        part = from_core.at[turn(item) % RING]
        return remote(part, part, out_c.at[turn(item)], in_c.at[turn(item)], (me, rank))

    def add_to(item, index, where, source):
        step = min(rows, tile)
        for start in range(0, rows, step):
            place = pl.ds(pl.multiple_of((2 * index + seat) * rows, rows) + start, step)
            here = held.at[slot(item), place, where]
            here[...] = (
                here[...].astype(F32) + source[pl.ds(start, step)].astype(F32)
            ).astype(BF16)

    def add_core(item):
        repeat(
            pairs,
            lambda step: add_to(
                item, step, pl.ds(0, full), from_core.at[turn(item) % RING, step]
            ),
        )

    def members(kind, colour, stage, step, kept):
        order = back_paths[kind][colour]
        later = order[stage + 1 :] + (0,) * kind
        index = pair if kept else flipped(pair, order[stage])
        return cleared(index, later) + spread(step, later)

    def give_path(item, kind, colour, stage):
        other = (2 * flipped(pair, back_paths[kind][colour][stage]) + seat, rank)

        def send(step):
            index = members(kind, colour, stage, step, False)
            remote(
                held.at[
                    slot(item), span(2 * index + seat, rows), pl.ds(colour * half, half)
                ],
                from_path[stage].at[turn(item), colour, step],
                out_p.at[turn(item), colour, stage],
                in_p.at[turn(item), colour, stage],
                other,
            ).start()

        each(pairs >> (stage + 1), send)

    def given_path(item, colour, stage):
        part = from_path[stage].at[turn(item), colour]
        return remote(
            part,
            part,
            out_p.at[turn(item), colour, stage],
            in_p.at[turn(item), colour, stage],
            (me, rank),
        )

    def add_path(item, kind, colour, stage):
        repeat(
            pairs >> (stage + 1),
            lambda step: add_to(
                item,
                members(kind, colour, stage, step, True),
                pl.ds(colour * half, half),
                from_path[stage].at[turn(item), colour, step],
            ),
        )

    def give_across(item, kind):
        for hop in range(1, ranks):
            to = lax.rem(rank + hop, ranks)
            for which in range(1 + kind):
                remote(
                    held.at[slot(item), span((me, beside)[which], rows), span(to, width)],
                    from_z.at[turn(item), (hop - 1) * (1 + kind) + which],
                    out_z.at[turn(item)],
                    in_z.at[turn(item)],
                    (me, to),
                ).start()

    def given_across(item, kind):
        part = from_z.at[turn(item), pl.ds(0, (ranks - 1) * (1 + kind))]
        return remote(part, part, out_z.at[turn(item)], in_z.at[turn(item)], (me, rank))

    def total_of(item, kind, which):
        total = held[slot(item), span((me, beside)[which], rows), columns].astype(F32)
        for hop in range(1, ranks):
            total = total + from_z[turn(item), (hop - 1) * (1 + kind) + which].astype(F32)
        return total

    def unit_place(item, which):
        return 4 + 2 * (which * (parts // 2) + item // 2) + item % 2

    def side_copy(item):
        return remote(
            side_out.at[item], side_in.at[item], out_x.at[item], in_x.at[item], (beside, rank)
        )

    def scatter_stage(item, kind, stage):
        if stage == 1:
            given_core(item).wait_recv()
            add_core(item)
        elif 1 < stage <= bits - kind:
            for colour in range(2):
                given_path(item, colour, stage - 2).wait_recv()
                add_path(item, kind, colour, stage - 2)
        elif stage == bits - kind + 1:
            given_across(item, kind).wait_recv()
            if kind:
                side_out[item] = total_of(item, kind, 1).astype(BF16)
                side_copy(item).start()
                sums[unit_place(item, side)] = total_of(item, kind, 0)
            else:
                sums[slot(item)] = total_of(item, kind, 0)
        elif stage == bits - kind + 2:
            side_copy(item).wait_recv()
            sums[unit_place(item, 1 - side)] = side_in[item].astype(F32)
        if stage == 0:
            give_core(item)
        elif stage < bits - kind:
            for colour in range(2):
                give_path(item, kind, colour, stage - 1)
        elif stage == bits - kind:
            give_across(item, kind)

    vec_ways = tuple(range(bits - 1, -1, -1))

    def vec_gather(stage):
        if stage > 0:
            part = vecs.at[pl.ds(0, 1 << (stage - 1))]
            remote(part, part, send_v.at[stage - 1], recv_v.at[stage - 1], (me, rank)).wait()
        if stage < bits:

            def send(step):
                index = cleared(me, vec_ways[:stage]) + spread(step, vec_ways[:stage])
                remote(
                    vecs.at[index],
                    vecs.at[index],
                    send_v.at[stage],
                    recv_v.at[stage],
                    (flipped(me, vec_ways[stage]), rank),
                ).start()

            each(1 << stage, send)

    def spell_params():
        params[...] = jnp.zeros_like(params)
        lane = lax.broadcasted_iota(jnp.int32, (128, full), 0)
        column = lax.broadcasted_iota(jnp.int32, (128, full), 1)

        def place(index):
            chosen = ((lane < rows) & (column == index * rows + lane)).astype(F32).astype(BF16)
            params[...] += contract(vecs[index].astype(BF16), chosen, 1, 0)

        if rows == 128:
            for index in range(1 << bits):
                params[:, index * rows : (index + 1) * rows] = vecs[index]
        else:
            repeat(1 << bits, place)

    vec_path_of = tuple(range(bits))

    def vec_stage(stage):
        if stage > 0:
            earlier = vec_path_of[stage:]
            amount = 1 << len(earlier)
            part = vec_path.at[pl.ds(amount - 1, amount)]
            remote(part, part, out_v.at[stage - 1], in_v.at[stage - 1], (me, rank)).wait()

            def add(step):
                index = cleared(me, earlier) + spread(step, earlier)
                grad_vecs[index] = grad_vecs[index] + vec_path[amount - 1 + step]

            repeat(amount, add)
        if stage < bits:
            bit, later = vec_path_of[stage], vec_path_of[stage + 1 :]
            amount = 1 << len(later)

            def send(step):
                index = cleared(flipped(me, bit), later) + spread(step, later)
                remote(
                    grad_vecs.at[index],
                    vec_path.at[amount - 1 + step],
                    out_v.at[stage],
                    in_v.at[stage],
                    (flipped(me, bit), rank),
                ).start()

            each(amount, send)
        else:
            for hop in range(1, ranks):
                to = (me, lax.rem(rank + hop, ranks))
                remote(
                    grad_vecs.at[me], vec_z.at[hop - 1], out_v.at[bits], in_v.at[bits], to
                ).start()

    def vec_finish():
        remote(vec_z, vec_z, out_v.at[bits], in_v.at[bits], (me, rank)).wait()
        total = grad_vecs[me]
        for hop in range(1, ranks):
            total = total + vec_z[hop - 1]
        vec_sum[...] = total

    def router():
        return params[0:1, :]

    def gain_one():
        return params[1:2, :]

    def gain_two():
        return params[2:3, :]

    def by_rows(body):
        repeat(count // tile, lambda index: body(span(index, tile)))

    def by_blocks(body):
        repeat(blocks, lambda index: body(span(index, block)))

    def inverse_of(values):
        return lax.rsqrt(jnp.mean(values * values, axis=-1, keepdims=True) + 1e-06)

    def wide(values):
        return jnp.broadcast_to(values, (values.shape[0], 128))

    def transpose_to(target, source, first=0):
        def turn_over(index):
            part = span(index, 128)
            values = source[first : first + count, part].astype(F32)
            target[part, first : first + count] = values.T.astype(BF16)

        repeat(full // 128, turn_over)

    def to_beside(which, source, target):
        return remote(source, target, act_out.at[which], act_in.at[which], (beside, rank))

    own_rows, their_rows = pl.ds(0, count), pl.ds(count, count)

    def branch_copy():
        return to_beside(0, branch.at[own_rows], branch.at[their_rows])

    def norm_copy():
        return to_beside(1, norm_two.at[own_rows], norm_two.at[their_rows])

    def grad_copy():
        return to_beside(2, grad_low, grad_in)

    def mlp_copy():
        return to_beside(3, mlp_low, mlp_in)

    slab = pairs * rows
    halves = length // slab

    def fetch(source, seq, step, place):
        def copy(index):
            pltpu.make_async_copy(
                source.at[seq, pl.ds(pl.multiple_of(index * rows, rows) + step * slab, rows)],
                from_core.at[place, index],
                fetched.at[place],
            ).start()

        each(pairs, copy)

    def down_and_across(seq):
        across = routes[pl.ds(rank * seqs + seq, 1), :].astype(F32)
        return jnp.broadcast_to(across, (caps, caps)).T, across

    def mask(seq):
        down, across = down_and_across(seq)
        begin = pic_start[rank * seqs + seq].astype(F32)
        inside_down = (down >= begin) & (down < begin + PIC)
        inside_across = (across >= begin) & (across < begin + PIC)
        seen = (across <= down) | (inside_down & inside_across)
        allowed[seq] = seen.astype(F32)

    def pick(target, seq, place):
        down, _ = down_and_across(seq)
        column = lax.broadcasted_iota(jnp.int32, (caps, slab), 1).astype(F32)
        for step in range(halves):
            pltpu.make_async_copy(
                from_core.at[place + step], from_core.at[place + step], fetched.at[place + step]
            ).wait()

        def body(part):
            total = 0.0
            for step in range(halves):
                chosen = (down[:, 0:1] == column + step * slab).astype(F32).astype(BF16)
                source = from_core[place + step, :, :, part].reshape(slab, block)
                total = total + contract(chosen, source, 1, 0)
            target[pl.ds(seq * caps, caps), part] = total.astype(BF16)

        by_blocks(body)

    def prepare():
        def body(part):
            values = picked[part].astype(F32)
            logit = jnp.sum(values * router(), axis=-1, keepdims=True)
            gate = 1.0 / (1.0 + jnp.exp(-logit))
            gates[part] = wide(gate)
            norm_one[part] = (values * inverse_of(values) * gain_one()).astype(BF16)
            branch[part] = (gate * grad_rows[part].astype(F32)).astype(BF16)

        by_rows(body)
        transpose_to(branch_t, branch)

    def send_branch():
        branch_copy().start()

    def project(which):
        def body(part):
            qkv[which, :, part] = contract(norm_one[...], held[which, :, part], 1, 0).astype(BF16)

        by_blocks(body)

    lanes = lax.broadcasted_iota(jnp.int32, (1, 2 * HD), 1)

    def own_lanes(values, head):
        inside = (lanes < HD) if head == 0 else (lanes >= HD)
        return jnp.where(inside, values, jnp.zeros_like(values))

    def probabilities(seq, queries, keys, head):
        scores = contract(own_lanes(queries, head), keys, 1, 1) * (1.0 / math.sqrt(HD))
        scores = jnp.where(allowed[seq] > 0, scores, -1e30)
        powers = jnp.exp(scores - jnp.max(scores, axis=-1, keepdims=True))
        return powers / jnp.sum(powers, axis=-1, keepdims=True)

    def attend():
        def body(index):
            part = span(index, 2 * HD)
            for seq in range(seqs):
                place = pl.ds(seq * caps, caps)
                queries, keys = qkv[0, place, part], qkv[1, place, part]
                values = qkv[2, place, part]
                total = 0.0
                for head in range(2):
                    probs = probabilities(seq, queries, keys, head).astype(BF16)
                    total = total + contract(probs, own_lanes(values, head), 1, 0)
                context[place, part] = total.astype(BF16)

        repeat(full // (2 * HD), body)

    def leave_attention():
        def body(part):
            attended[:, part] = contract(context[...], held[3, part, :], 1, 1)

        by_blocks(body)

        def rest(part):
            values = picked[part].astype(F32) + attended[part]
            norm_two[part] = (values * inverse_of(values) * gain_two()).astype(BF16)

        by_rows(rest)
        norm_copy().start()
        transpose_to(norm_two_t, norm_two)
        mlp[...] = jnp.zeros_like(mlp)
        grad_two[...] = jnp.zeros_like(grad_two)

    def by_lines(body):
        repeat(2 * blocks, lambda i: body(span(lax.rem(i, 2), count), span(lax.div(i, 2), block)))

    def go_up(up):
        if up == 4:
            norm_copy().wait_recv()
            transpose_to(norm_two_t, norm_two, count)

        def units_of(lines, part):
            pre = contract(norm_two[lines], held[up, :, part], 1, 0)
            bell = 0.5 * (1.0 + lax.erf(pre * inv_root_two))
            slopes[lines, part] = bell + pre * jnp.exp(-0.5 * pre * pre) * inv_root_two_pi
            hidden[lines, part] = (pre * bell).astype(BF16)

        by_lines(units_of)

    def go_down(up, down):
        if up == 4:
            branch_copy().wait_recv()
            transpose_to(branch_t, branch, count)

        def units_of(lines, part):
            grad_hidden = contract(branch[lines], held[down, :, part], 1, 0)
            grad_pre[lines, part] = (grad_hidden * slopes[lines, part]).astype(BF16)

        by_lines(units_of)

        def add_out(target, source, weight, lines):
            def body(part):
                target[lines, part] += contract(source[lines], held[weight, part, :], 1, 1)

            by_blocks(body)

        def pass_on(source, target, copy):
            if down == chunks - 1:

                def body(part):
                    target[part] = source[pl.ds(part.start + count, tile)].astype(BF16)

                by_rows(body)
                copy().start()

        add_out(grad_two, grad_pre, up, their_rows)
        pass_on(grad_two, grad_low, grad_copy)
        add_out(mlp, hidden, down, their_rows)
        pass_on(mlp, mlp_low, mlp_copy)
        add_out(grad_two, grad_pre, up, own_rows)
        add_out(mlp, hidden, down, own_rows)
        all_sent(up, 1)
        all_sent(down, 1)

        def gradients(part):
            held[down, :, part] = contract(branch_t[...], hidden[:, part], 1, 0).astype(BF16)
            held[up, :, part] = contract(norm_two_t[...], grad_pre[:, part], 1, 0).astype(BF16)

        by_blocks(gradients)

    small = params

    def enter_back():
        small[3:6, :] = jnp.zeros((3, full), F32)
        grad_copy().wait_recv()

        def body(part):
            values = picked[part].astype(F32)
            residual = values + attended[part]
            inverse = inverse_of(residual)
            grad = grad_two[part] + grad_in[part].astype(F32)
            small[5:6, :] += jnp.sum(grad * residual * inverse, axis=0, keepdims=True)
            scaled = grad * gain_two()
            mean = jnp.mean(scaled * residual, axis=-1, keepdims=True)
            grad_mid = inverse * scaled - residual * (inverse * inverse * inverse * mean)
            grad_two[part] = grad_mid
            rows_in = grad_rows[part].astype(F32)
            grad_attended[part] = (gates[part, 0:1] * rows_in + grad_mid).astype(BF16)

        by_rows(body)
        transpose_to(grad_attended_t, grad_attended)

        def through(part):
            grad_context[:, part] = contract(grad_attended[...], held[3, :, part], 1, 0).astype(BF16)

        by_blocks(through)
        for chunk in range(4):
            all_sent(chunk, 0)

        def weights(part):
            held[3, :, part] = contract(grad_attended_t[...], context[:, part], 1, 0).astype(BF16)

        by_blocks(weights)

    def recall():
        def body(index):
            part = span(index, 2 * HD)
            for seq in range(seqs):
                place = pl.ds(seq * caps, caps)
                queries, keys = qkv[0, place, part], qkv[1, place, part]
                for head in range(2):
                    slopes[pl.ds((2 * seq + head) * caps, caps), part] = probabilities(
                        seq, queries, keys, head
                    )

        repeat(full // (2 * HD), body)

    def attend_back():
        def body(index):
            part = span(index, 2 * HD)
            for seq in range(seqs):
                place = pl.ds(seq * caps, caps)
                queries, keys = qkv[0, place, part], qkv[1, place, part]
                values, grad = qkv[2, place, part], grad_context[place, part]
                grad_q, grad_k, grad_v = 0.0, 0.0, 0.0
                for head in range(2):
                    probs = slopes[pl.ds((2 * seq + head) * caps, caps), part]
                    grad_probs = contract(own_lanes(grad, head), values, 1, 1)
                    inner = jnp.sum(probs * grad_probs, axis=-1, keepdims=True)
                    grad_scores = (probs * (grad_probs - inner)).astype(BF16)
                    low = probs.astype(BF16)
                    grad_v = grad_v + contract(low, own_lanes(grad, head), 0, 0)
                    grad_q = grad_q + contract(grad_scores, own_lanes(keys, head), 1, 0)
                    grad_k = grad_k + contract(grad_scores, own_lanes(queries, head), 0, 0)
                scale = 1.0 / math.sqrt(HD)
                grad_qkv[0, place, part] = (grad_q * scale).astype(BF16)
                grad_qkv[1, place, part] = (grad_k * scale).astype(BF16)
                grad_qkv[2, place, part] = grad_v.astype(BF16)

        repeat(full // (2 * HD), body)

    def leave_back():
        def through(part):
            total = contract(grad_qkv[0], held[0, part, :], 1, 1)
            for which in (1, 2):
                total = total + contract(grad_qkv[which], held[which, part, :], 1, 1)
            grad_one[:, part] = total

        by_blocks(through)

    def weigh_back():
        transpose_to(norm_one_t, norm_one)

        def weights(part):
            for which in range(3):
                held[which, :, part] = contract(norm_one_t[...], grad_qkv[which, :, part], 1, 0).astype(
                    BF16
                )

        by_blocks(weights)

    def close():
        mlp_copy().wait_recv()

        def body(part):
            values = picked[part].astype(F32)
            rows_in = grad_rows[part].astype(F32)
            gate = gates[part, 0:1]
            delta = attended[part] + (mlp[part] + mlp_in[part].astype(F32))
            new_rows[part] = (values + gate * delta).astype(BF16)
            score = jnp.sum(rows_in * delta, axis=-1, keepdims=True) * gate * (1.0 - gate)
            small[3:4, :] += jnp.sum(score * values, axis=0, keepdims=True)
            inverse = inverse_of(values)
            grad = grad_one[part]
            small[4:5, :] += jnp.sum(grad * values * inverse, axis=0, keepdims=True)
            scaled = grad * gain_one()
            mean = jnp.mean(scaled * values, axis=-1, keepdims=True)
            grad_norm = inverse * scaled - values * (inverse * inverse * inverse * mean)
            total = rows_in + grad_two[part] + grad_norm + score * router()
            new_grads[part] = total.astype(BF16)

        by_rows(body)
        own = small[...]
        if rows == 128:
            for index in range(1 << bits):
                grad_vecs[index] = own[:, index * rows : (index + 1) * rows]
        else:
            column = lax.broadcasted_iota(jnp.int32, (full, 128), 0)
            lane = lax.broadcasted_iota(jnp.int32, (full, 128), 1)

            def place(index):
                chosen = ((lane < rows) & (column == index * rows + lane)).astype(F32)
                grad_vecs[index] = jnp.dot(
                    own, chosen, precision=lax.Precision.HIGHEST, preferred_element_type=F32
                )

            repeat(1 << bits, place)

    keep_vec = pltpu.make_async_copy(vec, vecs.at[me], local.at[chunks])
    keep_vec.start()
    for chunk in range(4):
        start(chunk)
        start_z(chunk)
    for chunk in range(4, chunks):
        start(chunk)
    for which, source in enumerate((activations, cotangent)):
        for seq in range(seqs):
            for step in range(halves):
                fetch(source, seq, step, (which * seqs + seq) * halves + step)
    keep_vec.wait()
    vec_gather(0)

    events = []

    def at(when, what, *args):
        events.append((when, len(events), functools.partial(what, *args)))

    def between(first, last, step, steps):
        return first + (last - first) * step / max(steps, 1)

    for stage in range(1, bits + 1):
        at(3.8 + 2.2 * stage, vec_gather, stage)
    for seq in range(seqs):
        at(9 + seq, mask, seq)
        for which, target in enumerate((picked, grad_rows)):
            at(9 + seq, pick, target, seq, (which * seqs + seq) * halves)
    for chunk in range(4, chunks):
        at(7.5, start_z, chunk)
    at(3.8 + 2.2 * bits + 3.2, spell_params)
    at(3.8 + 2.2 * bits + 3.2, prepare)
    weights_in = [33 + 8.5 * chunk for chunk in range(4)] + [
        71 + 11.2 * chunk for chunk in range(units)
    ]
    for chunk in range(chunks):
        kind = int(chunk >= 4)
        opened = (54 + 8.3 * (chunk - 4)) if kind else (13 + 8.5 * chunk)
        for stage in range(kind, bits):
            when = between(opened, weights_in[chunk] - 4, stage - kind, bits - 1 - kind)
            at(when, gather_stage, chunk, kind, stage)
        at(weights_in[chunk], gather_stage, chunk, kind, bits)
    for chunk in range(3):
        at(weights_in[chunk], project, chunk)
    at(47, send_branch)
    at(weights_in[2], attend)
    at(weights_in[3], leave_attention)
    for item in range(0, units, 2):
        up, down = item + 4, item + 5
        at(max(weights_in[up], 74) + 0.1, go_up, up)
        ready = weights_in[down] + 0.1
        at(ready, go_down, up, down)
        for one in (item, item + 1):
            at(ready, give_core, one)
    at(116.5, recall)
    at(120, enter_back)
    at(120, give_core, units)
    at(126, attend_back)
    at(134, leave_back)
    at(134, close)
    at(134.2, weigh_back)
    for item in range(units + 1, chunks):
        at(134.3, give_core, item)
    summed = [
        (93.1, 115, 116, 147, 178),
        (93.1, 123, 124, 147.1, 178),
        (115, 132, 133, 148, 178),
        (115.1, 143.1, 143.15, 173, 184),
        (125, 143.2, 160, 177, 0),
        (143, 158, 170, 181, 0),
        (143.3, 166, 175, 185, 0),
        (158.1, 172, 178, 187, 0),
    ]
    for item, (core_in, second, last, across, aside) in enumerate(summed):
        kind = int(item < units)
        final = bits - kind
        at(core_in, scatter_stage, item, kind, 1)
        for stage in range(2, final + 1):
            when = last if final == 2 else between(second, last, stage - 2, final - 2)
            at(when, scatter_stage, item, kind, stage)
        at(across, scatter_stage, item, kind, final + 1)
        if kind:
            at(aside, scatter_stage, item, kind, final + 2)
    for stage in range(bits + 1):
        when = (134.1, 142.9, 143.05, 164.5)[stage] if stage < 4 else 164.5 + 2 * stage
        at(when, vec_stage, stage)
    at(188, vec_finish)
    for _, _, event in sorted(events, key=lambda event: event[:2]):
        event()

    branch_copy().wait_send()
    norm_copy().wait_send()
    grad_copy().wait_send()
    mlp_copy().wait_send()

    def drain(item, kind):
        given_core(item).wait_send()
        for colour in range(2):
            for stage in range(bits - 1 - kind):
                given_path(item, colour, stage).wait_send()
        given_across(item, kind).wait_send()
        if kind:
            side_copy(item).wait_send()

    for item in range(chunks):
        drain(item, int(item < units))


def run_layer(bits, ranks, shards, vec, routes, pic_start, activations, cotangent):
    rows, width = shards[0].shape
    parts = shards[4].shape[1] // width
    chunks = 4 + parts
    depth, breadth, pairs = rows << bits, width * ranks, 1 << (bits - 1)
    seqs, _, full = activations.shape
    caps = routes.shape[1]
    count = seqs * caps
    dma = pltpu.SemaphoreType.DMA
    low = pltpu.VMEM((count, full), BF16)
    turned = pltpu.VMEM((full, count), BF16)
    high = pltpu.VMEM((count, full), F32)
    low_two = pltpu.VMEM((2 * count, full), BF16)
    turned_two = pltpu.VMEM((full, 2 * count), BF16)
    high_two = pltpu.VMEM((2 * count, full), F32)
    return pl.pallas_call(
        functools.partial(layer_kernel, bits, ranks, chunks, parts),
        out_shape=[
            jax.ShapeDtypeStruct((4 + 2 * parts, rows, width), F32),
            jax.ShapeDtypeStruct((8, 128), F32),
            jax.ShapeDtypeStruct((count, full), BF16),
            jax.ShapeDtypeStruct((count, full), BF16),
        ],
        in_specs=[ANY] * 6 + [VMEM] * 2 + [pl.BlockSpec(memory_space=pltpu.SMEM)] + [ANY] * 2,
        out_specs=[VMEM] * 4,
        scratch_shapes=[
            low,
            low,
            pltpu.VMEM((seqs, caps, caps), F32),
            pltpu.VMEM((chunks, depth, breadth), BF16),
            pltpu.VMEM((RING, pairs, rows, breadth), BF16),
            pltpu.VMEM((chunks, 2 * (ranks - 1), rows, width), BF16),
            pltpu.VMEM((1 << bits, 8, 128), F32),
            pltpu.VMEM((1 << bits, 8, 128), F32),
            pltpu.VMEM((1 << bits, 8, 128), F32),
            pltpu.VMEM((ranks - 1, 8, 128), F32),
            pltpu.VMEM((8, full), F32),
            pltpu.VMEM((count, 128), F32),
            low,
            pltpu.VMEM((3, count, full), BF16),
            low,
            high,
            low_two,
            turned_two,
            low_two,
            turned_two,
            low_two,
            low_two,
            high_two,
            high_two,
            high_two,
            low,
            low,
            low,
            low,
            low,
            turned,
            low,
            pltpu.VMEM((3, count, full), BF16),
            high,
            turned,
            pltpu.VMEM((parts, rows, width), BF16),
            pltpu.VMEM((parts, rows, width), BF16),
            dma((chunks,)),
            dma((chunks,)),
            dma((4,)),
            dma((4,)),
            dma((parts,)),
            dma((parts,)),
            dma((chunks,)),
            dma((chunks,)),
            dma((chunks, 2, bits - 1)),
            dma((chunks, 2, bits - 1)),
            dma((chunks,)),
            dma((chunks,)),
            dma((bits,)),
            dma((bits,)),
            dma((chunks + 1,)),
            dma((chunks,)),
            dma((chunks,)),
            dma((chunks, 2, bits - 1)),
            dma((chunks, 2, bits - 1)),
            dma((chunks,)),
            dma((chunks,)),
            dma((bits + 1,)),
            dma((bits + 1,)),
            dma((RING,)),
            *[
                pltpu.VMEM((chunks, 2, pairs >> (stage + 1), rows, breadth // 2), BF16)
                for stage in range(bits - 1)
            ],
        ],
        compiler_params=pltpu.CompilerParams(
            collective_id=1, has_side_effects=True, vmem_limit_bytes=67043328
        ),
        name="layer_kernel",
    )(*shards, vec, routes, pic_start, activations, cotangent)


def put_kernel(seqs, steps, routes, new_rows, new_grads, activations, cotangent, result, grad_input):
    index = pl.program_id(0)
    seq, step = lax.div(index, steps), lax.rem(index, steps)
    size, caps = activations.shape[1], routes.shape[1]
    place = routes[pl.ds(lax.axis_index("tensor") * seqs + seq, 1), :]
    line = lax.broadcasted_iota(jnp.int32, (size, caps), 0) + step * size
    chosen = (line == place).astype(F32)
    routed = jnp.max(chosen, axis=-1, keepdims=True) > 0
    chosen = chosen.astype(BF16)
    for new, base, out in (
        (new_rows, activations, result),
        (new_grads, cotangent, grad_input),
    ):
        placed = contract(chosen, new[...], 1, 0)
        out[0] = jnp.where(routed, placed, base[0].astype(F32)).astype(BF16)


def put_rows(routes, new_rows, new_grads, activations, cotangent):
    seqs, length, full = activations.shape
    caps = routes.shape[1]
    steps = 4
    size = length // steps
    large = pl.BlockSpec((1, size, full), lambda index: (index // steps, index % steps, 0))
    small = pl.BlockSpec((caps, full), lambda index: (index // steps, 0))
    return pl.pallas_call(
        functools.partial(put_kernel, seqs, steps),
        grid=(seqs * steps,),
        out_shape=[jax.ShapeDtypeStruct(activations.shape, BF16)] * 2,
        in_specs=[pl.BlockSpec(routes.shape, lambda index: (0, 0)), small, small, large, large],
        out_specs=[large, large],
        name="put_rows",
    )(routes, new_rows, new_grads, activations, cotangent)


def shards(
    activations,
    routes,
    pic_start,
    router_w,
    gain_attn,
    gain_mlp,
    w_query,
    w_key,
    w_value,
    w_proj,
    w_up,
    w_down,
    cotangent,
):
    ranks = lax.axis_size("tensor")
    bits = lax.axis_size("dp").bit_length() - 1
    rows, width = w_query.shape
    parts = w_up.shape[1] // width
    vec = jnp.stack([router_w, gain_attn, gain_mlp]).astype(F32)
    vec = jnp.pad(vec, ((0, 5), (0, 128 - rows)))
    weights = (w_query, w_key, w_value, w_proj, w_up, w_down)
    sums, small, new_rows, new_grads = run_layer(
        bits, ranks, weights, vec, routes, pic_start, activations, cotangent
    )
    result, grad_input = put_rows(routes, new_rows, new_grads, activations, cotangent)

    def side_by_side(first):
        return jnp.concatenate([sums[first + 2 * part] for part in range(parts)], axis=1)

    return (
        result,
        grad_input,
        small[3, :rows],
        small[4, :rows],
        small[5, :rows],
        sums[0],
        sums[1],
        sums[2],
        sums[3],
        side_by_side(4),
        side_by_side(5),
    )


def solution(mesh):
    both = P(("dp", "tensor"), None, None)
    cut = P("dp", "tensor")
    one = P("dp")
    return jax.shard_map(
        shards,
        mesh=mesh,
        in_specs=(both, P("dp", None), one, one, one, one) + (cut,) * 6 + (both,),
        out_specs=(both, both, one, one, one) + (cut,) * 6,
        check_vma=False,
    )
```

```python
import functools
import math

import jax
import jax.numpy as jnp
from jax import lax
from jax.experimental import pallas as pl
from jax.experimental.pallas import tpu as pltpu
from jax.sharding import PartitionSpec as P

HD = 64
PIC = 256
RING = 8
MESH = pl.DeviceIdType.MESH
ANY = pl.BlockSpec(memory_space=pl.ANY)
VMEM = pl.BlockSpec(memory_space=pltpu.VMEM)
BF16 = jnp.bfloat16
F32 = jnp.float32

inv_root_two = 0.7071067811865476
inv_root_two_pi = 0.3989422804014327


def bit_of(value, bit):
    return lax.rem(lax.div(value, 1 << bit), 2)


def flipped(value, bit):
    return value + (1 - 2 * bit_of(value, bit)) * (1 << bit)


def cleared(value, bits):
    for bit in bits:
        value = value - bit_of(value, bit) * (1 << bit)
    return value


def spread(step, bits):
    value = 0
    for place, bit in enumerate(bits):
        value = value + lax.rem(lax.div(step, 1 << place), 2) * (1 << bit)
    return value


def each(count, body):
    if count <= 4:
        for step in range(count):
            body(jnp.int32(step))
    else:
        lax.fori_loop(0, count, lambda step, _: body(step), None)


def repeat(count, body):
    def step(index, _):
        body(index)

    lax.fori_loop(0, count, step, None)


def span(index, size):
    return pl.ds(pl.multiple_of(index * size, size), size)


def sides(bits):
    return (tuple(range(bits - 1, 1, -1)),) * 2


def orders(bits):
    return (tuple(range(bits - 1, 0, -1)), tuple(range(1, bits)))


def remote(src, dst, send, recv, where):
    return pltpu.make_async_remote_copy(
        src_ref=src, dst_ref=dst, send_sem=send, recv_sem=recv, device_id=where, device_id_type=MESH
    )


def contract(left, right, axis_left, axis_right):
    return lax.dot_general(
        left, right, (((axis_left,), (axis_right,)), ((), ())), preferred_element_type=F32
    )


def layer_kernel(
    bits,
    ranks,
    chunks,
    parts,
    *refs,
):
    shards = refs[:6]
    (
    vec,
    routes,
    pic_start,
    activations,
    cotangent,
    sum_query,
    sum_key,
    sum_value,
    sum_proj,
    sum_up,
    sum_down,
    vec_sum,
    new_rows,
    new_grads,
    picked,
    grad_rows,
    allowed,
    held,
    from_core,
    from_z,
    vecs,
    grad_vecs,
    vec_path,
    vec_z,
    params,
    gates,
    norm_one,
    qkv,
    context,
    attended,
    norm_two,
    norm_two_t,
    branch,
    branch_t,
    hidden,
    grad_pre,
    mlp,
    grad_two,
    slopes,
    mlp_low,
    grad_low,
    mlp_in,
    grad_in,
    grad_attended,
    grad_attended_t,
    grad_context,
    grad_qkv,
    grad_one,
    norm_one_t,
    side_out,
    side_in,
    send_x,
    recv_x,
    act_out,
    act_in,
    out_x,
    in_x,
    send_z,
    recv_z,
    send_p,
    recv_p,
    send_c,
    recv_c,
    send_v,
    recv_v,
    local,
    out_c,
    in_c,
    out_p,
    in_p,
    out_z,
    in_z,
    out_v,
    in_v,
    fetched,
    *from_path,
    ) = refs[6:]
    me, rank = lax.axis_index("dp"), lax.axis_index("tensor")
    rows, width = shards[0].shape
    count, full = picked.shape
    length = activations.shape[1]
    seqs, caps, _ = allowed.shape
    half = full // 2
    seat, pair = bit_of(me, 0), lax.div(me, 2)
    pairs = 1 << (bits - 1)
    paths = (orders(bits), sides(bits))
    back_paths = tuple(
        tuple(tuple(bit - 1 for bit in order[::-1]) for order in kind) for kind in paths
    )
    side, beside = bit_of(me, 1), flipped(me, 1)
    tile = 32
    block = 256
    blocks = full // block

    barrier = pltpu.get_barrier_semaphore()
    for bit in range(bits):
        pl.semaphore_signal(barrier, 1, device_id=(flipped(me, bit), rank), device_id_type=MESH)
    for hop in range(1, ranks):
        pl.semaphore_signal(
            barrier, 1, device_id=(me, lax.rem(rank + hop, ranks)), device_id_type=MESH
        )
    pl.semaphore_wait(barrier, bits + ranks - 1)

    mine = span(me, rows)
    columns = span(rank, width)

    def shard(chunk, which):
        if chunk < 4:
            return shards[chunk]
        index = which * (parts // 2) + (chunk - 4) // 2
        return shards[4 + chunk % 2].at[:, span(index, width)]

    def keep_own(chunk, source=shards[0]):
        return pltpu.make_async_copy(source, held.at[chunk, mine, columns], local.at[chunk])

    def bulk(chunk, depth, breadth):
        return held.at[chunk, pl.ds(0, depth), pl.ds(0, breadth)]

    def send_z_of(chunk, source, index):
        for hop in range(1, ranks):
            remote(
                source,
                held.at[chunk, span(index, rows), columns],
                send_z.at[chunk],
                recv_z.at[chunk],
                (me, lax.rem(rank + hop, ranks)),
            ).start()

    def x_copy(chunk):
        part = bulk(chunk, rows, width)
        return remote(part, part, send_x.at[chunk], recv_x.at[chunk], (me, rank))

    def start(chunk):
        keep_own(chunk, shard(chunk, side)).start()
        if chunk >= 4:
            remote(
                shard(chunk, 1 - side),
                held.at[chunk, mine, columns],
                send_x.at[chunk],
                recv_x.at[chunk],
                (beside, rank),
            ).start()

    def start_z(chunk):
        if chunk >= 4:
            x_copy(chunk).wait_recv()
            send_z_of(chunk, held.at[chunk, span(beside, rows), columns], beside)
        send_z_of(chunk, shard(chunk, side), me)

    def z_copy(chunk, kind):
        part = bulk(chunk, rows << kind, width * (ranks - 1))
        return remote(part, part, send_z.at[chunk], recv_z.at[chunk], (me, rank))

    def send_path(chunk, kind, colour, stage):
        order = paths[kind][colour]
        earlier = order[:stage] + (1,) * kind
        other = (flipped(me, order[stage]), rank)

        def send(step):
            index = cleared(me, earlier) + spread(step, earlier)
            part = held.at[chunk, span(index, rows), pl.ds(colour * half, half)]
            remote(
                part,
                part,
                send_p.at[chunk, colour, stage],
                recv_p.at[chunk, colour, stage],
                other,
            ).start()

        each(1 << len(earlier), send)

    def path_copy(chunk, kind, colour, stage):
        part = bulk(chunk, rows << (stage + kind), half)
        return remote(
            part,
            part,
            send_p.at[chunk, colour, stage],
            recv_p.at[chunk, colour, stage],
            (me, rank),
        )

    def send_core(chunk):
        other = (flipped(me, 0), rank)

        def send(step):
            part = held.at[chunk, span(2 * step + seat, rows)]
            remote(part, part, send_c.at[chunk], recv_c.at[chunk], other).start()

        each(pairs, send)

    def core_copy(chunk):
        part = bulk(chunk, rows << (bits - 1), full)
        return remote(part, part, send_c.at[chunk], recv_c.at[chunk], (me, rank))

    def all_sent(chunk, kind):
        z_copy(chunk, kind).wait_send()
        if kind:
            x_copy(chunk).wait_send()
        for colour in range(2):
            for stage in range(bits - 1 - kind):
                path_copy(chunk, kind, colour, stage).wait_send()
        core_copy(chunk).wait_send()

    def gather_stage(chunk, kind, stage):
        if stage < kind:
            return
        if stage == kind:
            keep_own(chunk).wait()
            z_copy(chunk, kind).wait_recv()
        elif stage < bits:
            for colour in range(2):
                path_copy(chunk, kind, colour, stage - 1 - kind).wait_recv()
        else:
            core_copy(chunk).wait_recv()
        if stage < bits - 1:
            for colour in range(2):
                send_path(chunk, kind, colour, stage - kind)
        elif stage == bits - 1:
            send_core(chunk)

    units = chunks - 4

    def turn(item):
        return item

    def slot(item):
        return item + 4 if item < units else (item - units + 3) % 4

    def give_core(item):
        def send(step):
            remote(
                held.at[slot(item), span(2 * step + 1 - seat, rows)],
                from_core.at[turn(item) % RING, step],
                out_c.at[turn(item)],
                in_c.at[turn(item)],
                (flipped(me, 0), rank),
            ).start()

        each(pairs, send)

    def given_core(item):
        part = from_core.at[turn(item) % RING]
        return remote(part, part, out_c.at[turn(item)], in_c.at[turn(item)], (me, rank))

    def add_to(item, index, where, source):
        step = min(rows, tile)
        for start in range(0, rows, step):
            place = pl.ds(pl.multiple_of((2 * index + seat) * rows, rows) + start, step)
            here = held.at[slot(item), place, where]
            here[...] = (
                here[...].astype(F32) + source[pl.ds(start, step)].astype(F32)
            ).astype(BF16)

    def add_core(item):
        repeat(
            pairs,
            lambda step: add_to(
                item, step, pl.ds(0, full), from_core.at[turn(item) % RING, step]
            ),
        )

    def members(kind, colour, stage, step, kept):
        order = back_paths[kind][colour]
        later = order[stage + 1 :] + (0,) * kind
        index = pair if kept else flipped(pair, order[stage])
        return cleared(index, later) + spread(step, later)

    def give_path(item, kind, colour, stage):
        other = (2 * flipped(pair, back_paths[kind][colour][stage]) + seat, rank)

        def send(step):
            index = members(kind, colour, stage, step, False)
            remote(
                held.at[
                    slot(item), span(2 * index + seat, rows), pl.ds(colour * half, half)
                ],
                from_path[stage].at[turn(item), colour, step],
                out_p.at[turn(item), colour, stage],
                in_p.at[turn(item), colour, stage],
                other,
            ).start()

        each(pairs >> (stage + 1), send)

    def given_path(item, colour, stage):
        part = from_path[stage].at[turn(item), colour]
        return remote(
            part,
            part,
            out_p.at[turn(item), colour, stage],
            in_p.at[turn(item), colour, stage],
            (me, rank),
        )

    def add_path(item, kind, colour, stage):
        repeat(
            pairs >> (stage + 1),
            lambda step: add_to(
                item,
                members(kind, colour, stage, step, True),
                pl.ds(colour * half, half),
                from_path[stage].at[turn(item), colour, step],
            ),
        )

    def give_across(item, kind):
        for hop in range(1, ranks):
            to = lax.rem(rank + hop, ranks)
            for which in range(1 + kind):
                remote(
                    held.at[slot(item), span((me, beside)[which], rows), span(to, width)],
                    from_z.at[turn(item), (hop - 1) * (1 + kind) + which],
                    out_z.at[turn(item)],
                    in_z.at[turn(item)],
                    (me, to),
                ).start()

    def given_across(item, kind):
        part = from_z.at[turn(item), pl.ds(0, (ranks - 1) * (1 + kind))]
        return remote(part, part, out_z.at[turn(item)], in_z.at[turn(item)], (me, rank))

    def total_of(item, kind, which):
        total = held[slot(item), span((me, beside)[which], rows), columns].astype(F32)
        for hop in range(1, ranks):
            total = total + from_z[turn(item), (hop - 1) * (1 + kind) + which].astype(F32)
        return total

    def put_units(item, which, values):
        place = span(which * (parts // 2) + item // 2, width)
        (sum_up, sum_down)[item % 2][:, place] = values

    def side_copy(item):
        return remote(
            side_out.at[item], side_in.at[item], out_x.at[item], in_x.at[item], (beside, rank)
        )

    def scatter_stage(item, kind, stage):
        if stage == 1:
            given_core(item).wait_recv()
            add_core(item)
        elif 1 < stage <= bits - kind:
            for colour in range(2):
                given_path(item, colour, stage - 2).wait_recv()
                add_path(item, kind, colour, stage - 2)
        elif stage == bits - kind + 1:
            given_across(item, kind).wait_recv()
            if kind:
                side_out[item] = total_of(item, kind, 1).astype(BF16)
                side_copy(item).start()
                put_units(item, side, total_of(item, kind, 0))
            else:
                out = (sum_query, sum_key, sum_value, sum_proj)[slot(item)]
                out[...] = total_of(item, kind, 0)
        elif stage == bits - kind + 2:
            side_copy(item).wait_recv()
            put_units(item, 1 - side, side_in[item].astype(F32))
        if stage == 0:
            give_core(item)
        elif stage < bits - kind:
            for colour in range(2):
                give_path(item, kind, colour, stage - 1)
        elif stage == bits - kind:
            give_across(item, kind)

    vec_ways = tuple(range(bits - 1, -1, -1))

    def vec_gather(stage):
        if stage > 0:
            part = vecs.at[pl.ds(0, 1 << (stage - 1))]
            remote(part, part, send_v.at[stage - 1], recv_v.at[stage - 1], (me, rank)).wait()
        if stage < bits:

            def send(step):
                index = cleared(me, vec_ways[:stage]) + spread(step, vec_ways[:stage])
                remote(
                    vecs.at[index],
                    vecs.at[index],
                    send_v.at[stage],
                    recv_v.at[stage],
                    (flipped(me, vec_ways[stage]), rank),
                ).start()

            each(1 << stage, send)

    def spell_params():
        params[...] = jnp.zeros_like(params)
        lane = lax.broadcasted_iota(jnp.int32, (128, full), 0)
        column = lax.broadcasted_iota(jnp.int32, (128, full), 1)

        def place(index):
            chosen = ((lane < rows) & (column == index * rows + lane)).astype(F32).astype(BF16)
            params[...] += contract(vecs[index].astype(BF16), chosen, 1, 0)

        if rows == 128:
            for index in range(1 << bits):
                params[:, index * rows : (index + 1) * rows] = vecs[index]
        else:
            repeat(1 << bits, place)

    vec_path_of = tuple(range(bits))

    def vec_stage(stage):
        if stage > 0:
            earlier = vec_path_of[stage:]
            amount = 1 << len(earlier)
            part = vec_path.at[pl.ds(amount - 1, amount)]
            remote(part, part, out_v.at[stage - 1], in_v.at[stage - 1], (me, rank)).wait()

            def add(step):
                index = cleared(me, earlier) + spread(step, earlier)
                grad_vecs[index] = grad_vecs[index] + vec_path[amount - 1 + step]

            repeat(amount, add)
        if stage < bits:
            bit, later = vec_path_of[stage], vec_path_of[stage + 1 :]
            amount = 1 << len(later)

            def send(step):
                index = cleared(flipped(me, bit), later) + spread(step, later)
                remote(
                    grad_vecs.at[index],
                    vec_path.at[amount - 1 + step],
                    out_v.at[stage],
                    in_v.at[stage],
                    (flipped(me, bit), rank),
                ).start()

            each(amount, send)
        else:
            for hop in range(1, ranks):
                to = (me, lax.rem(rank + hop, ranks))
                remote(
                    grad_vecs.at[me], vec_z.at[hop - 1], out_v.at[bits], in_v.at[bits], to
                ).start()

    def vec_finish():
        remote(vec_z, vec_z, out_v.at[bits], in_v.at[bits], (me, rank)).wait()
        total = grad_vecs[me]
        for hop in range(1, ranks):
            total = total + vec_z[hop - 1]
        vec_sum[...] = total

    def router():
        return params[0:1, :]

    def gain_one():
        return params[1:2, :]

    def gain_two():
        return params[2:3, :]

    def by_rows(body):
        repeat(count // tile, lambda index: body(span(index, tile)))

    def by_blocks(body):
        repeat(blocks, lambda index: body(span(index, block)))

    def inverse_of(values):
        return lax.rsqrt(jnp.mean(values * values, axis=-1, keepdims=True) + 1e-06)

    def wide(values):
        return jnp.broadcast_to(values, (values.shape[0], 128))

    def transpose_to(target, source, first=0):
        def turn_over(index):
            part = span(index, 128)
            values = source[first : first + count, part].astype(F32)
            target[part, first : first + count] = values.T.astype(BF16)

        repeat(full // 128, turn_over)

    def to_beside(which, source, target):
        return remote(source, target, act_out.at[which], act_in.at[which], (beside, rank))

    own_rows, their_rows = pl.ds(0, count), pl.ds(count, count)

    def branch_copy():
        return to_beside(0, branch.at[own_rows], branch.at[their_rows])

    def norm_copy():
        return to_beside(1, norm_two.at[own_rows], norm_two.at[their_rows])

    def grad_copy():
        return to_beside(2, grad_low, grad_in)

    def mlp_copy():
        return to_beside(3, mlp_low, mlp_in)

    slab = pairs * rows
    halves = length // slab

    def fetch(source, seq, step, place):
        def copy(index):
            pltpu.make_async_copy(
                source.at[seq, pl.ds(pl.multiple_of(index * rows, rows) + step * slab, rows)],
                from_core.at[place, index],
                fetched.at[place],
            ).start()

        each(pairs, copy)

    def down_and_across(seq):
        across = routes[pl.ds(rank * seqs + seq, 1), :].astype(F32)
        return jnp.broadcast_to(across, (caps, caps)).T, across

    def mask(seq):
        down, across = down_and_across(seq)
        begin = pic_start[rank * seqs + seq].astype(F32)
        inside_down = (down >= begin) & (down < begin + PIC)
        inside_across = (across >= begin) & (across < begin + PIC)
        seen = (across <= down) | (inside_down & inside_across)
        allowed[seq] = seen.astype(F32)

    def pick(target, seq, place):
        down, _ = down_and_across(seq)
        column = lax.broadcasted_iota(jnp.int32, (caps, slab), 1).astype(F32)
        for step in range(halves):
            pltpu.make_async_copy(
                from_core.at[place + step], from_core.at[place + step], fetched.at[place + step]
            ).wait()

        def body(part):
            total = 0.0
            for step in range(halves):
                chosen = (down[:, 0:1] == column + step * slab).astype(F32).astype(BF16)
                source = from_core[place + step, :, :, part].reshape(slab, block)
                total = total + contract(chosen, source, 1, 0)
            target[pl.ds(seq * caps, caps), part] = total.astype(BF16)

        by_blocks(body)

    def prepare():
        def body(part):
            values = picked[part].astype(F32)
            logit = jnp.sum(values * router(), axis=-1, keepdims=True)
            gate = 1.0 / (1.0 + jnp.exp(-logit))
            gates[part] = wide(gate)
            norm_one[part] = (values * inverse_of(values) * gain_one()).astype(BF16)
            branch[part] = (gate * grad_rows[part].astype(F32)).astype(BF16)

        by_rows(body)
        transpose_to(branch_t, branch)

    def send_branch():
        branch_copy().start()

    def project(which):
        def body(part):
            qkv[which, :, part] = contract(norm_one[...], held[which, :, part], 1, 0).astype(BF16)

        by_blocks(body)

    lanes = lax.broadcasted_iota(jnp.int32, (1, 2 * HD), 1)

    def own_lanes(values, head):
        inside = (lanes < HD) if head == 0 else (lanes >= HD)
        return jnp.where(inside, values, jnp.zeros_like(values))

    def probabilities(seq, queries, keys, head):
        scores = contract(own_lanes(queries, head), keys, 1, 1) * (1.0 / math.sqrt(HD))
        scores = jnp.where(allowed[seq] > 0, scores, -1e30)
        powers = jnp.exp(scores - jnp.max(scores, axis=-1, keepdims=True))
        return powers / jnp.sum(powers, axis=-1, keepdims=True)

    def attend():
        def body(index):
            part = span(index, 2 * HD)
            for seq in range(seqs):
                place = pl.ds(seq * caps, caps)
                queries, keys = qkv[0, place, part], qkv[1, place, part]
                values = qkv[2, place, part]
                total = 0.0
                for head in range(2):
                    probs = probabilities(seq, queries, keys, head).astype(BF16)
                    total = total + contract(probs, own_lanes(values, head), 1, 0)
                context[place, part] = total.astype(BF16)

        repeat(full // (2 * HD), body)

    def leave_attention():
        def body(part):
            attended[:, part] = contract(context[...], held[3, part, :], 1, 1)

        by_blocks(body)

        def rest(part):
            values = picked[part].astype(F32) + attended[part]
            norm_two[part] = (values * inverse_of(values) * gain_two()).astype(BF16)

        by_rows(rest)
        norm_copy().start()
        transpose_to(norm_two_t, norm_two)
        mlp[...] = jnp.zeros_like(mlp)
        grad_two[...] = jnp.zeros_like(grad_two)

    def by_lines(body):
        repeat(2 * blocks, lambda i: body(span(lax.rem(i, 2), count), span(lax.div(i, 2), block)))

    def go_up(up):
        if up == 4:
            norm_copy().wait_recv()
            transpose_to(norm_two_t, norm_two, count)

        def units_of(lines, part):
            pre = contract(norm_two[lines], held[up, :, part], 1, 0)
            bell = 0.5 * (1.0 + lax.erf(pre * inv_root_two))
            slopes[lines, part] = bell + pre * jnp.exp(-0.5 * pre * pre) * inv_root_two_pi
            hidden[lines, part] = (pre * bell).astype(BF16)

        by_lines(units_of)

    def go_down(up, down):
        if up == 4:
            branch_copy().wait_recv()
            transpose_to(branch_t, branch, count)

        def units_of(lines, part):
            grad_hidden = contract(branch[lines], held[down, :, part], 1, 0)
            grad_pre[lines, part] = (grad_hidden * slopes[lines, part]).astype(BF16)

        by_lines(units_of)

        def add_out(target, source, weight, lines):
            def body(part):
                target[lines, part] += contract(source[lines], held[weight, part, :], 1, 1)

            by_blocks(body)

        def pass_on(source, target, copy):
            if down == chunks - 1:

                def body(part):
                    target[part] = source[pl.ds(part.start + count, tile)].astype(BF16)

                by_rows(body)
                copy().start()

        add_out(grad_two, grad_pre, up, their_rows)
        pass_on(grad_two, grad_low, grad_copy)
        add_out(mlp, hidden, down, their_rows)
        pass_on(mlp, mlp_low, mlp_copy)
        add_out(grad_two, grad_pre, up, own_rows)
        add_out(mlp, hidden, down, own_rows)
        all_sent(up, 1)
        all_sent(down, 1)

        def gradients(part):
            held[down, :, part] = contract(branch_t[...], hidden[:, part], 1, 0).astype(BF16)
            held[up, :, part] = contract(norm_two_t[...], grad_pre[:, part], 1, 0).astype(BF16)

        by_blocks(gradients)

    small = params

    def enter_back():
        small[3:6, :] = jnp.zeros((3, full), F32)
        grad_copy().wait_recv()

        def body(part):
            values = picked[part].astype(F32)
            residual = values + attended[part]
            inverse = inverse_of(residual)
            grad = grad_two[part] + grad_in[part].astype(F32)
            small[5:6, :] += jnp.sum(grad * residual * inverse, axis=0, keepdims=True)
            scaled = grad * gain_two()
            mean = jnp.mean(scaled * residual, axis=-1, keepdims=True)
            grad_mid = inverse * scaled - residual * (inverse * inverse * inverse * mean)
            grad_two[part] = grad_mid
            rows_in = grad_rows[part].astype(F32)
            grad_attended[part] = (gates[part, 0:1] * rows_in + grad_mid).astype(BF16)

        by_rows(body)
        transpose_to(grad_attended_t, grad_attended)

        def through(part):
            grad_context[:, part] = contract(grad_attended[...], held[3, :, part], 1, 0).astype(BF16)

        by_blocks(through)
        for chunk in range(4):
            all_sent(chunk, 0)

        def weights(part):
            held[3, :, part] = contract(grad_attended_t[...], context[:, part], 1, 0).astype(BF16)

        by_blocks(weights)

    def recall():
        def body(index):
            part = span(index, 2 * HD)
            for seq in range(seqs):
                place = pl.ds(seq * caps, caps)
                queries, keys = qkv[0, place, part], qkv[1, place, part]
                for head in range(2):
                    slopes[pl.ds((2 * seq + head) * caps, caps), part] = probabilities(
                        seq, queries, keys, head
                    )

        repeat(full // (2 * HD), body)

    def attend_back():
        def body(index):
            part = span(index, 2 * HD)
            for seq in range(seqs):
                place = pl.ds(seq * caps, caps)
                queries, keys = qkv[0, place, part], qkv[1, place, part]
                values, grad = qkv[2, place, part], grad_context[place, part]
                grad_q, grad_k, grad_v = 0.0, 0.0, 0.0
                for head in range(2):
                    probs = slopes[pl.ds((2 * seq + head) * caps, caps), part]
                    grad_probs = contract(own_lanes(grad, head), values, 1, 1)
                    inner = jnp.sum(probs * grad_probs, axis=-1, keepdims=True)
                    grad_scores = (probs * (grad_probs - inner)).astype(BF16)
                    low = probs.astype(BF16)
                    grad_v = grad_v + contract(low, own_lanes(grad, head), 0, 0)
                    grad_q = grad_q + contract(grad_scores, own_lanes(keys, head), 1, 0)
                    grad_k = grad_k + contract(grad_scores, own_lanes(queries, head), 0, 0)
                scale = 1.0 / math.sqrt(HD)
                grad_qkv[0, place, part] = (grad_q * scale).astype(BF16)
                grad_qkv[1, place, part] = (grad_k * scale).astype(BF16)
                grad_qkv[2, place, part] = grad_v.astype(BF16)

        repeat(full // (2 * HD), body)

    def leave_back():
        def through(part):
            total = contract(grad_qkv[0], held[0, part, :], 1, 1)
            for which in (1, 2):
                total = total + contract(grad_qkv[which], held[which, part, :], 1, 1)
            grad_one[:, part] = total

        by_blocks(through)

    def weigh_back():
        transpose_to(norm_one_t, norm_one)

        def weights(part):
            for which in range(3):
                held[which, :, part] = contract(norm_one_t[...], grad_qkv[which, :, part], 1, 0).astype(
                    BF16
                )

        by_blocks(weights)

    def close():
        mlp_copy().wait_recv()

        def body(part):
            values = picked[part].astype(F32)
            rows_in = grad_rows[part].astype(F32)
            gate = gates[part, 0:1]
            delta = attended[part] + (mlp[part] + mlp_in[part].astype(F32))
            new_rows[part] = (values + gate * delta).astype(BF16)
            score = jnp.sum(rows_in * delta, axis=-1, keepdims=True) * gate * (1.0 - gate)
            small[3:4, :] += jnp.sum(score * values, axis=0, keepdims=True)
            inverse = inverse_of(values)
            grad = grad_one[part]
            small[4:5, :] += jnp.sum(grad * values * inverse, axis=0, keepdims=True)
            scaled = grad * gain_one()
            mean = jnp.mean(scaled * values, axis=-1, keepdims=True)
            grad_norm = inverse * scaled - values * (inverse * inverse * inverse * mean)
            total = rows_in + grad_two[part] + grad_norm + score * router()
            new_grads[part] = total.astype(BF16)

        by_rows(body)
        own = small[...]
        if rows == 128:
            for index in range(1 << bits):
                grad_vecs[index] = own[:, index * rows : (index + 1) * rows]
        else:
            column = lax.broadcasted_iota(jnp.int32, (full, 128), 0)
            lane = lax.broadcasted_iota(jnp.int32, (full, 128), 1)

            def place(index):
                chosen = ((lane < rows) & (column == index * rows + lane)).astype(F32)
                grad_vecs[index] = jnp.dot(
                    own, chosen, precision=lax.Precision.HIGHEST, preferred_element_type=F32
                )

            repeat(1 << bits, place)

    keep_vec = pltpu.make_async_copy(vec, vecs.at[me], local.at[chunks])
    keep_vec.start()
    for chunk in range(4):
        start(chunk)
        start_z(chunk)
    for chunk in range(4, chunks):
        start(chunk)
    for which, source in enumerate((activations, cotangent)):
        for seq in range(seqs):
            for step in range(halves):
                fetch(source, seq, step, (which * seqs + seq) * halves + step)
    keep_vec.wait()
    vec_gather(0)

    events = []

    def at(when, what, *args):
        events.append((when, len(events), functools.partial(what, *args)))

    def between(first, last, step, steps):
        return first + (last - first) * step / max(steps, 1)

    for stage in range(1, bits + 1):
        at(3.8 + 2.2 * stage, vec_gather, stage)
    for seq in range(seqs):
        at(9 + seq, mask, seq)
        for which, target in enumerate((picked, grad_rows)):
            at(9 + seq, pick, target, seq, (which * seqs + seq) * halves)
    for chunk in range(4, chunks):
        at(7.5, start_z, chunk)
    at(3.8 + 2.2 * bits + 3.2, spell_params)
    at(3.8 + 2.2 * bits + 3.2, prepare)
    weights_in = [33 + 8.5 * chunk for chunk in range(4)] + [
        71 + 11.2 * chunk for chunk in range(units)
    ]
    for chunk in range(chunks):
        kind = int(chunk >= 4)
        opened = (54 + 8.3 * (chunk - 4)) if kind else (13 + 8.5 * chunk)
        for stage in range(kind, bits):
            when = between(opened, weights_in[chunk] - 4, stage - kind, bits - 1 - kind)
            at(when, gather_stage, chunk, kind, stage)
        at(weights_in[chunk], gather_stage, chunk, kind, bits)
    for chunk in range(3):
        at(weights_in[chunk], project, chunk)
    at(47, send_branch)
    at(weights_in[2], attend)
    at(weights_in[3], leave_attention)
    for item in range(0, units, 2):
        up, down = item + 4, item + 5
        at(max(weights_in[up], 74) + 0.1, go_up, up)
        ready = weights_in[down] + 0.1
        at(ready, go_down, up, down)
        for one in (item, item + 1):
            at(ready, give_core, one)
    at(116.5, recall)
    at(120, enter_back)
    at(120, give_core, units)
    at(126, attend_back)
    at(134, leave_back)
    at(134, close)
    at(134.2, weigh_back)
    for item in range(units + 1, chunks):
        at(134.3, give_core, item)
    summed = [
        (93.1, 115, 116, 147, 178),
        (93.1, 123, 124, 147.1, 178),
        (115, 132, 133, 148, 178),
        (115.1, 143.1, 143.15, 173, 184),
        (125, 143.2, 160, 177, 0),
        (143, 158, 170, 181, 0),
        (143.3, 166, 175, 185, 0),
        (158.1, 172, 178, 187, 0),
    ]
    for item, (core_in, second, last, across, aside) in enumerate(summed):
        kind = int(item < units)
        final = bits - kind
        at(core_in, scatter_stage, item, kind, 1)
        for stage in range(2, final + 1):
            when = last if final == 2 else between(second, last, stage - 2, final - 2)
            at(when, scatter_stage, item, kind, stage)
        at(across, scatter_stage, item, kind, final + 1)
        if kind:
            at(aside, scatter_stage, item, kind, final + 2)
    for stage in range(bits + 1):
        when = (134.1, 142.9, 143.05, 164.5)[stage] if stage < 4 else 164.5 + 2 * stage
        at(when, vec_stage, stage)
    at(188, vec_finish)
    for _, _, event in sorted(events, key=lambda event: event[:2]):
        event()

    branch_copy().wait_send()
    norm_copy().wait_send()
    grad_copy().wait_send()
    mlp_copy().wait_send()

    def drain(item, kind):
        given_core(item).wait_send()
        for colour in range(2):
            for stage in range(bits - 1 - kind):
                given_path(item, colour, stage).wait_send()
        given_across(item, kind).wait_send()
        if kind:
            side_copy(item).wait_send()

    for item in range(chunks):
        drain(item, int(item < units))


def run_layer(bits, ranks, shards, vec, routes, pic_start, activations, cotangent):
    rows, width = shards[0].shape
    parts = shards[4].shape[1] // width
    chunks = 4 + parts
    depth, breadth, pairs = rows << bits, width * ranks, 1 << (bits - 1)
    seqs, _, full = activations.shape
    caps = routes.shape[1]
    count = seqs * caps
    dma = pltpu.SemaphoreType.DMA
    low = pltpu.VMEM((count, full), BF16)
    turned = pltpu.VMEM((full, count), BF16)
    high = pltpu.VMEM((count, full), F32)
    low_two = pltpu.VMEM((2 * count, full), BF16)
    turned_two = pltpu.VMEM((full, 2 * count), BF16)
    high_two = pltpu.VMEM((2 * count, full), F32)
    return pl.pallas_call(
        functools.partial(layer_kernel, bits, ranks, chunks, parts),
        out_shape=[
            *[jax.ShapeDtypeStruct((rows, width), F32)] * 4,
            *[jax.ShapeDtypeStruct((rows, width * parts), F32)] * 2,
            jax.ShapeDtypeStruct((8, 128), F32),
            jax.ShapeDtypeStruct((count, full), BF16),
            jax.ShapeDtypeStruct((count, full), BF16),
        ],
        in_specs=[ANY] * 6 + [VMEM] * 2 + [pl.BlockSpec(memory_space=pltpu.SMEM)] + [ANY] * 2,
        out_specs=[VMEM] * 9,
        scratch_shapes=[
            low,
            low,
            pltpu.VMEM((seqs, caps, caps), F32),
            pltpu.VMEM((chunks, depth, breadth), BF16),
            pltpu.VMEM((RING, pairs, rows, breadth), BF16),
            pltpu.VMEM((chunks, 2 * (ranks - 1), rows, width), BF16),
            pltpu.VMEM((1 << bits, 8, 128), F32),
            pltpu.VMEM((1 << bits, 8, 128), F32),
            pltpu.VMEM((1 << bits, 8, 128), F32),
            pltpu.VMEM((ranks - 1, 8, 128), F32),
            pltpu.VMEM((8, full), F32),
            pltpu.VMEM((count, 128), F32),
            low,
            pltpu.VMEM((3, count, full), BF16),
            low,
            high,
            low_two,
            turned_two,
            low_two,
            turned_two,
            low_two,
            low_two,
            high_two,
            high_two,
            high_two,
            low,
            low,
            low,
            low,
            low,
            turned,
            low,
            pltpu.VMEM((3, count, full), BF16),
            high,
            turned,
            pltpu.VMEM((parts, rows, width), BF16),
            pltpu.VMEM((parts, rows, width), BF16),
            dma((chunks,)),
            dma((chunks,)),
            dma((4,)),
            dma((4,)),
            dma((parts,)),
            dma((parts,)),
            dma((chunks,)),
            dma((chunks,)),
            dma((chunks, 2, bits - 1)),
            dma((chunks, 2, bits - 1)),
            dma((chunks,)),
            dma((chunks,)),
            dma((bits,)),
            dma((bits,)),
            dma((chunks + 1,)),
            dma((chunks,)),
            dma((chunks,)),
            dma((chunks, 2, bits - 1)),
            dma((chunks, 2, bits - 1)),
            dma((chunks,)),
            dma((chunks,)),
            dma((bits + 1,)),
            dma((bits + 1,)),
            dma((RING,)),
            *[
                pltpu.VMEM((chunks, 2, pairs >> (stage + 1), rows, breadth // 2), BF16)
                for stage in range(bits - 1)
            ],
        ],
        compiler_params=pltpu.CompilerParams(
            collective_id=1, has_side_effects=True, vmem_limit_bytes=67043328
        ),
        name="layer_kernel",
    )(*shards, vec, routes, pic_start, activations, cotangent)


def shards(
    activations,
    routes,
    pic_start,
    router_w,
    gain_attn,
    gain_mlp,
    w_query,
    w_key,
    w_value,
    w_proj,
    w_up,
    w_down,
    cotangent,
):
    ranks = lax.axis_size("tensor")
    bits = lax.axis_size("dp").bit_length() - 1
    rows, width = w_query.shape
    parts = w_up.shape[1] // width
    vec = jnp.stack([router_w, gain_attn, gain_mlp]).astype(F32)
    vec = jnp.pad(vec, ((0, 5), (0, 128 - rows)))
    weights = (w_query, w_key, w_value, w_proj, w_up, w_down)
    *sums, small, new_rows, new_grads = run_layer(
        bits, ranks, weights, vec, routes, pic_start, activations, cotangent
    )
    seqs, length, features = activations.shape
    own = lax.dynamic_slice_in_dim(routes, lax.axis_index("tensor") * seqs, seqs, 0)
    chosen = (own[:, :, None] == jnp.arange(length)[None, None, :]).astype(BF16)
    routed = jnp.sum(chosen.astype(F32), axis=1) > 0

    def put(base, new):
        placed = jnp.einsum(
            "scl,scd->sld",
            chosen,
            new.reshape(seqs, -1, features),
            preferred_element_type=F32,
        )
        return jnp.where(routed[:, :, None], placed.astype(BF16), base)

    return (
        put(activations, new_rows),
        put(cotangent, new_grads),
        small[3, :rows],
        small[4, :rows],
        small[5, :rows],
        *sums,
    )


def solution(mesh):
    both = P(("dp", "tensor"), None, None)
    cut = P("dp", "tensor")
    one = P("dp")
    return jax.shard_map(
        shards,
        mesh=mesh,
        in_specs=(both, P("dp", None), one, one, one, one) + (cut,) * 6 + (both,),
        out_specs=(both, both, one, one, one) + (cut,) * 6,
        check_vma=False,
    )
```
